512 devices in a mesh: tok: 32 (over z_hi, y), voc: 16 (over z_lo, x, core).
Axes of the slice: x: 4, y: 8, z: 8 (z_hi: 4, z_lo: 2; z = z_hi * 2 + z_lo), core: 2. Of those that a mesh axis runs over, the one named last changes fastest.
Arguments:
- hidden: bfloat16 [4096, 2048], P('tok'), may hold values from -6 to 6
- mix_weight: bfloat16 [4, 2048], P(None, 'voc'), may hold values from -0.0546875 to 0.0546875
- comp_proj: bfloat16 [2048, 4, 2048], P(None, None, 'voc'), may hold values from -0.110485435 to 0.110485435
- vocab_weight: bfloat16 [2048, 4096], P(None, 'voc'), may hold values from -0.625 to 0.625
- log_normalizer: float32 [4, 4096], P(None, 'tok'), may hold values from 11 to 11.6
- targets: int32 [4096], P('tok'), may hold values from 0 to 4095
- loss_grad: float32 [4096], P('tok'), may hold values from 0.5 to 1.5
Outputs:
- hidden_grad: bfloat16 [4096, 2048], P('tok', 'voc')
- proj_grad: bfloat16 [2048, 4, 2048], P('tok', None, 'voc')
- vocab_grad: bfloat16 [2048, 4096], P('tok', 'voc')
The draws below stay inside these ranges and needn't reach their ends.
All inputs are finite; a program needn't handle non-finite values.
Results may differ from the reference program's by a relative error of at most 0.02.
Values may be sent and summed in bfloat16 or wider, within the bound.
A program may use at most 64 MiB of HBM per device.

```python
import jax
import jax.numpy as jnp
from jax import lax

D = 2048
K = 4
TOK_DEV = 128
V_DEV = 256
TOKENS = 4096
VOCAB = 4096
N_TOK = 32
N_VOC = 16


def draw_comp_proj(key, part):
    base_key = jax.random.fold_in(key, 11)
    noise_key = jax.random.fold_in(key, 12)
    shared = jax.random.truncated_normal(base_key, -4.0, 4.0, (D, 1, D), jnp.float32)
    private = jax.random.truncated_normal(noise_key, -4.0, 4.0, (D, K, D), jnp.float32)
    values = (0.98869 * shared + 0.15 * private) * D ** (-0.5)
    return values.astype(jnp.bfloat16)


def set_ends(array, stream_key, low, top_value):
    longest = array.shape.index(max(array.shape))
    spots = []
    for shift in (0, 1):
        where = [jax.random.randint(jax.random.fold_in(stream_key, axis), (), 0, length) for axis, length in enumerate(array.shape)]
        where[longest] = (where[longest] + shift) % array.shape[longest]
        spots.append(tuple(where))
    return array.at[spots[0]].set(low).at[spots[1]].set(top_value)


def level_of(key, shape, cuts, smallest, high):
    def one(position, parts):
        heights = jax.random.uniform(jax.random.fold_in(jax.random.fold_in(key, 6), position), (parts,), jnp.float32, smallest / len(cuts), high / len(cuts))
        return jnp.repeat(jnp.exp(heights), shape[position] // parts).reshape((-1,) + (1,) * (len(shape) - position - 1))

    level = one(*cuts[0])
    for cut in cuts[1:]:
        level = level * one(*cut)
    return level


def noise(key, extent, width, reach, split=(), kind=jnp.bfloat16):
    entries = jax.random.normal(key, extent, jnp.float32) * width
    if len(split) > 0:
        entries = level_of(key, extent, split, -0.22, 0.18) * entries
    return jnp.clip(entries, min=-reach, max=reach).astype(kind)


def setup_inputs(seed: int = 0) -> dict:
    key_of = jax.random.split(jax.random.key(seed), 8)
    hidden = noise(key_of[0], (TOKENS, D), 1.0, 6.0, ((0, 32),))
    mix_weight = noise(key_of[1], (K, D), (6 * D) ** -0.5, 0.0546875, ((1, 16),))
    comp_proj = draw_comp_proj(jax.random.fold_in(key_of[7], 71), 0)
    vocab_weight = noise(key_of[3], (D, VOCAB), 0.1, 0.625, ((1, 16),))
    log_normalizer = jnp.clip(11.0 + 0.6000004 * jax.random.uniform(key_of[4], (K, TOKENS), jnp.float32) ** level_of(key_of[4], (K, TOKENS), ((1, 32),), -0.2, 0.2), 11.0, 11.6)
    targets = set_ends(jax.random.randint(key_of[5], (TOKENS,), 0, VOCAB), jax.random.fold_in(key_of[5], 1), 0, VOCAB - 1).astype(jnp.int32)
    loss_grad = jnp.clip(0.5 + 1.0 * jax.random.uniform(key_of[6], (TOKENS,), jnp.float32) ** level_of(key_of[6], (TOKENS,), ((0, 32),), -0.2, 0.2), 0.5, 1.5)
    return {"hidden": hidden, "mix_weight": mix_weight, "comp_proj": comp_proj, "vocab_weight": vocab_weight, "log_normalizer": log_normalizer, "targets": targets, "loss_grad": loss_grad}


def rounded(values):
    return lax.optimization_barrier(values.astype(jnp.bfloat16)).astype(jnp.float32)


def reference(hidden, mix_weight, comp_proj, vocab_weight, log_normalizer, targets, loss_grad):
    highest = lax.Precision.HIGHEST
    weight_full = vocab_weight.astype(jnp.float32)
    proj_full = comp_proj.astype(jnp.float32)
    mix_full = mix_weight.astype(jnp.float32)
    vocab_ids = jnp.arange(VOCAB, dtype=jnp.int32)
    hidden_groups = hidden.reshape(N_TOK, TOK_DEV, D)
    norm_groups = jnp.transpose(log_normalizer.reshape(K, N_TOK, TOK_DEV), (1, 0, 2))
    target_groups = targets.reshape(N_TOK, TOK_DEV)
    cotangent_groups = loss_grad.reshape(N_TOK, TOK_DEV)

    def one_group(running, inputs):
        vocab_sum, proj_sum = running
        states, normalizer, wanted, cotangent = inputs
        states_f = states.astype(jnp.float32)
        contexts = jnp.tanh(jnp.einsum("td,dke->tke", states_f, proj_full, precision=highest)).astype(jnp.bfloat16)
        context_f = contexts.astype(jnp.float32)
        logits = jnp.einsum("tkd,dv->ktv", context_f, weight_full, precision=highest)
        mixing = jnp.einsum("td,kd->kt", states_f, mix_full, precision=highest)
        onehot = (wanted[:, None] == vocab_ids[None, :]).astype(jnp.float32)
        target = jnp.sum(logits * onehot[None], axis=2)
        exp_mix = jnp.exp(mixing)
        weights = exp_mix / jnp.sum(exp_mix, axis=0, keepdims=True)
        likely = jnp.exp(target - normalizer)
        joint_mass = weights * likely
        posterior = joint_mass / jnp.sum(joint_mass, axis=0, keepdims=True)
        factor = cotangent[None, :] * posterior
        logit_grad = (factor[:, :, None] * (jnp.exp(logits - normalizer[:, :, None]) - onehot[None])).astype(jnp.bfloat16)
        mixing_grad = cotangent[None, :] * (weights - posterior)
        grad_f = logit_grad.astype(jnp.float32)
        vocab_part = jnp.einsum("tkd,ktv->dv", context_f, grad_f, precision=highest)
        vocab_sum = vocab_sum + rounded(vocab_part)
        blocks = jnp.einsum("ktbv,dbv->btkd", grad_f.reshape(K, TOK_DEV, N_VOC, V_DEV), weight_full.reshape(D, N_VOC, V_DEV), precision=highest)
        context_grad = jnp.sum(rounded(blocks), axis=0)
        pre_grad = rounded(context_grad * (1.0 - context_f * context_f))
        hidden_grad = (jnp.einsum("tke,jke->tj", pre_grad, proj_full, precision=highest) + jnp.einsum("kt,kd->td", mixing_grad, mix_full, precision=highest)).astype(jnp.bfloat16)
        proj_sum = proj_sum + jnp.einsum("tj,tke->jke", states_f, pre_grad, precision=highest)
        return (vocab_sum, proj_sum), hidden_grad

    start_state = (jnp.zeros((D, VOCAB), jnp.float32), jnp.zeros((D, K, D), jnp.float32))
    final_state, hidden_grads = lax.scan(one_group, start_state, (hidden_groups, norm_groups, target_groups, cotangent_groups))
    vocab_sum, proj_sum = final_state
    return hidden_grads.reshape(TOKENS, D), proj_sum.astype(jnp.bfloat16), vocab_sum.astype(jnp.bfloat16)
```

```python
import jax
import jax.numpy as jnp
from jax import lax
from jax.experimental import pallas as pl
from jax.experimental.pallas import tpu as pltpu
from jax.sharding import Mesh
from jax.sharding import PartitionSpec as P

MESH = pl.DeviceIdType.MESH
BF, F32 = jnp.bfloat16, jnp.float32
ZH, Y, ZL, X, C = 4, 8, 2, 4, 2
D, K, T, V, E = 2048, 4, 128, 256, 128
N_SEND, N_RECV = 260, 230
ORDER = (0, 2, 1, 3)

NT = (((1,), (1,)), ((), ()))
TN = (((0,), (0,)), ((), ()))


def mm(a, b):
    return jnp.dot(a, b, preferred_element_type=F32)


def mm_nt(a, b):
    return lax.dot_general(a, b, NT, preferred_element_type=F32)


class Net:
    def __init__(self, send_sems, recv_sems):
        self.send_sems, self.recv_sems = send_sems, recv_sems
        self.roles, self.sent = {}, []

    def slot(self, role):
        return self.recv_sems.at[self.roles.setdefault(role, len(self.roles))]

    def send(self, src, dst, role, device):
        copy = pltpu.make_async_remote_copy(
            src_ref=src,
            dst_ref=dst,
            send_sem=self.send_sems.at[len(self.sent)],
            recv_sem=self.slot(role),
            device_id=device,
            device_id_type=MESH,
        )
        copy.start()
        self.sent.append(copy)

    def got(self, dst, role):
        pltpu.make_async_remote_copy(
            src_ref=dst,
            dst_ref=dst,
            send_sem=self.send_sems.at[0],
            recv_sem=self.slot(role),
            device_id={"c": 1 - lax.axis_index("c")},
            device_id_type=MESH,
        ).wait_recv()

    def finish(self):
        for copy in self.sent:
            copy.wait_send()


def kernel(
    hid_hbm, cp_hbm, w_hbm, mw_ref, ln_ref, tg_ref, loss_ref,
    hg_ref, pg_ref, vg_ref,
    hid, cpraw, stage, cp, w, wt, wp, ctx, eb, lgt, lgp, arx,
    cgb, r2, sp, rxm, rxp, xs, zs, zr, pgz, pgs, hx, ht, pp, prx, pst,
    hpb, hrx, vgb, vrx, vzs, vzr,
    send_sems, recv_sems, local_sems,
):
    zh, y = lax.axis_index("zh"), lax.axis_index("y")
    zl, x, c = lax.axis_index("zl"), lax.axis_index("x"), lax.axis_index("c")
    voc = zl * 8 + x * 2 + c
    net = Net(send_sems, recv_sems)

    def xat(dx):
        return lax.rem(x + dx + X, X)

    def yat(dy):
        return lax.rem(y + dy, Y)

    def zat(dz):
        return lax.rem(zh + dz, ZH)

    def peer(dl, dx, dc):
        return {"zl": (zl + dl) % 2, "x": xat(dx), "c": (c + dc) % 2}

    def lanes(k):
        return pl.ds(k * T, T)

    right, left = {"x": xat(1)}, {"x": xat(-1)}
    other, over = {"c": 1 - c}, {"zl": 1 - zl}
    voc_peers = [(dl, dx, dc) for dl in range(2) for dx in range(4) for dc in range(2)][1:]

    parts = 4
    rows = D * K // parts
    loads = [pltpu.make_async_copy(hid_hbm, hid, local_sems.at[0])]
    for q in range(parts):
        span = pl.ds(q * rows, rows)
        loads.append(pltpu.make_async_copy(cp_hbm.at[span], cpraw.at[span], local_sems.at[1 + q]))
    loads.append(pltpu.make_async_copy(w_hbm, w, local_sems.at[1 + parts]))
    for load in loads:
        load.start()
    barrier = pltpu.get_barrier_semaphore()
    greeted = [peer(*p) for p in voc_peers]
    greeted += [{"y": yat(dy)} for dy in range(1, Y)] + [{"zh": zat(dz)} for dz in range(1, ZH)]
    for device in greeted:
        pl.semaphore_signal(barrier, inc=1, device_id=device, device_id_type=MESH)

    loads[0].wait()
    pre = jnp.zeros((T, K * E), F32)
    for q in range(parts):
        loads[1 + q].wait()
        stage[...] = cpraw[pl.ds(q * rows, rows), :].astype(F32)
        span = pl.ds(q * (D // parts), D // parts)
        for k in range(K):
            cp[span, lanes(k)] = stage[pl.ds(k, D // parts, stride=K), :].astype(BF)
        pre = pre + mm(hid[:, span], cp[span, :])
    acts = jnp.tanh(pre)

    def block(dl, dx, dc, k):
        at = (zl + dl) % 2 * 8 + xat(dx) * 2 + (c + dc) % 2
        return ctx.at[pl.ds(pl.multiple_of(at * E, E), E), lanes(k)]

    for k in range(K):
        ctx[pl.ds(pl.multiple_of(voc * E, E), E), lanes(k)] = acts[:, k * E : (k + 1) * E].T.astype(BF)
    mw = jnp.concatenate([mw_ref[...].astype(F32), jnp.zeros((4, E), F32)], axis=0)
    own_hid = hid[:, pl.ds(pl.multiple_of(voc * E, E), E)]
    mix_part = mm_nt(mw.astype(BF), own_hid)

    pl.semaphore_wait(barrier, len(greeted))

    def push(dl, dx, k, role, device):
        net.send(block(dl, dx, 0, k), block(dl, dx, 0, k), role, device)

    for k in range(K):
        push(0, 0, k, ("ag", 1, 0, k), over)
        push(0, 0, k, ("ag", 0, -1, k), right)
        push(0, 0, k, ("ag", 0, 1, k), left)
        push(0, 0, k, ("ac", 0, 0, k), other)
    loads[1 + parts].wait()
    net.send(w.at[:, 1 - c], wp, ("wp",), other)
    for j in range(16):
        wt[:, j * 128 : (j + 1) * 128] = w[j // 2, j % 2].T

    def from_left(dl, k):
        net.got(block(dl, -1, 0, k), ("ag", dl, -1, k))
        if k < 2:
            push(dl, -1, k, ("ag", dl, 2, k), right)
        push(dl, -1, k, ("ac", dl, -1, k), other)

    def from_right(dl, k):
        net.got(block(dl, 1, 0, k), ("ag", dl, 1, k))
        if k >= 2:
            push(dl, 1, k, ("ag", dl, 2, k), left)
        push(dl, 1, k, ("ac", dl, 1, k), other)

    def from_far(dl, k):
        net.got(block(dl, 2, 0, k), ("ag", dl, 2, k))
        push(dl, 2, k, ("ac", dl, 2, k), other)

    for k in range(K):
        net.got(block(1, 0, 0, k), ("ag", 1, 0, k))
        push(1, 0, k, ("ag", 1, -1, k), right)
        push(1, 0, k, ("ag", 1, 1, k), left)
        push(1, 0, k, ("ac", 1, 0, k), other)
        from_left(0, k)
        from_right(0, k)
    for dz in (1, 3, 2):
        span = pl.ds(pl.multiple_of(zat(dz) * 512, 512), 512)
        net.send(hid.at[:, span], hx.at[dz], ("hx", dz), {"zh": zat(dz)})
    hx[0] = hid[:, pl.ds(pl.multiple_of(zh * 512, 512), 512)]
    for k in range(K):
        from_left(1, k)
        from_right(1, k)
        from_far(0, k)

    ids = lax.broadcasted_iota(jnp.int32, (V, T), 0) + voc * V
    hit = ids == tg_ref[...]
    targets = []
    for k in range(K):
        from_far(1, k)
        for dl in range(2):
            for dx in (0, -1, 1, 2):
                net.got(block(dl, dx, 1, k), ("ac", dl, dx, k))
        logits = mm(wt[...], ctx[:, lanes(k)])
        targets.append(jnp.sum(jnp.where(hit, logits, 0.0), axis=0, keepdims=True))
        eb[:, lanes(k)] = logits
    arx[0] = jnp.concatenate([*targets, mix_part[:4]], axis=0)
    for i, p in enumerate(voc_peers):
        net.send(arx.at[0], arx.at[i + 1], ("ar", i), peer(*p))
    onehot = hit.astype(F32)
    for k in range(K):
        eb[:, lanes(k)] = jnp.exp(eb[:, lanes(k)] - ln_ref[k : k + 1, :]) - onehot
    for i in range(len(voc_peers)):
        net.got(arx.at[i + 1], ("ar", i))
    sums = jnp.sum(arx[...], axis=0)
    exp_mix = jnp.exp(sums[4:])
    weights = exp_mix / jnp.sum(exp_mix, axis=0, keepdims=True)
    joint = weights * jnp.exp(sums[:4] - ln_ref[...])
    posterior = joint / jnp.sum(joint, axis=0, keepdims=True)
    factor = loss_ref[...] * posterior
    mix_grad = loss_ref[...] * (weights - posterior)

    for k in ORDER:
        lgt[:, lanes(k)] = (factor[k : k + 1] * eb[:, lanes(k)]).astype(BF)
        net.send(lgt.at[:, lanes(k)], lgp.at[:, lanes(k)], ("lg", k), other)

    net.got(wp, ("wp",))
    w_own = w[:, pl.ds(c, 1)].reshape(8 * E, V)
    for k in ORDER:
        net.got(lgp.at[:, lanes(k)], ("lg", k))
        part = mm(w_own, lgt[:, lanes(k)]) + mm(wp[...].reshape(8 * E, V), lgp[:, lanes(k)])
        cgb[k] = part.astype(BF).reshape(ZL, X, E, T)
        net.send(cgb.at[k, :, xat(2)], r2.at[k], ("r2", k), right if k < 2 else left)
    near = {k: (-1, left, rxp, "rp") if k < 2 else (1, right, rxm, "rm") for k in range(K)}

    def straight(k):
        dx, device, there, role = near[k]
        net.send(cgb.at[k, :, xat(dx)], there.at[k], (role, k), device)

    def combine(k):
        dx, device, there, role = (1, right, rxm, "rm") if k < 2 else (-1, left, rxp, "rp")
        net.got(r2.at[k], ("r2", k))
        sp[k] = (cgb[k, :, xat(dx)].astype(F32) + r2[k].astype(F32)).astype(BF)
        net.send(sp.at[k], there.at[k], (role, k), device)

    straight(0)
    straight(2)

    for a in range(ZH):
        part = mm_nt(ctx[a * 512 : (a + 1) * 512, :], lgt[...])
        vgb[a] = part.astype(BF).reshape(Y, 64, V)
    combine(0)
    combine(2)
    straight(1)
    straight(3)
    combine(1)
    combine(3)
    for dy in (1, 7, 2, 6, 3, 5, 4):
        net.send(vgb.at[:, yat(dy)], vrx.at[dy], ("vy", dy), {"y": yat(dy)})

    def x_done(k):
        net.got(rxm.at[k], ("rm", k))
        net.got(rxp.at[k], ("rp", k))
        xs[k] = cgb[k, :, x].astype(F32) + rxm[k].astype(F32) + rxp[k].astype(F32)
        zs[k] = xs[k, 1 - zl].astype(BF)
        net.send(zs.at[k], zr.at[k], ("zr", k), over)

    def z_done(k):
        net.got(zr.at[k], ("zr", k))
        own = ctx[pl.ds(pl.multiple_of(voc * E, E), E), lanes(k)].astype(F32)
        pre_grad = ((xs[k, zl] + zr[k].astype(F32)) * (1.0 - own * own)).astype(BF)
        pgz[k, :, 0:T] = pre_grad
        pgs[k * E : (k + 1) * E, :] = pre_grad
        net.send(pgz.at[k, :, lanes(0)], pgz.at[k, :, lanes(1)], ("pz", 1, k), {"zh": zat(1)})
        net.send(pgz.at[k, :, lanes(0)], pgz.at[k, :, lanes(3)], ("pz", 3, k), {"zh": zat(3)})

    x_done(0)
    x_done(2)
    for dz in (1, 3, 2):
        net.got(hx.at[dz], ("hx", dz))
    for dz in range(ZH):
        ht[:, lanes(dz)] = hx[dz].T
    z_done(0)
    z_done(2)
    x_done(1)
    x_done(3)
    z_done(1)
    z_done(3)

    for j in range(4):
        part = mm(cp[j * 512 : (j + 1) * 512, :], pgs[...])
        hpb[4 * j : 4 * j + 4] = part.astype(BF).reshape(4, 128, T)

    def far(k):
        net.got(pgz.at[k, :, lanes(1)], ("pz", 1, k))
        if k < 2:
            net.send(pgz.at[k, :, lanes(1)], pgz.at[k, :, lanes(2)], ("pz", 2, k), {"zh": zat(1)})
        net.got(pgz.at[k, :, lanes(3)], ("pz", 3, k))
        if k >= 2:
            net.send(pgz.at[k, :, lanes(3)], pgz.at[k, :, lanes(2)], ("pz", 2, k), {"zh": zat(3)})

    def proj(k):
        net.got(pgz.at[k, :, lanes(2)], ("pz", 2, k))
        pp[k] = mm_nt(ht[...], pgz[k]).astype(BF).reshape(Y, 64, E)
        for dy in (1, 7, 2, 6, 3, 5, 4):
            net.send(pp.at[k, yat(dy)], prx.at[k, dy], ("py", dy, k), {"y": yat(dy)})

    for k in ORDER:
        far(k)
    for i, p in enumerate(voc_peers):
        at = peer(*p)
        net.send(hpb.at[at["zl"] * 8 + at["x"] * 2 + at["c"]], hrx.at[i], ("hr", i), at)
    for k in ORDER:
        proj(k)

    for dy in range(1, Y):
        net.got(vrx.at[dy], ("vy", dy))
    vrx[0] = vgb[:, y]
    total = vrx[0].astype(F32)
    for dy in range(1, Y):
        total = total + vrx[dy].astype(F32)
    vzs[...] = total.astype(BF)
    for dz in (1, 3, 2):
        net.send(vzs.at[zat(dz)], vzr.at[dz], ("vz", dz), {"zh": zat(dz)})

    for i in range(len(voc_peers)):
        net.got(hrx.at[i], ("hr", i))
    total = hpb[voc].astype(F32)
    for i in range(len(voc_peers)):
        total = total + hrx[i].astype(F32)
    mix_grad = jnp.concatenate([mix_grad, jnp.zeros((4, T), F32)], axis=0)
    mix_term = lax.dot_general(mix_grad, mw, TN, precision=lax.Precision.HIGHEST, preferred_element_type=F32)
    hg_ref[...] = (total.T + mix_term).astype(BF)

    for k in ORDER:
        total = pp[k, y].astype(F32)
        for dy in range(1, Y):
            net.got(prx.at[k, dy], ("py", dy, k))
            total = total + prx[k, dy].astype(F32)
        pst[pl.ds(k, 64, stride=K), :] = total
    pg_ref[...] = pst[...].astype(BF)

    total = vzs[zh].astype(F32)
    for dz in range(1, ZH):
        net.got(vzr.at[dz], ("vz", dz))
        total = total + vzr[dz].astype(F32)
    vg_ref[...] = total.astype(BF)
    net.finish()


def body(hidden, mix_weight, comp_proj, vocab_weight, log_normalizer, targets, loss_grad):
    vmem = pl.BlockSpec(memory_space=pltpu.VMEM)
    hbm = pl.BlockSpec(memory_space=pl.ANY)
    scratch = [
        pltpu.VMEM(shape, dtype)
        for shape, dtype in (
            ((T, D), BF),
            ((D * K, E), BF),
            ((D, E), F32),
            ((D, K * E), BF),
            ((8, 2, 128, V), BF),
            ((V, D), BF),
            ((8, 128, V), BF),
            ((D, K * T), BF),
            ((V, K * T), F32),
            ((V, K * T), BF),
            ((V, K * T), BF),
            ((16, 8, T), F32),
            ((K, ZL, X, E, T), BF),
            ((K, ZL, E, T), BF),
            ((K, ZL, E, T), BF),
            ((K, ZL, E, T), BF),
            ((K, ZL, E, T), BF),
            ((K, ZL, E, T), F32),
            ((K, E, T), BF),
            ((K, E, T), BF),
            ((K, E, ZH * T), BF),
            ((K * E, T), BF),
            ((ZH, T, 512), BF),
            ((512, ZH * T), BF),
            ((K, Y, 64, E), BF),
            ((K, Y, 64, E), BF),
            ((64 * K, E), F32),
            ((16, 128, T), BF),
            ((15, 128, T), BF),
            ((ZH, Y, 64, V), BF),
            ((Y, ZH, 64, V), BF),
            ((ZH, 64, V), BF),
            ((ZH, 64, V), BF),
        )
    ]
    scratch += [pltpu.SemaphoreType.DMA((N_SEND,)), pltpu.SemaphoreType.DMA((N_RECV,)), pltpu.SemaphoreType.DMA((8,))]
    hidden_grad, proj_grad, vocab_grad = pl.pallas_call(
        kernel,
        out_shape=(
            jax.ShapeDtypeStruct((T, E), BF),
            jax.ShapeDtypeStruct((64 * K, E), BF),
            jax.ShapeDtypeStruct((64, V), BF),
        ),
        in_specs=[hbm, hbm, hbm, vmem, vmem, vmem, vmem],
        out_specs=(vmem, vmem, vmem),
        scratch_shapes=scratch,
        compiler_params=pltpu.CompilerParams(
            collective_id=0, has_side_effects=True, vmem_limit_bytes=56 * 1024 * 1024
        ),
    )(
        hidden,
        comp_proj.reshape(D * K, E),
        vocab_weight.reshape(8, 2, 128, V),
        mix_weight,
        log_normalizer,
        targets.reshape(1, T),
        loss_grad.reshape(1, T),
    )
    return hidden_grad, proj_grad.reshape(64, K, E), vocab_grad


def solution(mesh):
    split = Mesh(mesh.devices.reshape(ZH, Y, ZL, X, C), ("zh", "y", "zl", "x", "c"))
    tok, voc = ("zh", "y"), ("zl", "x", "c")
    in_specs = (P(tok, None), P(None, voc), P(None, None, voc), P(None, voc), P(None, tok), P(tok), P(tok))
    out_specs = (P(tok, voc), P(tok, None, voc), P(tok, voc))
    return jax.shard_map(body, mesh=split, in_specs=in_specs, out_specs=out_specs, check_vma=False)
```

```python
import jax
import jax.numpy as jnp
from jax import lax
from jax.experimental import pallas as pl
from jax.experimental.pallas import tpu as pltpu
from jax.sharding import Mesh
from jax.sharding import PartitionSpec as P

MESH = pl.DeviceIdType.MESH
BF, F32 = jnp.bfloat16, jnp.float32
ZH, Y, ZL, X, C = 4, 8, 2, 4, 2
D, K, T, V, E = 2048, 4, 128, 256, 128
N_SEND, N_RECV = 260, 230

NT = (((1,), (1,)), ((), ()))
TN = (((0,), (0,)), ((), ()))


def mm(a, b):
    return jnp.dot(a, b, preferred_element_type=F32)


def mm_nt(a, b):
    return lax.dot_general(a, b, NT, preferred_element_type=F32)


class Net:
    def __init__(self, send_sems, recv_sems):
        self.send_sems, self.recv_sems = send_sems, recv_sems
        self.roles, self.sent = {}, []

    def slot(self, role):
        return self.recv_sems.at[self.roles.setdefault(role, len(self.roles))]

    def send(self, src, dst, role, device):
        copy = pltpu.make_async_remote_copy(
            src_ref=src,
            dst_ref=dst,
            send_sem=self.send_sems.at[len(self.sent)],
            recv_sem=self.slot(role),
            device_id=device,
            device_id_type=MESH,
        )
        copy.start()
        self.sent.append(copy)

    def got(self, dst, role):
        pltpu.make_async_remote_copy(
            src_ref=dst,
            dst_ref=dst,
            send_sem=self.send_sems.at[0],
            recv_sem=self.slot(role),
            device_id={"c": 1 - lax.axis_index("c")},
            device_id_type=MESH,
        ).wait_recv()

    def finish(self):
        for copy in self.sent:
            copy.wait_send()


def kernel(
    hid_hbm, cp_hbm, w_hbm, mw_hbm, ln_hbm, tg_hbm, loss_hbm,
    hg_ref, pg_ref, vg_ref,
    hid, cpraw, stage, cp, w, wt, wp, mw_ref, ln_ref, tg_ref, loss_ref, ctx, eb, lgt, lgp, arx,
    cgb, zf, sf, r2, sp, rxm, rxp, rmo, rpo, zs, zr, pgz, pgs, hx, ht, pp, pc, pn, prx, pst,
    hpb, hrx, vgb, vsb, vrb, vzs, vzr,
    send_sems, recv_sems, local_sems,
):
    zh, y = lax.axis_index("zh"), lax.axis_index("y")
    zl, x, c = lax.axis_index("zl"), lax.axis_index("x"), lax.axis_index("c")
    voc = zl * 8 + x * 2 + c
    net = Net(send_sems, recv_sems)

    def xat(dx):
        return lax.rem(x + dx + X, X)

    def yat(dy):
        return lax.rem(y + dy + Y, Y)

    def zat(dz):
        return lax.rem(zh + dz, ZH)

    def peer(dl, dx, dc):
        return {"zl": (zl + dl) % 2, "x": xat(dx), "c": (c + dc) % 2}

    def lanes(k, n=1):
        return pl.ds(k * T, n * T)

    right, left = {"x": xat(1)}, {"x": xat(-1)}
    up, down = {"y": yat(1)}, {"y": yat(-1)}
    other, over = {"c": 1 - c}, {"zl": 1 - zl}
    voc_peers = [(dl, dx, dc) for dl in range(2) for dx in range(4) for dc in range(2)][1:]

    barrier = pltpu.get_barrier_semaphore()
    greeted = [peer(*p) for p in voc_peers]
    greeted += [{"y": yat(dy)} for dy in (1, 2, 3, 5, 6, 7)] + [{"zh": zat(dz)} for dz in range(1, ZH)]
    parts = 4
    rows = D * K // parts
    loads = [pltpu.make_async_copy(hid_hbm, hid, local_sems.at[0])]
    for q in range(parts):
        span = pl.ds(q * rows, rows)
        loads.append(pltpu.make_async_copy(cp_hbm.at[span], cpraw.at[span], local_sems.at[1 + q]))
    small = [(mw_hbm, mw_ref), (ln_hbm, ln_ref), (tg_hbm, tg_ref), (loss_hbm, loss_ref), (w_hbm, w)]
    for i, (src, dst) in enumerate(small):
        loads.append(pltpu.make_async_copy(src, dst, local_sems.at[1 + parts + i]))
    for load in loads:
        load.start()
    for device in greeted:
        pl.semaphore_signal(barrier, inc=1, device_id=device, device_id_type=MESH)

    loads[0].wait()
    pre = jnp.zeros((T, K * E), F32)
    for q in range(parts):
        loads[1 + q].wait()
        stage[...] = cpraw[pl.ds(q * rows, rows), :].astype(F32)
        span = pl.ds(q * (D // parts), D // parts)
        for k in range(K):
            cp[span, lanes(k)] = stage[pl.ds(k, D // parts, stride=K), :].astype(BF)
        pre = pre + mm(hid[:, span], cp[span, :])
    acts = jnp.tanh(pre)

    def block(dl, dx, dc, k):
        at = (zl + dl) % 2 * 8 + xat(dx) * 2 + (c + dc) % 2
        return ctx.at[pl.ds(pl.multiple_of(at * E, E), E), lanes(k)]

    for k in range(K):
        ctx[pl.ds(pl.multiple_of(voc * E, E), E), lanes(k)] = acts[:, k * E : (k + 1) * E].T.astype(BF)

    pl.semaphore_wait(barrier, len(greeted))

    def push(dl, dx, k, role, device):
        net.send(block(dl, dx, 0, k), block(dl, dx, 0, k), role, device)

    for k in range(K):
        push(0, 0, k, ("ag", 1, 0, k), over)
        push(0, 0, k, ("ag", 0, -1, k), right)
        push(0, 0, k, ("ag", 0, 1, k), left)
        push(0, 0, k, ("ac", 0, 0, k), other)

    def piece(dx, dc):
        return pl.ds(pl.multiple_of((xat(dx) * 2 + (c + dc) % 2) * 16, 16), 16)

    for dz in (1, 3, 2):
        span = pl.ds(pl.multiple_of(zat(dz) * 512, 512), 512)
        net.send(hid.at[piece(0, 0), span], hx.at[dz, piece(0, 0)], ("hx", dz), {"zh": zat(dz)})
    hx[0] = hid[:, pl.ds(pl.multiple_of(zh * 512, 512), 512)]
    for i in range(len(small)):
        loads[1 + parts + i].wait()
    net.send(w.at[:, 1 - c], wp, ("wp",), other)
    mw = jnp.concatenate([mw_ref[...].astype(F32), jnp.zeros((4, E), F32)], axis=0)
    mix_part = mm_nt(mw.astype(BF), hid[:, pl.ds(pl.multiple_of(voc * E, E), E)])
    for j in range(16):
        wt[:, j * 128 : (j + 1) * 128] = w[j // 2, j % 2].T

    def from_side(dl, dx, k):
        net.got(block(dl, dx, 0, k), ("ag", dl, dx, k))
        if dl == 0 and (k % 2 == 0) == (dx == -1):
            push(dl, dx, k, ("ag", 0, 2, k), right if dx == -1 else left)
        push(dl, dx, k, ("ac", dl, dx, k), other)

    def from_far(dl, k):
        net.got(block(dl, 2, 0, k), ("ag", dl, 2, k))
        if dl == 0:
            push(0, 2, k, ("ag", 1, 2, k), over)
        push(dl, 2, k, ("ac", dl, 2, k), other)

    def add_chip(dl, dx):
        for k in range(K):
            net.got(block(dl, dx, 1, k), ("ac", dl, dx, k))
        span = pl.ds(pl.multiple_of(((zl + dl) % 2 * X + xat(dx)) * 256, 256), 256)
        part = mm(wt[:, span], ctx[span, :])
        eb[...] = part if (dl, dx) == (0, 0) else eb[...] + part

    for k in range(K):
        net.got(block(1, 0, 0, k), ("ag", 1, 0, k))
        push(1, 0, k, ("ag", 1, -1, k), right)
        push(1, 0, k, ("ag", 1, 1, k), left)
        push(1, 0, k, ("ac", 1, 0, k), other)
        from_side(0, -1, k)
        from_side(0, 1, k)
    for k, chip in zip(range(K), ((0, 0), (1, 0), (0, -1), (0, 1))):
        from_far(0, k)
        from_side(1, -1, k)
        from_side(1, 1, k)
        add_chip(*chip)
    for k, chip in zip(range(K), ((1, -1), (1, 1), (0, 2), (1, 2))):
        from_far(1, k)
        add_chip(*chip)
    ids = lax.broadcasted_iota(jnp.int32, (V, T), 0) + voc * V
    hit = ids == tg_ref[...]
    targets = [jnp.sum(jnp.where(hit, eb[:, lanes(k)], 0.0), axis=0, keepdims=True) for k in range(K)]
    arx[0] = jnp.concatenate([*targets, mix_part[:4]], axis=0)
    for i, p in enumerate(voc_peers):
        net.send(arx.at[0], arx.at[i + 1], ("ar", i), peer(*p))
    onehot = hit.astype(F32)
    for k in range(K):
        eb[:, lanes(k)] = jnp.exp(eb[:, lanes(k)] - ln_ref[k : k + 1, :]) - onehot
    for i in range(len(voc_peers)):
        net.got(arx.at[i + 1], ("ar", i))
    sums = jnp.sum(arx[...], axis=0)
    exp_mix = jnp.exp(sums[4:])
    weights = exp_mix / jnp.sum(exp_mix, axis=0, keepdims=True)
    joint = weights * jnp.exp(sums[:4] - ln_ref[...])
    posterior = joint / jnp.sum(joint, axis=0, keepdims=True)
    factor = loss_ref[...] * posterior
    mix_grad = loss_ref[...] * (weights - posterior)

    for k in range(K):
        lgt[:, lanes(k)] = (factor[k : k + 1] * eb[:, lanes(k)]).astype(BF)
        net.send(lgt.at[:, lanes(k)], lgp.at[:, lanes(k)], ("lg", k), other)

    for a in range(ZH):
        part = mm_nt(ctx[a * 512 : (a + 1) * 512, :], lgt[...])
        vgb[a] = part.astype(BF).reshape(Y, 64, V)

    def chain_send(way, half, dist):
        sign = 1 - 2 * way
        owner = yat(sign * dist)
        src = vgb.at[2 * half : 2 * half + 2, owner]
        if dist < (4 if half == way else 3):
            got = vrb.at[way, half, dist]
            net.got(got, ("vy", way, half, dist + 1))
            vsb[way, half, dist - 1] = (src[...].astype(F32) + got[...].astype(F32)).astype(BF)
            src = vsb.at[way, half, dist - 1]
        net.send(src, vrb.at[way, half, dist - 1], ("vy", way, half, dist), up if way == 0 else down)

    def chain_round(n):
        for half in range(2):
            for way in range(2):
                dist = (4 if half == way else 3) - n
                if dist > 0:
                    chain_send(way, half, dist)

    chain_round(0)

    net.got(wp, ("wp",))
    w_own = w[:, pl.ds(c, 1)].reshape(8 * E, V)
    for k in (0, 2):
        net.got(lgp.at[:, lanes(k)], ("lg", k))
        net.got(lgp.at[:, lanes(k + 1)], ("lg", k + 1))
        part = mm(w_own, lgt[:, lanes(k, 2)]) + mm(wp[...].reshape(8 * E, V), lgp[:, lanes(k, 2)])
        for j in (k, k + 1):
            cgb[j] = part[:, (j - k) * T : (j - k + 1) * T].astype(BF).reshape(ZL, X, E, T)
        for j in (k, k + 1):
            net.send(cgb.at[j, 1 - zl, xat(2)], zf.at[j], ("zf", j), over)
            net.send(cgb.at[j, 1 - zl, xat(1)], rmo.at[j], ("rmo", j), right)
            net.send(cgb.at[j, 1 - zl, xat(-1)], rpo.at[j], ("rpo", j), left)

    def both(a, b):
        return (a[...].astype(F32) + b[...].astype(F32)).astype(BF)

    def far(k):
        net.got(zf.at[k], ("zf", k))
        sf[k] = both(cgb.at[k, zl, xat(2)], zf.at[k])
        net.send(sf.at[k], r2.at[k], ("r2", k), left if k % 2 else right)

    def straight(k):
        if k % 2:
            net.send(cgb.at[k, zl, xat(1)], rxm.at[k], ("rm", k), right)
        else:
            net.send(cgb.at[k, zl, xat(-1)], rxp.at[k], ("rp", k), left)

    def combine(k):
        net.got(r2.at[k], ("r2", k))
        sp[k] = both(cgb.at[k, zl, xat(-1 if k % 2 else 1)], r2.at[k])
        if k % 2:
            net.send(sp.at[k], rxp.at[k], ("rp", k), left)
        else:
            net.send(sp.at[k], rxm.at[k], ("rm", k), right)

    def cross(k):
        net.got(rmo.at[k], ("rmo", k))
        net.got(rpo.at[k], ("rpo", k))
        zs[k] = (cgb[k, 1 - zl, x].astype(F32) + rmo[k].astype(F32) + rpo[k].astype(F32)).astype(BF)
        net.send(zs.at[k], zr.at[k], ("zr", k), over)

    far(0)
    far(1)
    straight(0)
    straight(1)
    far(2)
    far(3)
    straight(2)
    straight(3)
    cross(0)
    cross(1)
    combine(0)
    combine(1)
    cross(2)
    cross(3)
    combine(2)
    combine(3)
    chain_round(1)

    def pre_grads(k):
        net.got(rxm.at[k], ("rm", k))
        net.got(rxp.at[k], ("rp", k))
        net.got(zr.at[k], ("zr", k))
        own = ctx[pl.ds(pl.multiple_of(voc * E, E), E), lanes(k)].astype(F32)
        grad = cgb[k, zl, x].astype(F32) + rxm[k].astype(F32) + rxp[k].astype(F32) + zr[k].astype(F32)
        grad = (grad * (1.0 - own * own)).astype(BF)
        pgz[k, :, 0:T] = grad
        pgs[k * E : (k + 1) * E, :] = grad
        net.send(pgz.at[k, :, lanes(0)], pgz.at[k, :, lanes(1)], ("pz", 1, k), {"zh": zat(1)})
        net.send(pgz.at[k, :, lanes(0)], pgz.at[k, :, lanes(3)], ("pz", 3, k), {"zh": zat(3)})

    pre_grads(0)
    pre_grads(1)
    pre_grads(2)
    pre_grads(3)

    for dz in (1, 3, 2):
        net.got(hx.at[dz, piece(0, 0)], ("hx", dz))
    row_peers = [(dx, dc) for dx in (1, 3, 2, 0) for dc in range(2) if (dx, dc) != (0, 0)]
    for dx, dc in row_peers:
        at = {"x": xat(dx), "c": (c + dc) % 2}
        net.send(hx.at[1:4, piece(0, 0)], hx.at[1:4, piece(0, 0)], ("hy", (4 - dx) % 4, dc), at)

    for j in range(4):
        part = mm(cp[j * 512 : (j + 1) * 512, :], pgs[...])
        hpb[4 * j : 4 * j + 4] = part.astype(BF).reshape(4, 128, T)
    chain_round(2)

    for k in range(K):
        net.got(pgz.at[k, :, lanes(1)], ("pz", 1, k))
        if k % 2 == 0:
            net.send(pgz.at[k, :, lanes(1)], pgz.at[k, :, lanes(2)], ("pz", 2, k), {"zh": zat(1)})
        net.got(pgz.at[k, :, lanes(3)], ("pz", 3, k))
        if k % 2 == 1:
            net.send(pgz.at[k, :, lanes(3)], pgz.at[k, :, lanes(2)], ("pz", 2, k), {"zh": zat(3)})
    for i, p in enumerate(voc_peers):
        at = peer(*p)
        net.send(hpb.at[at["zl"] * 8 + at["x"] * 2 + at["c"]], hrx.at[i], ("hr", i), at)
    for dx, dc in row_peers:
        net.got(hx.at[1:4, piece(dx, dc)], ("hy", dx, dc))
    for dz in range(ZH):
        ht[:, lanes(dz)] = hx[dz].T

    def proj(k):
        for j in (k, k + 1):
            net.got(pgz.at[j, :, lanes(2)], ("pz", 2, j))
        part = mm_nt(ht[...], pgz[k : k + 2].reshape(2 * E, ZH * T))
        for j in (k, k + 1):
            pp[j] = part[:, (j - k) * E : (j - k + 1) * E].astype(BF).reshape(Y, 64, E)
        for j in (k, k + 1):
            sign, far_way, near_way = (-1, down, up) if j % 2 else (1, up, down)
            net.send(pp.at[j, yat(4 * sign)], pn.at[j, 0], ("pn", j, 0), far_way)
            net.send(pp.at[j, yat(2 * sign)], pn.at[j, 1], ("pn", j, 1), far_way)
            net.send(pp.at[j, yat(-3 * sign)], pn.at[j, 2], ("pn", j, 2), near_way)
            net.send(pp.at[j, yat(-sign)], prx.at[j, 3], ("py", j, 3), near_way)

    def proj_on(j):
        sign = -1 if j % 2 else 1
        for i, dist in enumerate((3 * sign, sign, -2 * sign)):
            net.got(pn.at[j, i], ("pn", j, i))
            pc[j, i] = both(pp.at[j, yat(dist)], pn.at[j, i])
            net.send(pc.at[j, i], prx.at[j, i], ("py", j, i), {"y": yat(dist)})

    proj(0)
    proj(2)
    chain_round(3)
    for k in range(K):
        proj_on(k)

    for half in range(2):
        span = slice(2 * half, 2 * half + 2)
        total = vgb[span, y].astype(F32)
        for way in range(2):
            net.got(vrb.at[way, half, 0], ("vy", way, half, 1))
            total = total + vrb[way, half, 0].astype(F32)
        vzs[span] = total.astype(BF)
    for dz in (1, 3, 2):
        net.send(vzs.at[zat(dz)], vzr.at[dz], ("vz", dz), {"zh": zat(dz)})

    for i in range(len(voc_peers)):
        net.got(hrx.at[i], ("hr", i))
    total = hpb[voc].astype(F32)
    for i in range(len(voc_peers)):
        total = total + hrx[i].astype(F32)
    mix_grad = jnp.concatenate([mix_grad, jnp.zeros((4, T), F32)], axis=0)
    mix_term = lax.dot_general(mix_grad, mw, TN, precision=lax.Precision.HIGHEST, preferred_element_type=F32)
    hg_ref[...] = (total.T + mix_term).astype(BF)

    for k in range(K):
        total = pp[k, y].astype(F32)
        for i in range(4):
            net.got(prx.at[k, i], ("py", k, i))
            total = total + prx[k, i].astype(F32)
        pst[pl.ds(k, 64, stride=K), :] = total
    pg_ref[...] = pst[...].astype(BF)

    total = vzs[zh].astype(F32)
    for dz in range(1, ZH):
        net.got(vzr.at[dz], ("vz", dz))
        total = total + vzr[dz].astype(F32)
    vg_ref[...] = total.astype(BF)
    net.finish()


def hand_over(*refs):
    for src, dst in zip(refs[:3], refs[3:]):
        dst[...] = src[...]


def body(hidden, mix_weight, comp_proj, vocab_weight, log_normalizer, targets, loss_grad):
    vmem = pl.BlockSpec(memory_space=pltpu.VMEM)
    hbm = pl.BlockSpec(memory_space=pl.ANY)
    scratch = [
        pltpu.VMEM(shape, dtype)
        for shape, dtype in (
            ((T, D), BF),
            ((D * K, E), BF),
            ((D, E), F32),
            ((D, K * E), BF),
            ((8, 2, 128, V), BF),
            ((V, D), BF),
            ((8, 128, V), BF),
            ((K, E), BF),
            ((K, T), F32),
            ((1, T), jnp.int32),
            ((1, T), F32),
            ((D, K * T), BF),
            ((V, K * T), F32),
            ((V, K * T), BF),
            ((V, K * T), BF),
            ((16, 8, T), F32),
            ((K, ZL, X, E, T), BF),
            *[((K, E, T), BF)] * 10,
            ((K, E, ZH * T), BF),
            ((K * E, T), BF),
            ((ZH, T, 512), BF),
            ((512, ZH * T), BF),
            ((K, Y, 64, E), BF),
            ((K, 3, 64, E), BF),
            ((K, 3, 64, E), BF),
            ((K, 4, 64, E), BF),
            ((64 * K, E), F32),
            ((16, 128, T), BF),
            ((15, 128, T), BF),
            ((ZH, Y, 64, V), BF),
            ((2, 2, 4, 2, 64, V), BF),
            ((2, 2, 4, 2, 64, V), BF),
            ((ZH, 64, V), BF),
            ((ZH, 64, V), BF),
        )
    ]
    scratch += [pltpu.SemaphoreType.DMA((N_SEND,)), pltpu.SemaphoreType.DMA((N_RECV,)), pltpu.SemaphoreType.DMA((10,))]
    shapes = (
        jax.ShapeDtypeStruct((T, E), BF),
        jax.ShapeDtypeStruct((64 * K, E), BF),
        jax.ShapeDtypeStruct((64, V), BF),
    )
    results = pl.pallas_call(
        kernel,
        out_shape=shapes,
        in_specs=[hbm] * 7,
        out_specs=(vmem, vmem, vmem),
        scratch_shapes=scratch,
        compiler_params=pltpu.CompilerParams(
            collective_id=0, has_side_effects=True, vmem_limit_bytes=56 * 1024 * 1024
        ),
    )(
        hidden,
        comp_proj.reshape(D * K, E),
        vocab_weight.reshape(8, 2, 128, V),
        mix_weight,
        log_normalizer,
        targets.reshape(1, T),
        loss_grad.reshape(1, T),
    )
    hidden_grad, proj_grad, vocab_grad = pl.pallas_call(
        hand_over, out_shape=shapes, in_specs=[vmem] * 3, out_specs=(vmem,) * 3
    )(*results)
    return hidden_grad, proj_grad.reshape(64, K, E), vocab_grad


def solution(mesh):
    split = Mesh(mesh.devices.reshape(ZH, Y, ZL, X, C), ("zh", "y", "zl", "x", "c"))
    tok, voc = ("zh", "y"), ("zl", "x", "c")
    in_specs = (P(tok, None), P(None, voc), P(None, None, voc), P(None, voc), P(None, tok), P(tok), P(tok))
    out_specs = (P(tok, voc), P(tok, None, voc), P(tok, voc))
    return jax.shard_map(body, mesh=split, in_specs=in_specs, out_specs=out_specs, check_vma=False)
```

```python
import math

import jax
import jax.numpy as jnp
from jax import lax
from jax.experimental import pallas as pl
from jax.experimental.pallas import tpu as pltpu
from jax.sharding import Mesh
from jax.sharding import PartitionSpec as P

MESH = pl.DeviceIdType.MESH
BF, F32 = jnp.bfloat16, jnp.float32
ZH, Y, ZL, X, C = 4, 8, 2, 4, 2
D, K, T, V, E = 2048, 4, 128, 256, 128
BULK = 2 * 1024 * 1024
N_SEND, N_RECV = 4, 102

NT = (((1,), (1,)), ((), ()))
TN = (((0,), (0,)), ((), ()))


def mm(a, b):
    return jnp.dot(a, b, preferred_element_type=F32)


def mm_nt(a, b):
    return lax.dot_general(a, b, NT, preferred_element_type=F32)


class Net:
    def __init__(self, send_sems, recv_sems, yard):
        self.send_sems, self.recv_sems, self.yard = send_sems, recv_sems, yard
        self.roles, self.bulk = {}, []

    def slot(self, role):
        return self.recv_sems.at[self.roles.setdefault(role, len(self.roles))]

    def copy(self, src, dst, role, device):
        return pltpu.make_async_remote_copy(
            src_ref=src,
            dst_ref=dst,
            send_sem=self.send_sems.at[max(len(self.bulk), 1) - 1],
            recv_sem=self.slot(role),
            device_id=device,
            device_id_type=MESH,
        )

    def send(self, src, dst, role, device):
        size = math.prod(src.shape) * src.dtype.itemsize
        if not self.bulk or self.bulk[-1] + size > BULK:
            self.bulk.append(0)
        self.bulk[-1] += size
        self.copy(src, dst, role, device).start()

    def got(self, dst, role):
        self.copy(dst, dst, role, {"c": 1 - lax.axis_index("c")}).wait_recv()

    def finish(self):
        for i, size in enumerate(self.bulk):
            sent = self.yard.at[pl.ds(0, size // (E * 2))]
            pltpu.make_async_copy(sent, sent, self.send_sems.at[i]).wait()


def kernel(
    hid_hbm, cp_hbm, w_hbm, mw_hbm, ln_hbm, tg_hbm, loss_hbm,
    hg_ref, pg_ref, vg_ref,
    hid, cpraw, stage, cp, w, wt, wp, mw_ref, ln_ref, tg_ref, loss_ref, ctx, eb, lgt, lgp, arx,
    cgb, zf, sf, r2, sp, zs, rx, ro, pgz, pgs, hx, ht, pp, pc, pn, prx, pst,
    hpb, hq, hs, hrx, hsum, hz, hzr, vgb, vsb, vrb, vzs, vzr,
    send_sems, recv_sems, local_sems,
):
    zh, y = lax.axis_index("zh"), lax.axis_index("y")
    zl, x, c = lax.axis_index("zl"), lax.axis_index("x"), lax.axis_index("c")
    voc = zl * 8 + x * 2 + c
    net = Net(send_sems, recv_sems, cpraw)

    def xat(dx):
        return lax.rem(x + dx + X, X)

    def yat(dy):
        return lax.rem(y + dy + Y, Y)

    def zat(dz):
        return lax.rem(zh + dz, ZH)

    def peer(dl, dx, dc):
        return {"zl": (zl + dl) % 2, "x": xat(dx), "c": (c + dc) % 2}

    def lanes(k, n=1):
        return pl.ds(k * T, n * T)

    right, left = {"x": xat(1)}, {"x": xat(-1)}
    up, down = {"y": yat(1)}, {"y": yat(-1)}
    other, over = {"c": 1 - c}, {"zl": 1 - zl}
    voc_peers = [(dl, dx, dc) for dl in range(2) for dx in range(4) for dc in range(2)][1:]

    barrier = pltpu.get_barrier_semaphore()
    greeted = [peer(*p) for p in voc_peers]
    greeted += [{"y": yat(dy)} for dy in (1, 2, 3, 5, 6, 7)] + [{"zh": zat(dz)} for dz in range(1, ZH)]
    parts = 4
    rows = D * K // parts
    loads = [pltpu.make_async_copy(hid_hbm, hid, local_sems.at[0])]
    for q in range(parts):
        span = pl.ds(q * rows, rows)
        loads.append(pltpu.make_async_copy(cp_hbm.at[span], cpraw.at[span], local_sems.at[1 + q]))
    small = [(mw_hbm, mw_ref), (ln_hbm, ln_ref), (tg_hbm, tg_ref), (loss_hbm, loss_ref), (w_hbm, w)]
    for i, (src, dst) in enumerate(small):
        loads.append(pltpu.make_async_copy(src, dst, local_sems.at[1 + parts + i]))
    for load in loads:
        load.start()
    for device in greeted:
        pl.semaphore_signal(barrier, inc=1, device_id=device, device_id_type=MESH)

    loads[0].wait()
    pre = jnp.zeros((T, K * E), F32)
    for q in range(parts):
        loads[1 + q].wait()
        stage[...] = cpraw[pl.ds(q * rows, rows), :].astype(F32)
        span = pl.ds(q * (D // parts), D // parts)
        for k in range(K):
            cp[span, lanes(k)] = stage[pl.ds(k, D // parts, stride=K), :].astype(BF)
        pre = pre + mm(hid[:, span], cp[span, :])
    acts = jnp.tanh(pre)

    def block(dl, dx, dc, k):
        at = (zl + dl) % 2 * 8 + xat(dx) * 2 + (c + dc) % 2
        return ctx.at[pl.ds(pl.multiple_of(at * E, E), E), lanes(k)]

    for k in range(K):
        ctx[pl.ds(pl.multiple_of(voc * E, E), E), lanes(k)] = acts[:, k * E : (k + 1) * E].T.astype(BF)

    pl.semaphore_wait(barrier, len(greeted))

    def push(dl, dx, k, role, device):
        net.send(block(dl, dx, 0, k), block(dl, dx, 0, k), role, device)

    for k, to_right, to_left in zip(range(K), (0, 2, 1, 3), (1, 3, 0, 2)):
        push(0, 0, to_right, ("ag", 0, -1, to_right), right)
        push(0, 0, to_left, ("ag", 0, 1, to_left), left)
        push(0, 0, k, ("ag", 1, 0, k), over)
        push(0, 0, k, ("ac", 0, 0), other)

    def piece(dx, dc):
        return pl.ds(pl.multiple_of((xat(dx) * 2 + (c + dc) % 2) * 16, 16), 16)

    for dz in (1, 3, 2):
        span = pl.ds(pl.multiple_of(zat(dz) * 512, 512), 512)
        net.send(hid.at[piece(0, 0), span], hx.at[dz, piece(0, 0)], ("hx",), {"zh": zat(dz)})
    hx[0] = hid[:, pl.ds(pl.multiple_of(zh * 512, 512), 512)]
    for i in range(len(small)):
        loads[1 + parts + i].wait()
    net.send(w.at[:, 1 - c], wp, ("wp",), other)
    mw = jnp.concatenate([mw_ref[...].astype(F32), jnp.zeros((4, E), F32)], axis=0)
    mix_part = mm_nt(mw.astype(BF), hid[:, pl.ds(pl.multiple_of(voc * E, E), E)])
    for j in range(16):
        wt[:, j * 128 : (j + 1) * 128] = w[j // 2, j % 2].T

    def from_side(dl, dx, k):
        net.got(block(dl, dx, 0, k), ("ag", dl, dx, k))
        if dl == 0 and (k % 2 == 0) == (dx == -1):
            push(dl, dx, k, ("ag", 0, 2, k), right if dx == -1 else left)
        push(dl, dx, k, ("ac", dl, dx), other)

    def from_far(dl, k):
        net.got(block(dl, 2, 0, k), ("ag", dl, 2, k))
        if dl == 0:
            push(0, 2, k, ("ag", 1, 2, k), over)
        push(dl, 2, k, ("ac", dl, 2), other)

    def add_chip(dl, dx):
        at = (zl + dl) % 2 * 8 + xat(dx) * 2 + 1 - c
        net.got(ctx.at[pl.ds(pl.multiple_of(at * E, E), E)], ("ac", dl, dx))
        span = pl.ds(pl.multiple_of(((zl + dl) % 2 * X + xat(dx)) * 256, 256), 256)
        part = mm(wt[:, span], ctx[span, :])
        eb[...] = part if (dl, dx) == (0, 0) else eb[...] + part

    for dx, k in ((-1, 0), (1, 1), (-1, 2), (1, 3)):
        from_side(0, dx, k)
    for k in range(K):
        net.got(block(1, 0, 0, k), ("ag", 1, 0, k))
        push(1, 0, k, ("ag", 1, -1, k), right)
        push(1, 0, k, ("ag", 1, 1, k), left)
        push(1, 0, k, ("ac", 1, 0), other)
    for dx, k in ((-1, 1), (1, 0), (-1, 3), (1, 2)):
        from_side(0, dx, k)
    add_chip(0, 0)
    for k in range(K):
        from_far(0, k)
    for k, chip in zip(range(K), ((1, 0), (0, -1), (0, 1), (0, 2))):
        from_side(1, -1, k)
        from_side(1, 1, k)
        add_chip(*chip)
    for k in range(K):
        from_far(1, k)
    for chip in ((1, -1), (1, 1), (1, 2)):
        add_chip(*chip)
    ids = lax.broadcasted_iota(jnp.int32, (V, T), 0) + voc * V
    hit = ids == tg_ref[...]
    targets = [jnp.sum(jnp.where(hit, eb[:, lanes(k)], 0.0), axis=0, keepdims=True) for k in range(K)]
    arx[0] = jnp.concatenate([*targets, mix_part[:4]], axis=0)
    for i, p in enumerate(voc_peers):
        net.send(arx.at[0], arx.at[i + 1], ("ar",), peer(*p))
    onehot = hit.astype(F32)
    for k in range(K):
        eb[:, lanes(k)] = jnp.exp(eb[:, lanes(k)] - ln_ref[k : k + 1, :]) - onehot
    net.got(arx.at[1:16], ("ar",))
    sums = jnp.sum(arx[...], axis=0)
    exp_mix = jnp.exp(sums[4:])
    weights = exp_mix / jnp.sum(exp_mix, axis=0, keepdims=True)
    joint = weights * jnp.exp(sums[:4] - ln_ref[...])
    posterior = joint / jnp.sum(joint, axis=0, keepdims=True)
    factor = loss_ref[...] * posterior
    mix_grad = loss_ref[...] * (weights - posterior)

    for k in range(K):
        lgt[:, lanes(k)] = (factor[k : k + 1] * eb[:, lanes(k)]).astype(BF)
        if k % 2:
            net.send(lgt.at[:, lanes(k - 1, 2)], lgp.at[:, lanes(k - 1, 2)], ("lg", k - 1), other)

    for a in range(ZH):
        part = mm_nt(ctx[a * 512 : (a + 1) * 512, :], lgt[...])
        vgb[a] = part.astype(BF).reshape(Y, 64, V)

    def chain_send(way, half, dist):
        sign = 1 - 2 * way
        owner = yat(sign * dist)
        src = vgb.at[2 * half : 2 * half + 2, owner]
        if dist < (4 if half == way else 3):
            got = vrb.at[way, half, dist]
            net.got(got, ("vy", way, half, dist + 1))
            vsb[way, half, dist - 1] = (src[...].astype(F32) + got[...].astype(F32)).astype(BF)
            src = vsb.at[way, half, dist - 1]
        net.send(src, vrb.at[way, half, dist - 1], ("vy", way, half, dist), up if way == 0 else down)

    def chain_round(n):
        for half in range(2):
            for way in range(2):
                dist = (4 if half == way else 3) - n
                if dist > 0:
                    chain_send(way, half, dist)

    chain_round(0)

    net.got(wp, ("wp",))
    w_own = w[:, pl.ds(c, 1)].reshape(8 * E, V)
    for k in (0, 2):
        net.got(lgp.at[:, lanes(k, 2)], ("lg", k))
        part = mm(w_own, lgt[:, lanes(k, 2)]) + mm(wp[...].reshape(8 * E, V), lgp[:, lanes(k, 2)])
        for j in (k, k + 1):
            cgb[j] = part[:, (j - k) * T : (j - k + 1) * T].astype(BF).reshape(ZL, X, E, T)
        for j in (k, k + 1):
            net.send(cgb.at[j, 1 - zl, xat(2)], zf.at[j], ("zf", j), over)
            net.send(cgb.at[j, 1 - zl, xat(1)], ro.at[j, 0], ("ro", j), right)
            net.send(cgb.at[j, 1 - zl, xat(-1)], ro.at[j, 1], ("ro", j), left)

    def both(a, b):
        return (a[...].astype(F32) + b[...].astype(F32)).astype(BF)

    def far(k):
        net.got(zf.at[k], ("zf", k))
        sf[k] = both(cgb.at[k, zl, xat(2)], zf.at[k])
        net.send(sf.at[k], r2.at[k], ("r2", k), left if k % 2 else right)

    def straight(k):
        if k % 2:
            net.send(cgb.at[k, zl, xat(1)], rx.at[k, 0], ("rx", k), right)
        else:
            net.send(cgb.at[k, zl, xat(-1)], rx.at[k, 1], ("rx", k), left)

    def combine(k):
        net.got(r2.at[k], ("r2", k))
        sp[k] = both(cgb.at[k, zl, xat(-1 if k % 2 else 1)], r2.at[k])
        if k % 2:
            net.send(sp.at[k], rx.at[k, 1], ("rx", k), left)
        else:
            net.send(sp.at[k], rx.at[k, 0], ("rx", k), right)

    def cross(k):
        net.got(ro.at[k], ("ro", k))
        zs[k] = (cgb[k, 1 - zl, x].astype(F32) + ro[k, 0].astype(F32) + ro[k, 1].astype(F32)).astype(BF)
        net.send(zs.at[k], rx.at[k, 2], ("rx", k), over)

    far(0)
    far(1)
    straight(0)
    straight(1)
    far(2)
    far(3)
    straight(2)
    straight(3)
    cross(0)
    cross(1)
    combine(0)
    combine(1)
    cross(2)
    cross(3)
    combine(2)
    combine(3)
    chain_round(1)

    def pre_grads(k):
        net.got(rx.at[k], ("rx", k))
        own = ctx[pl.ds(pl.multiple_of(voc * E, E), E), lanes(k)].astype(F32)
        grad = cgb[k, zl, x].astype(F32) + rx[k, 0].astype(F32) + rx[k, 1].astype(F32) + rx[k, 2].astype(F32)
        grad = (grad * (1.0 - own * own)).astype(BF)
        pgz[k, :, 0:T] = grad
        pgs[k * E : (k + 1) * E, :] = grad
        net.send(pgz.at[k, :, lanes(0)], pgz.at[k, :, lanes(1)], ("pz", 1, k), {"zh": zat(1)})
        net.send(pgz.at[k, :, lanes(0)], pgz.at[k, :, lanes(3)], ("pz", 3, k), {"zh": zat(3)})

    pre_grads(0)
    pre_grads(1)
    pre_grads(2)
    pre_grads(3)

    net.got(hx.at[1:4, piece(0, 0)], ("hx",))
    row_peers = [(dx, dc) for dx in (1, 3, 2, 0) for dc in range(2) if (dx, dc) != (0, 0)]
    for dx, dc in row_peers:
        at = {"x": xat(dx), "c": (c + dc) % 2}
        net.send(hx.at[1:4, piece(0, 0)], hx.at[1:4, piece(0, 0)], ("hy", (4 - dx) % 4, dc), at)

    for j in range(4):
        part = mm(cp[j * 512 : (j + 1) * 512, :], pgs[...])
        hpb[2 * j : 2 * j + 2] = part.astype(BF).reshape(2, 2, 128, T)
    net.send(hpb.at[:, 1 - c], hq, ("hq",), other)
    chain_round(2)

    def z_forward(k):
        net.got(pgz.at[k, :, lanes(1)], ("pz", 1, k))
        if k % 2 == 0:
            net.send(pgz.at[k, :, lanes(1)], pgz.at[k, :, lanes(2)], ("pz", 2, k), {"zh": zat(1)})
        net.got(pgz.at[k, :, lanes(3)], ("pz", 3, k))
        if k % 2 == 1:
            net.send(pgz.at[k, :, lanes(3)], pgz.at[k, :, lanes(2)], ("pz", 2, k), {"zh": zat(3)})

    net.got(hq, ("hq",))
    for j in range(8):
        hs[j // X, j % X] = both(hpb.at[j, c], hq.at[j])
    for dx in (1, 3, 2):
        net.send(hs.at[:, xat(dx)], hrx.at[dx - 1], ("hr",), {"x": xat(dx)})
    for k in range(K):
        z_forward(k)
    chain_round(3)
    for dx, dc in row_peers:
        net.got(hx.at[1:4, piece(dx, dc)], ("hy", dx, dc))
    for dz in range(ZH):
        ht[:, lanes(dz)] = hx[dz].T

    def proj(k):
        for j in (k, k + 1):
            net.got(pgz.at[j, :, lanes(2)], ("pz", 2, j))
        part = mm_nt(ht[...], pgz[k : k + 2].reshape(2 * E, ZH * T))
        for j in (k, k + 1):
            pp[j] = part[:, (j - k) * E : (j - k + 1) * E].astype(BF).reshape(Y, 64, E)
        for j in (k, k + 1):
            sign, far_way, near_way = (-1, down, up) if j % 2 else (1, up, down)
            net.send(pp.at[j, yat(4 * sign)], pn.at[j, 0], ("pn", j), far_way)
            net.send(pp.at[j, yat(2 * sign)], pn.at[j, 1], ("pn", j), far_way)
            net.send(pp.at[j, yat(-3 * sign)], pn.at[j, 2], ("pn", j), near_way)
            net.send(pp.at[j, yat(-sign)], prx.at[j, 3], ("py", j), near_way)

    def proj_on(j):
        sign = -1 if j % 2 else 1
        net.got(pn.at[j], ("pn", j))
        for i, dist in enumerate((3 * sign, sign, -2 * sign)):
            pc[j, i] = both(pp.at[j, yat(dist)], pn.at[j, i])
            net.send(pc.at[j, i], prx.at[j, i], ("py", j), {"y": yat(dist)})

    proj(0)
    proj(2)

    for half in range(2):
        span = slice(2 * half, 2 * half + 2)
        total = vgb[span, y].astype(F32)
        for way in range(2):
            net.got(vrb.at[way, half, 0], ("vy", way, half, 1))
            total = total + vrb[way, half, 0].astype(F32)
        vzs[span] = total.astype(BF)
    for dz in (1, 3, 2):
        net.send(vzs.at[zat(dz)], vzr.at[dz], ("vz",), {"zh": zat(dz)})
    for k in range(K):
        proj_on(k)
    net.got(hrx, ("hr",))
    hsum[...] = hs[:, x].astype(F32)
    for i in range(3):
        hsum[...] += hrx[i].astype(F32)
    hz[...] = hsum[1 - zl].astype(BF)
    net.send(hz, hzr, ("hz",), over)

    for k in range(K):
        net.got(prx.at[k], ("py", k))
        total = pp[k, y].astype(F32)
        for i in range(4):
            total = total + prx[k, i].astype(F32)
        pst[pl.ds(k, 64, stride=K), :] = total
    pg_ref[...] = pst[...].astype(BF)

    net.got(hzr, ("hz",))
    total = hsum[zl] + hzr[...].astype(F32)
    mix_grad = jnp.concatenate([mix_grad, jnp.zeros((4, T), F32)], axis=0)
    mix_term = lax.dot_general(mix_grad, mw, TN, precision=lax.Precision.HIGHEST, preferred_element_type=F32)
    hg_ref[...] = (total.T + mix_term).astype(BF)

    total = vzs[zh].astype(F32)
    net.got(vzr.at[1:4], ("vz",))
    for dz in range(1, ZH):
        total = total + vzr[dz].astype(F32)
    vg_ref[...] = total.astype(BF)
    net.finish()
    assert len(net.bulk) <= N_SEND and len(net.roles) <= N_RECV


def hand_over(*refs):
    for src, dst in zip(refs[:3], refs[3:]):
        dst[...] = src[...]


def body(hidden, mix_weight, comp_proj, vocab_weight, log_normalizer, targets, loss_grad):
    vmem = pl.BlockSpec(memory_space=pltpu.VMEM)
    hbm = pl.BlockSpec(memory_space=pl.ANY)
    scratch = [
        pltpu.VMEM(shape, dtype)
        for shape, dtype in (
            ((T, D), BF),
            ((D * K, E), BF),
            ((D, E), F32),
            ((D, K * E), BF),
            ((8, 2, 128, V), BF),
            ((V, D), BF),
            ((8, 128, V), BF),
            ((K, E), BF),
            ((K, T), F32),
            ((1, T), jnp.int32),
            ((1, T), F32),
            ((D, K * T), BF),
            ((V, K * T), F32),
            ((V, K * T), BF),
            ((V, K * T), BF),
            ((16, 8, T), F32),
            ((K, ZL, X, E, T), BF),
            *[((K, E, T), BF)] * 5,
            ((K, 3, E, T), BF),
            ((K, 2, E, T), BF),
            ((K, E, ZH * T), BF),
            ((K * E, T), BF),
            ((ZH, T, 512), BF),
            ((512, ZH * T), BF),
            ((K, Y, 64, E), BF),
            ((K, 3, 64, E), BF),
            ((K, 3, 64, E), BF),
            ((K, 4, 64, E), BF),
            ((64 * K, E), F32),
            ((8, 2, 128, T), BF),
            ((8, 128, T), BF),
            ((ZL, X, 128, T), BF),
            ((3, ZL, 128, T), BF),
            ((ZL, 128, T), F32),
            ((128, T), BF),
            ((128, T), BF),
            ((ZH, Y, 64, V), BF),
            ((2, 2, 4, 2, 64, V), BF),
            ((2, 2, 4, 2, 64, V), BF),
            ((ZH, 64, V), BF),
            ((ZH, 64, V), BF),
        )
    ]
    scratch += [pltpu.SemaphoreType.DMA((N_SEND,)), pltpu.SemaphoreType.DMA((N_RECV,)), pltpu.SemaphoreType.DMA((10,))]
    shapes = (
        jax.ShapeDtypeStruct((T, E), BF),
        jax.ShapeDtypeStruct((64 * K, E), BF),
        jax.ShapeDtypeStruct((64, V), BF),
    )
    results = pl.pallas_call(
        kernel,
        out_shape=shapes,
        in_specs=[hbm] * 7,
        out_specs=(vmem, vmem, vmem),
        scratch_shapes=scratch,
        compiler_params=pltpu.CompilerParams(
            collective_id=0, has_side_effects=True, vmem_limit_bytes=56 * 1024 * 1024
        ),
    )(
        hidden,
        comp_proj.reshape(D * K, E),
        vocab_weight.reshape(8, 2, 128, V),
        mix_weight,
        log_normalizer,
        targets.reshape(1, T),
        loss_grad.reshape(1, T),
    )
    hidden_grad, proj_grad, vocab_grad = pl.pallas_call(
        hand_over, out_shape=shapes, in_specs=[vmem] * 3, out_specs=(vmem,) * 3
    )(*results)
    return hidden_grad, proj_grad.reshape(64, K, E), vocab_grad


def solution(mesh):
    split = Mesh(mesh.devices.reshape(ZH, Y, ZL, X, C), ("zh", "y", "zl", "x", "c"))
    tok, voc = ("zh", "y"), ("zl", "x", "c")
    in_specs = (P(tok, None), P(None, voc), P(None, None, voc), P(None, voc), P(None, tok), P(tok), P(tok))
    out_specs = (P(tok, voc), P(tok, None, voc), P(tok, voc))
    return jax.shard_map(body, mesh=split, in_specs=in_specs, out_specs=out_specs, check_vma=False)
```

```python
import math

import jax
import jax.numpy as jnp
from jax import lax
from jax.experimental import pallas as pl
from jax.experimental.pallas import tpu as pltpu
from jax.sharding import Mesh
from jax.sharding import PartitionSpec as P

MESH = pl.DeviceIdType.MESH
BF, F32 = jnp.bfloat16, jnp.float32
ZH, Y, ZL, X, C = 4, 8, 2, 4, 2
D, K, T, V, E = 2048, 4, 128, 256, 128
SCALE = 2.0**-16
BULK = 2 * 1024 * 1024
N_SEND, N_RECV = 4, 102

NT = (((1,), (1,)), ((), ()))
TN = (((0,), (0,)), ((), ()))


def mm(a, b):
    return jnp.dot(a, b, preferred_element_type=F32)


def mm_nt(a, b):
    return lax.dot_general(a, b, NT, preferred_element_type=F32)


class Net:
    def __init__(self, send_sems, recv_sems, yard):
        self.send_sems, self.recv_sems, self.yard = send_sems, recv_sems, yard
        self.roles, self.bulk = {}, []

    def slot(self, role):
        return self.recv_sems.at[self.roles.setdefault(role, len(self.roles))]

    def copy(self, src, dst, role, device):
        return pltpu.make_async_remote_copy(
            src_ref=src,
            dst_ref=dst,
            send_sem=self.send_sems.at[max(len(self.bulk), 1) - 1],
            recv_sem=self.slot(role),
            device_id=device,
            device_id_type=MESH,
        )

    def send(self, src, dst, role, device):
        size = math.prod(src.shape) * src.dtype.itemsize
        if not self.bulk or self.bulk[-1] + size > BULK:
            self.bulk.append(0)
        self.bulk[-1] += size
        self.copy(src, dst, role, device).start()

    def got(self, dst, role):
        self.copy(dst, dst, role, {"c": 1 - lax.axis_index("c")}).wait_recv()

    def finish(self):
        for i, size in enumerate(self.bulk):
            sent = self.yard.at[pl.ds(0, size // (E * 2))]
            pltpu.make_async_copy(sent, sent, self.send_sems.at[i]).wait()


def kernel(
    hid_hbm, cp_hbm, w_hbm, mw_hbm, ln_hbm, tg_hbm, loss_hbm,
    hg_hbm, pg_hbm, vg_hbm,
    hid, cpraw, stage, cp, w, wt, wp, mw_ref, ln_ref, tg_ref, loss_ref, ctx, eb, lgt, lgu, lgp, arx,
    cgb, zf, sf, r2, sp, zs, rx, ro, pgz, pgs, hx, ht, pp, pc, pn, prx, pst,
    hpb, hq, hs, hrx, hsum, hz, hzr, vgb, vsb, vrb, vzs, vzr, hgo, pgo, vgo,
    send_sems, recv_sems, local_sems,
):
    zh, y = lax.axis_index("zh"), lax.axis_index("y")
    zl, x, c = lax.axis_index("zl"), lax.axis_index("x"), lax.axis_index("c")
    voc = zl * 8 + x * 2 + c
    net = Net(send_sems, recv_sems, cpraw)

    def xat(dx):
        return lax.rem(x + dx + X, X)

    def yat(dy):
        return lax.rem(y + dy + Y, Y)

    def zat(dz):
        return lax.rem(zh + dz, ZH)

    def peer(dl, dx, dc):
        return {"zl": (zl + dl) % 2, "x": xat(dx), "c": (c + dc) % 2}

    def lanes(k, n=1):
        return pl.ds(k * T, n * T)

    right, left = {"x": xat(1)}, {"x": xat(-1)}
    up, down = {"y": yat(1)}, {"y": yat(-1)}
    other, over = {"c": 1 - c}, {"zl": 1 - zl}
    voc_peers = [(dl, dx, dc) for dl in range(2) for dx in range(4) for dc in range(2)][1:]

    barrier = pltpu.get_barrier_semaphore()
    greeted = [peer(*p) for p in voc_peers]
    greeted += [{"y": yat(dy)} for dy in (1, 2, 3, 5, 6, 7)] + [{"zh": zat(dz)} for dz in range(1, ZH)]
    parts = 4
    rows = D * K // parts
    loads = [pltpu.make_async_copy(hid_hbm, hid, local_sems.at[0])]
    for q in range(parts):
        span = pl.ds(q * rows, rows)
        loads.append(pltpu.make_async_copy(cp_hbm.at[span], cpraw.at[span], local_sems.at[1 + q]))
    small = [(mw_hbm, mw_ref), (ln_hbm, ln_ref), (tg_hbm, tg_ref), (loss_hbm, loss_ref), (w_hbm, w)]
    for i, (src, dst) in enumerate(small):
        loads.append(pltpu.make_async_copy(src, dst, local_sems.at[1 + parts + i]))
    for load in loads:
        load.start()
    for device in greeted:
        pl.semaphore_signal(barrier, inc=1, device_id=device, device_id_type=MESH)

    loads[0].wait()
    pre = jnp.zeros((T, K * E), F32)
    for q in range(parts):
        loads[1 + q].wait()
        stage[...] = cpraw[pl.ds(q * rows, rows), :].astype(F32)
        span = pl.ds(q * (D // parts), D // parts)
        for k in range(K):
            cp[span, lanes(k)] = stage[pl.ds(k, D // parts, stride=K), :].astype(BF)
        pre = pre + mm(hid[:, span], cp[span, :])
    acts = jnp.tanh(pre)

    def block(dl, dx, dc, k):
        at = (zl + dl) % 2 * 8 + xat(dx) * 2 + (c + dc) % 2
        return ctx.at[pl.ds(pl.multiple_of(at * E, E), E), lanes(k)]

    for k in range(K):
        ctx[pl.ds(pl.multiple_of(voc * E, E), E), lanes(k)] = acts[:, k * E : (k + 1) * E].T.astype(BF)

    pl.semaphore_wait(barrier, len(greeted))

    def push(dl, dx, k, role, device):
        net.send(block(dl, dx, 0, k), block(dl, dx, 0, k), role, device)

    for k, to_right, to_left in zip(range(K), (0, 2, 1, 3), (1, 3, 0, 2)):
        push(0, 0, to_right, ("ag", 0, -1, to_right), right)
        push(0, 0, to_left, ("ag", 0, 1, to_left), left)
        push(0, 0, k, ("ag", 1, 0, k), over)
        push(0, 0, k, ("ac", 0, 0), other)

    def piece(dx, dc):
        return pl.ds(pl.multiple_of((xat(dx) * 2 + (c + dc) % 2) * 16, 16), 16)

    for dz in (1, 3, 2):
        span = pl.ds(pl.multiple_of(zat(dz) * 512, 512), 512)
        net.send(hid.at[piece(0, 0), span], hx.at[dz, piece(0, 0)], ("hx",), {"zh": zat(dz)})
    hx[0] = hid[:, pl.ds(pl.multiple_of(zh * 512, 512), 512)]
    for i in range(len(small)):
        loads[1 + parts + i].wait()
    net.send(w.at[:, 1 - c], wp, ("wp",), other)
    mw = jnp.concatenate([mw_ref[...].astype(F32), jnp.zeros((4, E), F32)], axis=0)
    mix_part = mm_nt(mw.astype(BF), hid[:, pl.ds(pl.multiple_of(voc * E, E), E)])
    for j in range(16):
        wt[:, j * 128 : (j + 1) * 128] = w[j // 2, j % 2].T

    def from_side(dl, dx, k):
        net.got(block(dl, dx, 0, k), ("ag", dl, dx, k))
        if dl == 0 and (k % 2 == 0) == (dx == -1):
            push(dl, dx, k, ("ag", 0, 2, k), right if dx == -1 else left)
        push(dl, dx, k, ("ac", dl, dx), other)

    def from_far(dl, k):
        net.got(block(dl, 2, 0, k), ("ag", dl, 2, k))
        if dl == 0:
            push(0, 2, k, ("ag", 1, 2, k), over)
        push(dl, 2, k, ("ac", dl, 2), other)

    def add_chip(dl, dx):
        at = (zl + dl) % 2 * 8 + xat(dx) * 2 + 1 - c
        net.got(ctx.at[pl.ds(pl.multiple_of(at * E, E), E)], ("ac", dl, dx))
        span = pl.ds(pl.multiple_of(((zl + dl) % 2 * X + xat(dx)) * 256, 256), 256)
        part = mm(wt[:, span], ctx[span, :])
        eb[...] = part if (dl, dx) == (0, 0) else eb[...] + part

    for dx, k in ((-1, 0), (1, 1), (-1, 2), (1, 3)):
        from_side(0, dx, k)
    for k in range(K):
        net.got(block(1, 0, 0, k), ("ag", 1, 0, k))
        push(1, 0, k, ("ag", 1, -1, k), right)
        push(1, 0, k, ("ag", 1, 1, k), left)
        push(1, 0, k, ("ac", 1, 0), other)
    for dx, k in ((-1, 1), (1, 0), (-1, 3), (1, 2)):
        from_side(0, dx, k)
    add_chip(0, 0)
    for k in range(K):
        from_far(0, k)
    for k, chip in zip(range(K), ((1, 0), (0, -1), (0, 1), (0, 2))):
        from_side(1, -1, k)
        from_side(1, 1, k)
        add_chip(*chip)
    for k in range(K):
        from_far(1, k)
    for chip in ((1, -1), (1, 1), (1, 2)):
        add_chip(*chip)
    ids = lax.broadcasted_iota(jnp.int32, (V, T), 0) + voc * V
    hit = ids == tg_ref[...]
    targets = [jnp.sum(jnp.where(hit, eb[:, lanes(k)], 0.0), axis=0, keepdims=True) for k in range(K)]
    onehot = hit.astype(F32)
    for k in range(K):
        grad = jnp.exp(eb[:, lanes(k)] - ln_ref[k : k + 1, :]) - onehot
        eb[:, lanes(k)] = grad
        lgu[:, lanes(k)] = (grad * SCALE).astype(BF)
        if k % 2:
            net.send(lgu.at[:, lanes(k - 1, 2)], lgp.at[:, lanes(k - 1, 2)], ("lg", k - 1), other)
    arx[0] = jnp.concatenate([*targets, mix_part[:4]], axis=0)
    for i, p in enumerate(voc_peers):
        net.send(arx.at[0], arx.at[i + 1], ("ar",), peer(*p))

    net.got(wp, ("wp",))
    w_own = w[:, pl.ds(c, 1)].reshape(8 * E, V)
    w_partner = wp[...].reshape(8 * E, V)
    for k in (0, 2):
        part = mm(w_own, lgu[:, lanes(k, 2)])
        net.got(lgp.at[:, lanes(k, 2)], ("lg", k))
        part = part + mm(w_partner, lgp[:, lanes(k, 2)])
        for j in (k, k + 1):
            cgb[j] = part[:, (j - k) * T : (j - k + 1) * T].astype(BF).reshape(ZL, X, E, T)
        for j in (k, k + 1):
            net.send(cgb.at[j, 1 - zl, xat(2)], zf.at[j], ("zf", j), over)
            net.send(cgb.at[j, 1 - zl, xat(1)], ro.at[j, 0], ("ro", j), right)
            net.send(cgb.at[j, 1 - zl, xat(-1)], ro.at[j, 1], ("ro", j), left)

    net.got(arx.at[1:16], ("ar",))
    sums = jnp.sum(arx[...], axis=0)
    exp_mix = jnp.exp(sums[4:])
    weights = exp_mix / jnp.sum(exp_mix, axis=0, keepdims=True)
    joint = weights * jnp.exp(sums[:4] - ln_ref[...])
    posterior = joint / jnp.sum(joint, axis=0, keepdims=True)
    factor = loss_ref[...] * posterior
    mix_grad = loss_ref[...] * (weights - posterior)

    for k in range(K):
        lgt[:, lanes(k)] = (factor[k : k + 1] * eb[:, lanes(k)]).astype(BF)
    factor = factor * (1.0 / SCALE)

    for a in range(ZH):
        part = mm_nt(ctx[a * 512 : (a + 1) * 512, :], lgt[...])
        vgb[a] = part.astype(BF).reshape(Y, 64, V)

    def chain_send(way, half, dist):
        sign = 1 - 2 * way
        owner = yat(sign * dist)
        src = vgb.at[2 * half : 2 * half + 2, owner]
        if dist < (4 if half == way else 3):
            got = vrb.at[way, half, dist]
            net.got(got, ("vy", way, half, dist + 1))
            vsb[way, half, dist - 1] = (src[...].astype(F32) + got[...].astype(F32)).astype(BF)
            src = vsb.at[way, half, dist - 1]
        net.send(src, vrb.at[way, half, dist - 1], ("vy", way, half, dist), up if way == 0 else down)

    def chain_round(n):
        for half in range(2):
            for way in range(2):
                dist = (4 if half == way else 3) - n
                if dist > 0:
                    chain_send(way, half, dist)

    chain_round(0)

    def both(a, b):
        return (a[...].astype(F32) + b[...].astype(F32)).astype(BF)

    def far(k):
        net.got(zf.at[k], ("zf", k))
        sf[k] = both(cgb.at[k, zl, xat(2)], zf.at[k])
        net.send(sf.at[k], r2.at[k], ("r2", k), left if k % 2 else right)

    def straight(k):
        if k % 2:
            net.send(cgb.at[k, zl, xat(1)], rx.at[k, 0], ("rx", k), right)
        else:
            net.send(cgb.at[k, zl, xat(-1)], rx.at[k, 1], ("rx", k), left)

    def combine(k):
        net.got(r2.at[k], ("r2", k))
        sp[k] = both(cgb.at[k, zl, xat(-1 if k % 2 else 1)], r2.at[k])
        if k % 2:
            net.send(sp.at[k], rx.at[k, 1], ("rx", k), left)
        else:
            net.send(sp.at[k], rx.at[k, 0], ("rx", k), right)

    def cross(k):
        net.got(ro.at[k], ("ro", k))
        zs[k] = (cgb[k, 1 - zl, x].astype(F32) + ro[k, 0].astype(F32) + ro[k, 1].astype(F32)).astype(BF)
        net.send(zs.at[k], rx.at[k, 2], ("rx", k), over)

    far(0)
    far(1)
    straight(0)
    straight(1)
    far(2)
    far(3)
    straight(2)
    straight(3)
    cross(0)
    cross(1)
    combine(0)
    combine(1)
    cross(2)
    cross(3)
    combine(2)
    combine(3)
    chain_round(1)

    def pre_grads(k):
        net.got(rx.at[k], ("rx", k))
        own = ctx[pl.ds(pl.multiple_of(voc * E, E), E), lanes(k)].astype(F32)
        grad = cgb[k, zl, x].astype(F32) + rx[k, 0].astype(F32) + rx[k, 1].astype(F32) + rx[k, 2].astype(F32)
        grad = (grad * factor[k : k + 1] * (1.0 - own * own)).astype(BF)
        pgz[k, :, 0:T] = grad
        pgs[k * E : (k + 1) * E, :] = grad
        net.send(pgz.at[k, :, lanes(0)], pgz.at[k, :, lanes(1)], ("pz", 1, k), {"zh": zat(1)})
        net.send(pgz.at[k, :, lanes(0)], pgz.at[k, :, lanes(3)], ("pz", 3, k), {"zh": zat(3)})

    pre_grads(0)
    pre_grads(1)
    pre_grads(2)
    pre_grads(3)

    net.got(hx.at[1:4, piece(0, 0)], ("hx",))
    row_peers = [(dx, dc) for dx in (1, 3, 2, 0) for dc in range(2) if (dx, dc) != (0, 0)]
    for dx, dc in row_peers:
        at = {"x": xat(dx), "c": (c + dc) % 2}
        net.send(hx.at[1:4, piece(0, 0)], hx.at[1:4, piece(0, 0)], ("hy", (4 - dx) % 4, dc), at)

    for j in range(4):
        part = mm(cp[j * 512 : (j + 1) * 512, :], pgs[...])
        hpb[2 * j : 2 * j + 2] = part.astype(BF).reshape(2, 2, 128, T)
    net.send(hpb.at[:, 1 - c], hq, ("hq",), other)
    chain_round(2)

    def z_forward(k):
        net.got(pgz.at[k, :, lanes(1)], ("pz", 1, k))
        if k % 2 == 0:
            net.send(pgz.at[k, :, lanes(1)], pgz.at[k, :, lanes(2)], ("pz", 2, k), {"zh": zat(1)})
        net.got(pgz.at[k, :, lanes(3)], ("pz", 3, k))
        if k % 2 == 1:
            net.send(pgz.at[k, :, lanes(3)], pgz.at[k, :, lanes(2)], ("pz", 2, k), {"zh": zat(3)})

    net.got(hq, ("hq",))
    for j in range(8):
        hs[j // X, j % X] = both(hpb.at[j, c], hq.at[j])
    for dx in (1, 3, 2):
        net.send(hs.at[:, xat(dx)], hrx.at[dx - 1], ("hr",), {"x": xat(dx)})
    for k in range(K):
        z_forward(k)
    chain_round(3)
    for dx, dc in row_peers:
        net.got(hx.at[1:4, piece(dx, dc)], ("hy", dx, dc))
    for dz in range(ZH):
        ht[:, lanes(dz)] = hx[dz].T

    def proj(k):
        for j in (k, k + 1):
            net.got(pgz.at[j, :, lanes(2)], ("pz", 2, j))
        part = mm_nt(ht[...], pgz[k : k + 2].reshape(2 * E, ZH * T))
        for j in (k, k + 1):
            pp[j] = part[:, (j - k) * E : (j - k + 1) * E].astype(BF).reshape(Y, 64, E)
        for j in (k, k + 1):
            sign, far_way, near_way = (-1, down, up) if j % 2 else (1, up, down)
            net.send(pp.at[j, yat(4 * sign)], pn.at[j, 0], ("pn", j), far_way)
            net.send(pp.at[j, yat(2 * sign)], pn.at[j, 1], ("pn", j), far_way)
            net.send(pp.at[j, yat(-3 * sign)], pn.at[j, 2], ("pn", j), near_way)
            net.send(pp.at[j, yat(-sign)], prx.at[j, 3], ("py", j), near_way)

    def proj_on(j):
        sign = -1 if j % 2 else 1
        net.got(pn.at[j], ("pn", j))
        for i, dist in enumerate((3 * sign, sign, -2 * sign)):
            pc[j, i] = both(pp.at[j, yat(dist)], pn.at[j, i])
            net.send(pc.at[j, i], prx.at[j, i], ("py", j), {"y": yat(dist)})

    proj(0)
    proj(2)

    outs = []

    def put_out(src, dst):
        outs.append(pltpu.make_async_copy(src, dst, local_sems.at[10 + len(outs)]))
        outs[-1].start()

    for half in range(2):
        span = slice(2 * half, 2 * half + 2)
        total = vgb[span, y].astype(F32)
        for way in range(2):
            net.got(vrb.at[way, half, 0], ("vy", way, half, 1))
            total = total + vrb[way, half, 0].astype(F32)
        vzs[span] = total.astype(BF)
    for dz in (1, 3, 2):
        net.send(vzs.at[zat(dz)], vzr.at[dz], ("vz",), {"zh": zat(dz)})
    for k in range(K):
        proj_on(k)
    net.got(hrx, ("hr",))
    hsum[...] = hs[:, x].astype(F32)
    for i in range(3):
        hsum[...] += hrx[i].astype(F32)
    hz[...] = hsum[1 - zl].astype(BF)
    net.send(hz, hzr, ("hz",), over)

    for k in range(K):
        net.got(prx.at[k], ("py", k))
        total = pp[k, y].astype(F32)
        for i in range(4):
            total = total + prx[k, i].astype(F32)
        pst[pl.ds(k, 64, stride=K), :] = total
    pgo[...] = pst[...].astype(BF)
    put_out(pgo, pg_hbm)

    net.got(hzr, ("hz",))
    total = hsum[zl] + hzr[...].astype(F32)
    mix_grad = jnp.concatenate([mix_grad, jnp.zeros((4, T), F32)], axis=0)
    mix_term = lax.dot_general(mix_grad, mw, TN, precision=lax.Precision.HIGHEST, preferred_element_type=F32)
    hgo[...] = (total.T + mix_term).astype(BF)
    put_out(hgo, hg_hbm)

    total = vzs[zh].astype(F32)
    net.got(vzr.at[1:4], ("vz",))
    for dz in range(1, ZH):
        total = total + vzr[dz].astype(F32)
    vgo[...] = total.astype(BF)
    put_out(vgo, vg_hbm)
    for copy in outs:
        copy.wait()
    net.finish()
    assert len(net.bulk) <= N_SEND and len(net.roles) <= N_RECV


def hand_over(*refs):
    for src, dst in zip(refs[:3], refs[3:]):
        dst[...] = src[...]


def body(hidden, mix_weight, comp_proj, vocab_weight, log_normalizer, targets, loss_grad):
    hbm, vmem = (pl.BlockSpec(memory_space=m) for m in (pl.ANY, pltpu.VMEM))
    scratch = [
        pltpu.VMEM(shape, dtype)
        for shape, dtype in (
            ((T, D), BF),
            ((D * K, E), BF),
            ((D, E), F32),
            ((D, K * E), BF),
            ((8, 2, 128, V), BF),
            ((V, D), BF),
            ((8, 128, V), BF),
            ((K, E), BF),
            ((K, T), F32),
            ((1, T), jnp.int32),
            ((1, T), F32),
            ((D, K * T), BF),
            ((V, K * T), F32),
            ((V, K * T), BF),
            ((V, K * T), BF),
            ((V, K * T), BF),
            ((16, 8, T), F32),
            ((K, ZL, X, E, T), BF),
            *[((K, E, T), BF)] * 5,
            ((K, 3, E, T), BF),
            ((K, 2, E, T), BF),
            ((K, E, ZH * T), BF),
            ((K * E, T), BF),
            ((ZH, T, 512), BF),
            ((512, ZH * T), BF),
            ((K, Y, 64, E), BF),
            ((K, 3, 64, E), BF),
            ((K, 3, 64, E), BF),
            ((K, 4, 64, E), BF),
            ((64 * K, E), F32),
            ((8, 2, 128, T), BF),
            ((8, 128, T), BF),
            ((ZL, X, 128, T), BF),
            ((3, ZL, 128, T), BF),
            ((ZL, 128, T), F32),
            ((128, T), BF),
            ((128, T), BF),
            ((ZH, Y, 64, V), BF),
            ((2, 2, 4, 2, 64, V), BF),
            ((2, 2, 4, 2, 64, V), BF),
            ((ZH, 64, V), BF),
            ((ZH, 64, V), BF),
            ((T, E), BF),
            ((64 * K, E), BF),
            ((64, V), BF),
        )
    ]
    scratch += [pltpu.SemaphoreType.DMA((N_SEND,)), pltpu.SemaphoreType.DMA((N_RECV,)), pltpu.SemaphoreType.DMA((13,))]
    shapes = (
        jax.ShapeDtypeStruct((T, E), BF),
        jax.ShapeDtypeStruct((64 * K, E), BF),
        jax.ShapeDtypeStruct((64, V), BF),
    )
    results = pl.pallas_call(
        kernel,
        out_shape=shapes,
        in_specs=[hbm] * 7,
        out_specs=(hbm,) * 3,
        scratch_shapes=scratch,
        compiler_params=pltpu.CompilerParams(
            collective_id=0, has_side_effects=True, vmem_limit_bytes=56 * 1024 * 1024
        ),
    )(
        hidden,
        comp_proj.reshape(D * K, E),
        vocab_weight.reshape(8, 2, 128, V),
        mix_weight,
        log_normalizer,
        targets.reshape(1, T),
        loss_grad.reshape(1, T),
    )
    hidden_grad, proj_grad, vocab_grad = pl.pallas_call(
        hand_over, out_shape=shapes, in_specs=[vmem] * 3, out_specs=(vmem,) * 3
    )(*results)
    return hidden_grad, proj_grad.reshape(64, K, E), vocab_grad


def solution(mesh):
    split = Mesh(mesh.devices.reshape(ZH, Y, ZL, X, C), ("zh", "y", "zl", "x", "c"))
    tok, voc = ("zh", "y"), ("zl", "x", "c")
    in_specs = (P(tok, None), P(None, voc), P(None, None, voc), P(None, voc), P(None, tok), P(tok), P(tok))
    out_specs = (P(tok, voc), P(tok, None, voc), P(tok, voc))
    return jax.shard_map(body, mesh=split, in_specs=in_specs, out_specs=out_specs, check_vma=False)
```

```python
import math

import jax
import jax.numpy as jnp
from jax import lax
from jax.experimental import pallas as pl
from jax.experimental.pallas import tpu as pltpu
from jax.sharding import Mesh
from jax.sharding import PartitionSpec as P

MESH = pl.DeviceIdType.MESH
BF, F32 = jnp.bfloat16, jnp.float32
ZH, Y, ZL, X, C = 4, 8, 2, 4, 2
D, K, T, V, E = 2048, 4, 128, 256, 128
SCALE = 2.0**-16
BULK = 2 * 1024 * 1024
N_SEND, N_RECV = 4, 102

NT = (((1,), (1,)), ((), ()))
TN = (((0,), (0,)), ((), ()))


def mm(a, b):
    return jnp.dot(a, b, preferred_element_type=F32)


def mm_nt(a, b):
    return lax.dot_general(a, b, NT, preferred_element_type=F32)


class Net:
    def __init__(self, send_sems, recv_sems, yard):
        self.send_sems, self.recv_sems, self.yard = send_sems, recv_sems, yard
        self.roles, self.bulk = {}, []

    def slot(self, role):
        return self.recv_sems.at[self.roles.setdefault(role, len(self.roles))]

    def copy(self, src, dst, role, device):
        return pltpu.make_async_remote_copy(
            src_ref=src,
            dst_ref=dst,
            send_sem=self.send_sems.at[max(len(self.bulk), 1) - 1],
            recv_sem=self.slot(role),
            device_id=device,
            device_id_type=MESH,
        )

    def send(self, src, dst, role, device):
        size = math.prod(src.shape) * src.dtype.itemsize
        if not self.bulk or self.bulk[-1] + size > BULK:
            self.bulk.append(0)
        self.bulk[-1] += size
        self.copy(src, dst, role, device).start()

    def got(self, dst, role):
        self.copy(dst, dst, role, {"c": 1 - lax.axis_index("c")}).wait_recv()

    def finish(self):
        for i, size in enumerate(self.bulk):
            sent = self.yard.at[pl.ds(0, size // (E * 2))]
            pltpu.make_async_copy(sent, sent, self.send_sems.at[i]).wait()


def kernel(
    hid_hbm, cp_hbm, w_hbm, mw_hbm, ln_hbm, tg_hbm, loss_hbm,
    hg_ref, pg_ref, vg_ref,
    hid, cpraw, stage, cp, w, wt, wp, mw_ref, ln_ref, tg_ref, loss_ref, ctx, eb, lgt, lgu, lgp, arx,
    cgb, zf, sf, r2, sp, zs, rx, ro, pgz, pgs, hx, ht, pp, pc, pn, prx, pst,
    hpb, hq, hs, hrx, hsum, hz, hzr, vgb, vsb, vrb, vzs, vzr,
    send_sems, recv_sems, local_sems,
):
    zh, y = lax.axis_index("zh"), lax.axis_index("y")
    zl, x, c = lax.axis_index("zl"), lax.axis_index("x"), lax.axis_index("c")
    voc = zl * 8 + x * 2 + c
    net = Net(send_sems, recv_sems, cpraw)

    def xat(dx):
        return lax.rem(x + dx + X, X)

    def yat(dy):
        return lax.rem(y + dy + Y, Y)

    def zat(dz):
        return lax.rem(zh + dz, ZH)

    def peer(dl, dx, dc):
        return {"zl": (zl + dl) % 2, "x": xat(dx), "c": (c + dc) % 2}

    def lanes(k, n=1):
        return pl.ds(k * T, n * T)

    right, left = {"x": xat(1)}, {"x": xat(-1)}
    up, down = {"y": yat(1)}, {"y": yat(-1)}
    other, over = {"c": 1 - c}, {"zl": 1 - zl}
    voc_peers = [(dl, dx, dc) for dl in range(2) for dx in range(4) for dc in range(2)][1:]

    barrier = pltpu.get_barrier_semaphore()
    greeted = [peer(*p) for p in voc_peers]
    greeted += [{"y": yat(dy)} for dy in (1, 2, 3, 5, 6, 7)] + [{"zh": zat(dz)} for dz in range(1, ZH)]
    parts = 4
    rows = D * K // parts
    loads = [pltpu.make_async_copy(hid_hbm, hid, local_sems.at[0])]
    for q in range(parts):
        span = pl.ds(q * rows, rows)
        loads.append(pltpu.make_async_copy(cp_hbm.at[span], cpraw.at[span], local_sems.at[1 + q]))
    small = [(mw_hbm, mw_ref), (ln_hbm, ln_ref), (tg_hbm, tg_ref), (loss_hbm, loss_ref), (w_hbm, w)]
    for i, (src, dst) in enumerate(small):
        loads.append(pltpu.make_async_copy(src, dst, local_sems.at[1 + parts + i]))
    for i in (1, 0, *range(2, len(loads))):
        loads[i].start()
    for device in greeted:
        pl.semaphore_signal(barrier, inc=1, device_id=device, device_id_type=MESH)

    pre = jnp.zeros((T, K * E), F32)
    for q in range(parts):
        loads[1 + q].wait()
        stage[...] = cpraw[pl.ds(q * rows, rows), :].astype(F32)
        span = pl.ds(q * (D // parts), D // parts)
        for k in range(K):
            cp[span, lanes(k)] = stage[pl.ds(k, D // parts, stride=K), :].astype(BF)
        if q == 0:
            loads[0].wait()
        pre = pre + mm(hid[:, span], cp[span, :])
    acts = jnp.tanh(pre)

    def block(dl, dx, dc, k):
        at = (zl + dl) % 2 * 8 + xat(dx) * 2 + (c + dc) % 2
        return ctx.at[pl.ds(pl.multiple_of(at * E, E), E), lanes(k)]

    for k in range(K):
        ctx[pl.ds(pl.multiple_of(voc * E, E), E), lanes(k)] = acts[:, k * E : (k + 1) * E].T.astype(BF)

    pl.semaphore_wait(barrier, len(greeted))

    def push(dl, dx, k, role, device):
        net.send(block(dl, dx, 0, k), block(dl, dx, 0, k), role, device)

    for k, to_right, to_left in zip(range(K), (0, 2, 1, 3), (1, 3, 0, 2)):
        push(0, 0, to_right, ("ag", 0, -1, to_right), right)
        push(0, 0, to_left, ("ag", 0, 1, to_left), left)
        push(0, 0, k, ("ag", 1, 0, k), over)
        push(0, 0, k, ("ac", 0, 0), other)

    def piece(dx, dc):
        return pl.ds(pl.multiple_of((xat(dx) * 2 + (c + dc) % 2) * 16, 16), 16)

    for dz in (1, 3, 2):
        span = pl.ds(pl.multiple_of(zat(dz) * 512, 512), 512)
        net.send(hid.at[piece(0, 0), span], hx.at[dz, piece(0, 0)], ("hx",), {"zh": zat(dz)})
    hx[0] = hid[:, pl.ds(pl.multiple_of(zh * 512, 512), 512)]
    for i in range(len(small)):
        loads[1 + parts + i].wait()
    net.send(w.at[:, 1 - c], wp, ("wp",), other)
    mw = jnp.concatenate([mw_ref[...].astype(F32), jnp.zeros((4, E), F32)], axis=0)
    mix_part = mm_nt(mw.astype(BF), hid[:, pl.ds(pl.multiple_of(voc * E, E), E)])
    for j in range(16):
        wt[:, j * 128 : (j + 1) * 128] = w[j // 2, j % 2].T

    def from_side(dx, k):
        net.got(block(0, dx, 0, k), ("ag", 0, dx, k))
        if (k % 2 == 0) == (dx == -1):
            push(0, dx, k, ("ag", 0, 2, k), right if dx == -1 else left)
        push(0, dx, k, ("ac", 0, dx), other)

    def from_corner(dx):
        at = (1 - zl) * 8 + xat(dx) * 2 + c
        whole = ctx.at[pl.ds(pl.multiple_of(at * E, E), E)]
        net.got(whole, ("ag", 1, dx))
        net.send(whole, whole, ("ac", 1, dx), other)

    def from_far(dl, k):
        net.got(block(dl, 2, 0, k), ("ag", dl, 2, k))
        if dl == 0:
            push(0, 2, k, ("ag", 1, 2, k), over)
        push(dl, 2, k, ("ac", dl, 2), other)

    def add_chip(dl, dx):
        at = (zl + dl) % 2 * 8 + xat(dx) * 2 + 1 - c
        net.got(ctx.at[pl.ds(pl.multiple_of(at * E, E), E)], ("ac", dl, dx))
        span = pl.ds(pl.multiple_of(((zl + dl) % 2 * X + xat(dx)) * 256, 256), 256)
        part = mm(wt[:, span], ctx[span, :])
        eb[...] = part if (dl, dx) == (0, 0) else eb[...] + part

    for dx, k in ((-1, 0), (1, 1), (-1, 2), (1, 3)):
        from_side(dx, k)
    for k in range(K):
        net.got(block(1, 0, 0, k), ("ag", 1, 0, k))
        push(1, 0, k, ("ag", 1, -1), right)
        push(1, 0, k, ("ag", 1, 1), left)
        push(1, 0, k, ("ac", 1, 0), other)
    for dx, k in ((-1, 1), (1, 0), (-1, 3), (1, 2)):
        from_side(dx, k)
    add_chip(0, 0)
    for k in range(K):
        from_far(0, k)
    for chip in ((1, 0), (0, -1), (0, 1), (0, 2)):
        add_chip(*chip)
    from_corner(-1)
    from_corner(1)
    for k in range(K):
        from_far(1, k)
    for chip in ((1, -1), (1, 1), (1, 2)):
        add_chip(*chip)
    ids = lax.broadcasted_iota(jnp.int32, (V, T), 0) + voc * V
    hit = ids == tg_ref[...]
    targets = [jnp.sum(jnp.where(hit, eb[:, lanes(k)], 0.0), axis=0, keepdims=True) for k in range(K)]
    onehot = hit.astype(F32)
    for k in range(K):
        grad = jnp.exp(eb[:, lanes(k)] - ln_ref[k : k + 1, :]) - onehot
        eb[:, lanes(k)] = grad
        lgu[:, lanes(k)] = (grad * SCALE).astype(BF)
        if k % 2:
            net.send(lgu.at[:, lanes(k - 1, 2)], lgp.at[:, lanes(k - 1, 2)], ("lg", k - 1), other)
    arx[0] = jnp.concatenate([*targets, mix_part[:4]], axis=0)
    for i, p in enumerate(voc_peers):
        net.send(arx.at[0], arx.at[i + 1], ("ar",), peer(*p))

    net.got(wp, ("wp",))
    w_own = w[:, pl.ds(c, 1)].reshape(8 * E, V)
    w_partner = wp[...].reshape(8 * E, V)
    for k in (0, 2):
        part = mm(w_own, lgu[:, lanes(k, 2)])
        net.got(lgp.at[:, lanes(k, 2)], ("lg", k))
        part = part + mm(w_partner, lgp[:, lanes(k, 2)])
        for j in (k, k + 1):
            cgb[j] = part[:, (j - k) * T : (j - k + 1) * T].astype(BF).reshape(ZL, X, E, T)
        for j in (k, k + 1):
            net.send(cgb.at[j, 1 - zl, xat(2)], zf.at[j], ("zf", j), over)
            net.send(cgb.at[j, 1 - zl, xat(1)], ro.at[j, 0], ("ro", j), right)
            net.send(cgb.at[j, 1 - zl, xat(-1)], ro.at[j, 1], ("ro", j), left)

    def both(a, b):
        return (a[...].astype(F32) + b[...].astype(F32)).astype(BF)

    def far(k):
        net.got(zf.at[k], ("zf", k))
        sf[k] = both(cgb.at[k, zl, xat(2)], zf.at[k])
        net.send(sf.at[k], r2.at[k], ("r2", k), left if k % 2 else right)

    def straight(k):
        if k % 2:
            net.send(cgb.at[k, zl, xat(1)], rx.at[k, 0], ("rx", k), right)
        else:
            net.send(cgb.at[k, zl, xat(-1)], rx.at[k, 1], ("rx", k), left)

    def combine(k):
        net.got(r2.at[k], ("r2", k))
        sp[k] = both(cgb.at[k, zl, xat(-1 if k % 2 else 1)], r2.at[k])
        if k % 2:
            net.send(sp.at[k], rx.at[k, 1], ("rx", k), left)
        else:
            net.send(sp.at[k], rx.at[k, 0], ("rx", k), right)

    def cross(k):
        net.got(ro.at[k], ("ro", k))
        zs[k] = (cgb[k, 1 - zl, x].astype(F32) + ro[k, 0].astype(F32) + ro[k, 1].astype(F32)).astype(BF)
        net.send(zs.at[k], rx.at[k, 2], ("rx", k), over)

    far(0)
    far(1)
    straight(0)
    straight(1)
    net.got(arx.at[1:16], ("ar",))
    sums = jnp.sum(arx[...], axis=0)
    exp_mix = jnp.exp(sums[4:])
    weights = exp_mix / jnp.sum(exp_mix, axis=0, keepdims=True)
    joint = weights * jnp.exp(sums[:4] - ln_ref[...])
    posterior = joint / jnp.sum(joint, axis=0, keepdims=True)
    factor = loss_ref[...] * posterior
    mix_grad = loss_ref[...] * (weights - posterior)

    for k in range(K):
        lgt[:, lanes(k)] = (factor[k : k + 1] * eb[:, lanes(k)]).astype(BF)
    factor = factor * (1.0 / SCALE)

    for a in range(ZH):
        part = mm_nt(ctx[a * 512 : (a + 1) * 512, :], lgt[...])
        vgb[a] = part.astype(BF).reshape(Y, 64, V)

    def chain_send(way, half, dist):
        sign = 1 - 2 * way
        owner = yat(sign * dist)
        src = vgb.at[2 * half : 2 * half + 2, owner]
        if dist < (4 if half == way else 3):
            got = vrb.at[way, half, dist]
            net.got(got, ("vy", way, half, dist + 1))
            vsb[way, half, dist - 1] = (src[...].astype(F32) + got[...].astype(F32)).astype(BF)
            src = vsb.at[way, half, dist - 1]
        net.send(src, vrb.at[way, half, dist - 1], ("vy", way, half, dist), up if way == 0 else down)

    def chain_round(n):
        for half in range(2):
            for way in range(2):
                dist = (4 if half == way else 3) - n
                if dist > 0:
                    chain_send(way, half, dist)

    chain_round(0)

    far(2)
    far(3)
    straight(2)
    straight(3)
    cross(0)
    cross(1)
    combine(0)
    combine(1)
    cross(2)
    cross(3)
    combine(2)
    combine(3)
    def pre_grads(k):
        net.got(rx.at[k], ("rx", k))
        own = ctx[pl.ds(pl.multiple_of(voc * E, E), E), lanes(k)].astype(F32)
        grad = cgb[k, zl, x].astype(F32) + rx[k, 0].astype(F32) + rx[k, 1].astype(F32) + rx[k, 2].astype(F32)
        grad = (grad * factor[k : k + 1] * (1.0 - own * own)).astype(BF)
        pgz[k, :, 0:T] = grad
        pgs[k * E : (k + 1) * E, :] = grad
        net.send(pgz.at[k, :, lanes(0)], pgz.at[k, :, lanes(1)], ("pz", 1, k), {"zh": zat(1)})
        net.send(pgz.at[k, :, lanes(0)], pgz.at[k, :, lanes(3)], ("pz", 3, k), {"zh": zat(3)})

    net.got(hx.at[1:4, piece(0, 0)], ("hx",))

    def pass_hidden(dx, role, device):
        net.send(hx.at[1:4, piece(dx, 0)], hx.at[1:4, piece(dx, 0)], role, device)

    for dx in (1, 3, 2):
        pass_hidden(0, ("hy", 4 - dx), {"x": xat(dx)})
    pass_hidden(0, ("hc", 0), other)
    chain_round(1)
    pre_grads(0)
    pre_grads(1)
    pre_grads(2)
    pre_grads(3)

    for j in range(4):
        part = mm(cp[j * 512 : (j + 1) * 512, :], pgs[...])
        hpb[2 * j : 2 * j + 2] = part.astype(BF).reshape(2, 2, 128, T)
    net.send(hpb.at[:, 1 - c], hq, ("hq",), other)
    def z_forward(k):
        net.got(pgz.at[k, :, lanes(1)], ("pz", 1, k))
        if k % 2 == 0:
            net.send(pgz.at[k, :, lanes(1)], pgz.at[k, :, lanes(2)], ("pz", 2, k), {"zh": zat(1)})
        net.got(pgz.at[k, :, lanes(3)], ("pz", 3, k))
        if k % 2 == 1:
            net.send(pgz.at[k, :, lanes(3)], pgz.at[k, :, lanes(2)], ("pz", 2, k), {"zh": zat(3)})

    net.got(hq, ("hq",))
    for j in range(8):
        hs[j // X, j % X] = both(hpb.at[j, c], hq.at[j])
    for dx in (1, 3, 2):
        net.send(hs.at[:, xat(dx)], hrx.at[dx - 1], ("hr",), {"x": xat(dx)})
    for dx in (1, 3, 2):
        net.got(hx.at[1:4, piece(dx, 0)], ("hy", dx))
        pass_hidden(dx, ("hc", dx), other)
    z_forward(0)
    z_forward(1)
    chain_round(2)
    z_forward(2)
    z_forward(3)
    for dx in range(X):
        net.got(hx.at[1:4, piece(dx, 1)], ("hc", dx))
    for dz in range(ZH):
        ht[:, lanes(dz)] = hx[dz].T

    chain_round(3)
    def proj(k):
        for j in (k, k + 1):
            net.got(pgz.at[j, :, lanes(2)], ("pz", 2, j))
        part = mm_nt(ht[...], pgz[k : k + 2].reshape(2 * E, ZH * T))
        for j in (k, k + 1):
            pp[j] = part[:, (j - k) * E : (j - k + 1) * E].astype(BF).reshape(Y, 64, E)
        for j in (k, k + 1):
            sign, far_way, near_way = (-1, down, up) if j % 2 else (1, up, down)
            net.send(pp.at[j, yat(4 * sign)], pn.at[j, 0], ("pn", j), far_way)
            net.send(pp.at[j, yat(2 * sign)], pn.at[j, 1], ("pn", j), far_way)
            net.send(pp.at[j, yat(-3 * sign)], pn.at[j, 2], ("pn", j), near_way)
            net.send(pp.at[j, yat(-sign)], prx.at[j, 3], ("py", j), near_way)

    def proj_on(j):
        sign = -1 if j % 2 else 1
        net.got(pn.at[j], ("pn", j))
        for i, dist in enumerate((3 * sign, sign, -2 * sign)):
            pc[j, i] = both(pp.at[j, yat(dist)], pn.at[j, i])
            net.send(pc.at[j, i], prx.at[j, i], ("py", j), {"y": yat(dist)})

    proj(0)
    proj(2)

    for half in range(2):
        span = slice(2 * half, 2 * half + 2)
        total = vgb[span, y].astype(F32)
        for way in range(2):
            net.got(vrb.at[way, half, 0], ("vy", way, half, 1))
            total = total + vrb[way, half, 0].astype(F32)
        vzs[span] = total.astype(BF)
    for dz in (1, 3, 2):
        net.send(vzs.at[zat(dz)], vzr.at[dz], ("vz",), {"zh": zat(dz)})
    net.got(hrx, ("hr",))
    hsum[...] = hs[:, x].astype(F32)
    for i in range(3):
        hsum[...] += hrx[i].astype(F32)
    hz[...] = hsum[1 - zl].astype(BF)
    net.send(hz, hzr, ("hz",), over)
    for k in range(K):
        proj_on(k)

    for k in range(K):
        net.got(prx.at[k], ("py", k))
        total = pp[k, y].astype(F32)
        for i in range(4):
            total = total + prx[k, i].astype(F32)
        pst[pl.ds(k, 64, stride=K), :] = total
    pg_ref[...] = pst[...].astype(BF)

    net.got(hzr, ("hz",))
    total = hsum[zl] + hzr[...].astype(F32)
    mix_grad = jnp.concatenate([mix_grad, jnp.zeros((4, T), F32)], axis=0)
    mix_term = lax.dot_general(mix_grad, mw, TN, precision=lax.Precision.HIGHEST, preferred_element_type=F32)
    hg_ref[...] = (total.T + mix_term).astype(BF)

    total = vzs[zh].astype(F32)
    net.got(vzr.at[1:4], ("vz",))
    for dz in range(1, ZH):
        total = total + vzr[dz].astype(F32)
    vg_ref[...] = total.astype(BF)
    net.finish()
    assert len(net.bulk) <= N_SEND and len(net.roles) <= N_RECV


def hand_over(*refs):
    copies = [pltpu.make_async_copy(refs[i], refs[3 + i], refs[6].at[i]) for i in range(3)]
    for copy in copies:
        copy.start()
    for copy in copies:
        copy.wait()


def body(hidden, mix_weight, comp_proj, vocab_weight, log_normalizer, targets, loss_grad):
    hbm, vmem = (pl.BlockSpec(memory_space=m) for m in (pl.ANY, pltpu.VMEM))
    scratch = [
        pltpu.VMEM(shape, dtype)
        for shape, dtype in (
            ((T, D), BF),
            ((D * K, E), BF),
            ((D, E), F32),
            ((D, K * E), BF),
            ((8, 2, 128, V), BF),
            ((V, D), BF),
            ((8, 128, V), BF),
            ((K, E), BF),
            ((K, T), F32),
            ((1, T), jnp.int32),
            ((1, T), F32),
            ((D, K * T), BF),
            ((V, K * T), F32),
            ((V, K * T), BF),
            ((V, K * T), BF),
            ((V, K * T), BF),
            ((16, 8, T), F32),
            ((K, ZL, X, E, T), BF),
            *[((K, E, T), BF)] * 5,
            ((K, 3, E, T), BF),
            ((K, 2, E, T), BF),
            ((K, E, ZH * T), BF),
            ((K * E, T), BF),
            ((ZH, T, 512), BF),
            ((512, ZH * T), BF),
            ((K, Y, 64, E), BF),
            ((K, 3, 64, E), BF),
            ((K, 3, 64, E), BF),
            ((K, 4, 64, E), BF),
            ((64 * K, E), F32),
            ((8, 2, 128, T), BF),
            ((8, 128, T), BF),
            ((ZL, X, 128, T), BF),
            ((3, ZL, 128, T), BF),
            ((ZL, 128, T), F32),
            ((128, T), BF),
            ((128, T), BF),
            ((ZH, Y, 64, V), BF),
            ((2, 2, 4, 2, 64, V), BF),
            ((2, 2, 4, 2, 64, V), BF),
            ((ZH, 64, V), BF),
            ((ZH, 64, V), BF),
        )
    ]
    scratch += [pltpu.SemaphoreType.DMA((N_SEND,)), pltpu.SemaphoreType.DMA((N_RECV,)), pltpu.SemaphoreType.DMA((10,))]
    shapes = (
        jax.ShapeDtypeStruct((T, E), BF),
        jax.ShapeDtypeStruct((64 * K, E), BF),
        jax.ShapeDtypeStruct((64, V), BF),
    )
    results = pl.pallas_call(
        kernel,
        out_shape=tuple(pltpu.VMEM(s.shape, s.dtype) for s in shapes),
        in_specs=[hbm] * 7,
        out_specs=(vmem,) * 3,
        scratch_shapes=scratch,
        compiler_params=pltpu.CompilerParams(
            collective_id=0, has_side_effects=True, vmem_limit_bytes=56 * 1024 * 1024
        ),
    )(
        hidden,
        comp_proj.reshape(D * K, E),
        vocab_weight.reshape(8, 2, 128, V),
        mix_weight,
        log_normalizer,
        targets.reshape(1, T),
        loss_grad.reshape(1, T),
    )
    hidden_grad, proj_grad, vocab_grad = pl.pallas_call(
        hand_over,
        out_shape=shapes,
        in_specs=[vmem] * 3,
        out_specs=(hbm,) * 3,
        scratch_shapes=[pltpu.SemaphoreType.DMA((3,))],
    )(*[pltpu.with_memory_space_constraint(r, pltpu.VMEM) for r in results])
    return hidden_grad, proj_grad.reshape(64, K, E), vocab_grad


def solution(mesh):
    split = Mesh(mesh.devices.reshape(ZH, Y, ZL, X, C), ("zh", "y", "zl", "x", "c"))
    tok, voc = ("zh", "y"), ("zl", "x", "c")
    in_specs = (P(tok, None), P(None, voc), P(None, None, voc), P(None, voc), P(None, tok), P(tok), P(tok))
    out_specs = (P(tok, voc), P(tok, None, voc), P(tok, voc))
    return jax.shard_map(body, mesh=split, in_specs=in_specs, out_specs=out_specs, check_vma=False)
```

```python
import math

import jax
import jax.numpy as jnp
from jax import lax
from jax.experimental import pallas as pl
from jax.experimental.pallas import tpu as pltpu
from jax.sharding import Mesh
from jax.sharding import PartitionSpec as P

MESH = pl.DeviceIdType.MESH
BF, F32 = jnp.bfloat16, jnp.float32
ZH, Y, ZL, X, C = 4, 8, 2, 4, 2
D, K, T, V, E = 2048, 4, 128, 256, 128
SCALE = 2.0**-16
BULK = 2 * 1024 * 1024
N_SEND, N_RECV = 5, 129

NT = (((1,), (1,)), ((), ()))
TN = (((0,), (0,)), ((), ()))


def mm(a, b):
    return jnp.dot(a, b, preferred_element_type=F32)


def mm_nt(a, b):
    return lax.dot_general(a, b, NT, preferred_element_type=F32)


class Net:
    def __init__(self, send_sems, recv_sems, yard):
        self.send_sems, self.recv_sems, self.yard = send_sems, recv_sems, yard
        self.roles, self.bulk = {}, []

    def slot(self, role):
        return self.recv_sems.at[self.roles.setdefault(role, len(self.roles))]

    def copy(self, src, dst, role, device):
        return pltpu.make_async_remote_copy(
            src_ref=src,
            dst_ref=dst,
            send_sem=self.send_sems.at[max(len(self.bulk), 1) - 1],
            recv_sem=self.slot(role),
            device_id=device,
            device_id_type=MESH,
        )

    def send(self, src, dst, role, device):
        size = math.prod(src.shape) * src.dtype.itemsize
        if not self.bulk or self.bulk[-1] + size > BULK:
            self.bulk.append(0)
        self.bulk[-1] += size
        self.copy(src, dst, role, device).start()

    def got(self, dst, role):
        self.copy(dst, dst, role, {"c": 1 - lax.axis_index("c")}).wait_recv()

    def finish(self):
        for i, size in enumerate(self.bulk):
            sent = self.yard.at[pl.ds(0, size // (E * 2))]
            pltpu.make_async_copy(sent, sent, self.send_sems.at[i]).wait()


def kernel(
    hid_hbm, cp_hbm, w_hbm, mw_hbm, ln_hbm, tg_hbm, loss_hbm,
    hg_ref, pg_ref, vg_ref,
    hid, cpraw, stage, cp, w, wt, mw_ref, ln_ref, tg_ref, loss_ref, mixb, mixs, ctx, eb, lgt, lgu, arx, sumb, sumr,
    cgb, zf, sf, r2, sp, zs, rx, ro, pgz, pgs, hx, ht, pp, pc, pn, prx, pst, pgo, pgr,
    hpb, hq, hs, hrx, hsum, hz, hzr, vgb, vsb, vrb, vzs, vzr, vgo, vgr,
    send_sems, recv_sems, local_sems,
):
    zh, y = lax.axis_index("zh"), lax.axis_index("y")
    zl, x, c = lax.axis_index("zl"), lax.axis_index("x"), lax.axis_index("c")
    chip = zl * X + x
    voc = chip * 2 + c
    net = Net(send_sems, recv_sems, cpraw)

    def xat(dx):
        return lax.rem(x + dx + X, X)

    def yat(dy):
        return lax.rem(y + dy + Y, Y)

    def zat(dz):
        return lax.rem(zh + dz, ZH)

    def lanes(k, n=1):
        return pl.ds(k * T, n * T)

    right, left = {"x": xat(1)}, {"x": xat(-1)}
    up, down = {"y": yat(1)}, {"y": yat(-1)}
    other, over = {"c": 1 - c}, {"zl": 1 - zl}
    chips = [(dl, dx) for dl in range(2) for dx in range(4)][1:]

    barrier = pltpu.get_barrier_semaphore()
    greeted = [{"zl": (zl + dl) % 2, "x": xat(dx)} for dl, dx in chips] + [other]
    greeted += [{"y": yat(dy)} for dy in (1, 2, 3, 5, 6, 7)] + [{"zh": zat(dz)} for dz in range(1, ZH)]
    parts = 4
    rows = D * K // parts
    loads = [pltpu.make_async_copy(hid_hbm, hid, local_sems.at[0])]
    for q in range(parts):
        span = pl.ds(q * rows, rows)
        loads.append(pltpu.make_async_copy(cp_hbm.at[span], cpraw.at[span], local_sems.at[1 + q]))
    small = [(mw_hbm, mw_ref), (ln_hbm, ln_ref), (tg_hbm, tg_ref), (loss_hbm, loss_ref)]
    small += [(w_hbm, w.at[:, pl.ds(pl.multiple_of(c * V, V), V)])]
    for i, (src, dst) in enumerate(small):
        loads.append(pltpu.make_async_copy(src, dst, local_sems.at[1 + parts + i]))
    for i in (1, 0, *range(2, len(loads))):
        loads[i].start()
    for device in greeted:
        pl.semaphore_signal(barrier, inc=1, device_id=device, device_id_type=MESH)

    pre = jnp.zeros((T, K * E), F32)
    for q in range(parts):
        loads[1 + q].wait()
        stage[...] = cpraw[pl.ds(q * rows, rows), :].astype(F32)
        span = pl.ds(q * (D // parts), D // parts)
        for k in range(K):
            cp[span, lanes(k)] = stage[pl.ds(k, D // parts, stride=K), :].astype(BF)
        if q == 0:
            loads[0].wait()
        pre = pre + mm(hid[:, span], cp[span, :])
    acts = jnp.tanh(pre)
    for k in range(K):
        ctx[pl.ds(pl.multiple_of(voc * E, E), E), lanes(k)] = acts[:, k * E : (k + 1) * E].T.astype(BF)

    pl.semaphore_wait(barrier, len(greeted))

    def chip_at(dl, dx):
        return (zl + dl) % 2 * X + xat(dx)

    def block(dl, dx, half, k):
        at = chip_at(dl, dx) * 256 + half * E
        return ctx.at[pl.ds(pl.multiple_of(at, E), E), lanes(k)]

    def half_of(dl, dx, half):
        return ctx.at[pl.ds(pl.multiple_of(chip_at(dl, dx) * 256 + half * E, E), E)]

    def whole(dl, dx):
        return ctx.at[pl.ds(pl.multiple_of(chip_at(dl, dx) * 256, 256), 256)]

    def push(dl, dx, half, k, role, device):
        net.send(block(dl, dx, half, k), block(dl, dx, half, k), role, device)

    def small_loads():
        for i in range(len(small)):
            loads[1 + parts + i].wait()

    def mixing():
        mw = jnp.concatenate([mw_ref[...].astype(F32), jnp.zeros((4, E), F32)], axis=0)
        return mw, mm_nt(mw.astype(BF), hid[:, pl.ds(pl.multiple_of(voc * E, E), E)])

    def turn(start):
        for j in range(16):
            wt[start : start + V, j * 128 : (j + 1) * 128] = w[j * 128 : (j + 1) * 128, start : start + V].T

    def add_chip(dl, dx, n):
        span = pl.ds(pl.multiple_of(chip_at(dl, dx) * 256, 256), 256)
        eb[0:n] += mm(wt[0:n, span], ctx[span, :])

    def add_row(n):
        span = pl.ds(pl.multiple_of(zl * 1024, 1024), 1024)
        eb[0:n] = mm(wt[0:n, span], ctx[span, :])

    def hits(n):
        return (lax.broadcasted_iota(jnp.int32, (n, T), 0) + chip * 512) == tg_ref[...]

    def shares(sums):
        exp_mix = jnp.exp(sums[4:])
        weights = exp_mix / jnp.sum(exp_mix, axis=0, keepdims=True)
        joint = weights * jnp.exp(sums[:4] - ln_ref[...])
        posterior = joint / jnp.sum(joint, axis=0, keepdims=True)
        return loss_ref[...] * posterior, loss_ref[...] * (weights - posterior)

    def both(a, b):
        return (a[...].astype(F32) + b[...].astype(F32)).astype(BF)

    def scaled(factor, start):
        for k in range(K):
            lgt[start : start + V, lanes(k)] = (factor[k : k + 1] * eb[start : start + V, lanes(k)]).astype(BF)

    def vocab(ids):
        for a in range(ZH):
            part = mm_nt(ctx[a * 512 : (a + 1) * 512, :], lgt[ids * V : (ids + 1) * V])
            vgb[ids, a] = part.astype(BF).reshape(Y, 64, V)
        chain_part(ids, 0)

    def chain_send(ids, way, half, dist):
        sign = 1 - 2 * way
        owner = yat(sign * dist)
        src = vgb.at[ids, 2 * half : 2 * half + 2, owner]
        if dist < (4 if half == way else 3):
            got = vrb.at[ids, way, half, dist]
            net.got(got, ("vy", ids, way, half, dist + 1))
            vsb[ids, way, half, dist - 1] = both(src, got)
            src = vsb.at[ids, way, half, dist - 1]
        there = vrb.at[ids, way, half, dist - 1]
        net.send(src, there, ("vy", ids, way, half, dist), up if way == 0 else down)

    def chain_part(ids, n):
        for half in range(2):
            for way in range(2):
                dist = (4 if half == way else 3) - n
                if dist > 0:
                    chain_send(ids, way, half, dist)

    def chain_round(n):
        for ids in range(2):
            chain_part(ids, n)

    def chain_end():
        for ids in range(2):
            for half in range(2):
                span = slice(2 * half, 2 * half + 2)
                total = vgb[ids, span, y].astype(F32)
                for way in range(2):
                    net.got(vrb.at[ids, way, half, 0], ("vy", ids, way, half, 1))
                    total = total + vrb[ids, way, half, 0].astype(F32)
                vzs[ids, span] = total.astype(BF)
            for dz in (2, 1, 3):
                net.send(vzs.at[ids, zat(dz)], vzr.at[ids, dz], ("vz", ids), {"zh": zat(dz)})

    def vocab_out():
        for ids in (1, 0):
            total = vzs[ids, zh].astype(F32)
            net.got(vzr.at[ids, 1:4], ("vz", ids))
            for dz in range(1, ZH):
                total = total + vzr[ids, dz].astype(F32)
            if ids:
                vgo[...] = total.astype(BF)
                net.send(vgo, vgr, ("vgr",), other)
            else:
                vg_ref[...] = total.astype(BF)

    def hidden_part():
        for j in range(4):
            part = mm(cp[j * 512 : (j + 1) * 512, :], pgs[...])
            hpb[2 * j : 2 * j + 2] = part.astype(BF).reshape(2, 2, 128, T)
        net.send(hpb.at[:, 1 - c], hq, ("hq",), other)

    def hidden_x():
        net.got(hq, ("hq",))
        for j in range(8):
            hs[j // X, j % X] = both(hpb.at[j, c], hq.at[j])
        for dx in (1, 3, 2):
            net.send(hs.at[:, xat(dx)], hrx.at[dx - 1], ("hr",), {"x": xat(dx)})

    def hidden_z():
        net.got(hrx, ("hr",))
        hsum[...] = hs[:, x].astype(F32)
        for i in range(3):
            hsum[...] += hrx[i].astype(F32)
        hz[...] = hsum[1 - zl].astype(BF)
        net.send(hz, hzr, ("hz",), over)

    def hidden_out(mix_grad, mw):
        net.got(hzr, ("hz",))
        total = hsum[zl] + hzr[...].astype(F32)
        mix_grad = jnp.concatenate([mix_grad, jnp.zeros((4, T), F32)], axis=0)
        mix_term = lax.dot_general(mix_grad, mw, TN, precision=lax.Precision.HIGHEST, preferred_element_type=F32)
        hg_ref[...] = (total.T + mix_term).astype(BF)

    def leader():
        for k, to_right, to_left in zip(range(K), (0, 2, 1, 3), (1, 3, 0, 2)):
            push(0, 0, 1, to_right, ("ag", 0, -1, 1, to_right), right)
            push(0, 0, 1, to_left, ("ag", 0, 1, 1, to_left), left)
            push(0, 0, 1, k, ("ag", 1, 0, 1, k), over)
            push(0, 0, 1, k, ("ac", 0, 0), other)
        def piece(dx):
            return pl.ds(pl.multiple_of(xat(dx) * 32, 32), 32)

        for k, ways in enumerate((((0,), ()), ((), (1,)), ((2,), ()), ((1, 3), (3, 0, 2)))):
            net.got(block(0, 0, 0, k), ("own", k))
            for j in ways[0]:
                push(0, 0, 0, j, ("ag", 0, -1, 0, j), right)
            for j in ways[1]:
                push(0, 0, 0, j, ("ag", 0, 1, 0, j), left)
            push(0, 0, 0, k, ("ag", 1, 0, 0, k), over)
        for dz in (1, 3, 2):
            span = pl.ds(pl.multiple_of(zat(dz) * 512, 512), 512)
            net.send(hid.at[piece(0), span], hx.at[dz, piece(0)], ("hx",), {"zh": zat(dz)})
        hx[0] = hid[:, pl.ds(pl.multiple_of(zh * 512, 512), 512)]
        small_loads()
        mw, mix_part = mixing()
        turn(V)

        def from_side(half, dx, k):
            net.got(block(0, dx, half, k), ("ag", 0, dx, half, k))
            if (k % 2 == 0) == (dx == -1):
                push(0, dx, half, k, ("ag", 0, 2, half, k), right if dx == -1 else left)
            push(0, dx, half, k, ("ac", 0, dx), other)

        for half in (1, 0):
            for dx, k in ((-1, 0), (1, 1), (-1, 2), (1, 3)):
                from_side(half, dx, k)
            for k in range(K):
                net.got(block(1, 0, half, k), ("ag", 1, 0, half, k))
                push(1, 0, half, k, ("ag", 1, -1), right)
                push(1, 0, half, k, ("ag", 1, 1), left)
                push(1, 0, half, k, ("ac", 1, 0), other)
            for dx, k in ((-1, 1), (1, 0), (-1, 3), (1, 2)):
                from_side(half, dx, k)
        net.got(w.at[:, 0:V], ("ws",))
        turn(0)

        def from_far(half):
            for k in range(K):
                net.got(block(0, 2, half, k), ("ag", 0, 2, half, k))
                push(0, 2, half, k, ("ag", 1, 2, half), over)
                push(0, 2, half, k, ("ac", 0, 2), other)

        from_far(1)
        from_far(0)
        add_row(512)
        add_chip(1, 0, 512)
        for dx in (-1, 1):
            net.got(whole(1, dx), ("ag", 1, dx))
            net.send(whole(1, dx), whole(1, dx), ("ac", 1, dx), other)
            add_chip(1, dx, 512)
        for half in (1, 0):
            net.got(half_of(1, 2, half), ("ag", 1, 2, half))
            net.send(half_of(1, 2, half), half_of(1, 2, half), ("ac", 1, 2), other)
        add_chip(1, 2, 512)

        hit = hits(512)
        onehot = hit.astype(F32)
        targets = [jnp.sum(jnp.where(hit, eb[:, lanes(k)], 0.0), axis=0, keepdims=True) for k in range(K)]
        net.got(mixs, ("mix",))
        arx[0] = jnp.concatenate([*targets, mix_part[:4] + mixs[0:4]], axis=0)
        for i, (dl, dx) in enumerate(chips):
            net.send(arx.at[0], arx.at[i + 1], ("ar",), {"zl": (zl + dl) % 2, "x": xat(dx)})
        for k in range(K):
            grad = jnp.exp(eb[:, lanes(k)] - ln_ref[k : k + 1, :]) - onehot
            eb[:, lanes(k)] = grad
            lgu[:, lanes(k)] = (grad * SCALE).astype(BF)

        for row in (1 - zl, zl):
            for k in (0, 2):
                part = mm(w[pl.ds(pl.multiple_of(row * 1024, 1024), 1024), :], lgu[:, lanes(k, 2)])
                for j in (k, k + 1):
                    cgb[j, row] = part[:, (j - k) * T : (j - k + 1) * T].astype(BF).reshape(X, 2 * E, T)
                if row is zl:
                    continue
                for j in (k, k + 1):
                    net.send(cgb.at[j, 1 - zl, xat(2)], zf.at[j], ("zf", j), over)
                    net.send(cgb.at[j, 1 - zl, xat(1)], ro.at[j, 0], ("ro", j), right)
                    net.send(cgb.at[j, 1 - zl, xat(-1)], ro.at[j, 1], ("ro", j), left)

        def far(k):
            net.got(zf.at[k], ("zf", k))
            sf[k] = both(cgb.at[k, zl, xat(2)], zf.at[k])
            net.send(sf.at[k], r2.at[k], ("r2", k), left if k % 2 else right)

        def straight(k):
            if k % 2:
                net.send(cgb.at[k, zl, xat(1)], rx.at[k, 0], ("rx", k), right)
            else:
                net.send(cgb.at[k, zl, xat(-1)], rx.at[k, 1], ("rx", k), left)

        def combine(k):
            net.got(r2.at[k], ("r2", k))
            sp[k] = both(cgb.at[k, zl, xat(-1 if k % 2 else 1)], r2.at[k])
            if k % 2:
                net.send(sp.at[k], rx.at[k, 1], ("rx", k), left)
            else:
                net.send(sp.at[k], rx.at[k, 0], ("rx", k), right)

        def cross(k):
            net.got(ro.at[k], ("ro", k))
            zs[k] = (cgb[k, 1 - zl, x].astype(F32) + ro[k, 0].astype(F32) + ro[k, 1].astype(F32)).astype(BF)
            net.send(zs.at[k], rx.at[k, 2], ("rx", k), over)

        far(0)
        far(1)
        straight(0)
        straight(1)
        net.got(arx.at[1:8], ("ar",))
        sums = jnp.sum(arx[...], axis=0)
        sumb[...] = sums
        net.send(sumb, sumr, ("sum",), other)
        factor, mix_grad = shares(sums)
        scaled(factor, V)
        net.send(lgt.at[V : 2 * V], lgt.at[V : 2 * V], ("lgt",), other)
        far(2)
        far(3)
        straight(2)
        straight(3)
        factor = factor * (1.0 / SCALE)
        cross(0)
        cross(1)
        combine(0)
        combine(1)
        cross(2)
        cross(3)
        combine(2)
        combine(3)

        def z_send(k):
            net.send(pgz.at[k, :, lanes(0)], pgz.at[k, :, lanes(1)], ("pz", 1, k), {"zh": zat(1)})
            net.send(pgz.at[k, :, lanes(0)], pgz.at[k, :, lanes(3)], ("pz", 3, k), {"zh": zat(3)})

        def pre_grads(k):
            net.got(rx.at[k], ("rx", k))
            own = whole(0, 0)[:, k * T : (k + 1) * T].astype(F32)
            grad = cgb[k, zl, x].astype(F32) + rx[k, 0].astype(F32) + rx[k, 1].astype(F32) + rx[k, 2].astype(F32)
            grad = (grad * factor[k : k + 1] * (1.0 - own * own)).astype(BF)
            pgz[k, :, 0:T] = grad
            z_send(k)
            net.send(pgz.at[k, 0:E, lanes(0)], pgs.at[k * E : (k + 1) * E], ("pgs",), other)
            pgs[k * E : (k + 1) * E, :] = grad[E:]

        net.got(hx.at[1:4, piece(0)], ("hx",))
        for dx in (1, 3, 2):
            net.send(hx.at[1:4, piece(0)], hx.at[1:4, piece(0)], ("hy", 4 - dx), {"x": xat(dx)})
        pre_grads(0)
        pre_grads(1)
        pre_grads(2)
        pre_grads(3)
        hidden_part()

        def z_forward(k):
            side = 3 if k % 2 else 1
            net.got(pgz.at[k, :, lanes(side)], ("pz", side, k))
            net.send(pgz.at[k, :, lanes(side)], pgz.at[k, :, lanes(2)], ("pz", 2, k), {"zh": zat(side)})

        z_forward(0)
        z_forward(1)
        hidden_x()
        z_forward(2)
        z_forward(3)
        for dx in (1, 3, 2):
            net.got(hx.at[1:4, piece(dx)], ("hy", dx))
        for dz in range(ZH):
            ht[:, lanes(dz)] = hx[dz].T

        def proj(k):
            for j in (k, k + 1):
                net.got(pgz.at[j, :, lanes(1 if j % 2 else 3)], ("pz", 1 if j % 2 else 3, j))
                net.got(pgz.at[j, :, lanes(2)], ("pz", 2, j))
            part = mm_nt(ht[...], pgz[k : k + 2].reshape(4 * E, ZH * T))
            for j in (k, k + 1):
                pp[j] = part[:, (j - k) * 2 * E : (j - k + 1) * 2 * E].astype(BF).reshape(Y, 64, 2 * E)
            for j in (k, k + 1):
                sign, far_way, near_way = (-1, down, up) if j % 2 else (1, up, down)
                net.send(pp.at[j, yat(4 * sign)], pn.at[j, 0], ("pn", j), far_way)
                net.send(pp.at[j, yat(2 * sign)], pn.at[j, 1], ("pn", j), far_way)
                net.send(pp.at[j, yat(-3 * sign)], pn.at[j, 2], ("pn", j), near_way)
                net.send(pp.at[j, yat(-sign)], prx.at[j, 3], ("py", j), near_way)

        def proj_on(j):
            sign = -1 if j % 2 else 1
            net.got(pn.at[j], ("pn", j))
            for i, dist in enumerate((3 * sign, sign, -2 * sign)):
                pc[j, i] = both(pp.at[j, yat(dist)], pn.at[j, i])
                net.send(pc.at[j, i], prx.at[j, i], ("py", j), {"y": yat(dist)})

        proj(0)
        proj(2)
        for k in range(K):
            proj_on(k)
        hidden_z()
        for k in range(K):
            net.got(prx.at[k], ("py", k))
            total = pp[k, y].astype(F32)
            for i in range(4):
                total = total + prx[k, i].astype(F32)
            pst[0, pl.ds(k, 64, stride=K), :] = total[:, :E]
            pst[1, pl.ds(k, 64, stride=K), :] = total[:, E:]
        pgo[...] = pst[0].astype(BF)
        net.send(pgo, pgr, ("pgr",), other)
        pg_ref[...] = pst[1].astype(BF)
        hidden_out(mix_grad, mw)
        net.got(vgr, ("vgr",))
        vg_ref[...] = vgr[...]
        net.finish()

    def helper():
        for k in range(K):
            push(0, 0, 0, k, ("own", k), other)
        small_loads()
        net.send(w.at[:, 0:V], w.at[:, 0:V], ("ws",), other)
        mw, mix_part = mixing()
        mixb[...] = mix_part
        net.send(mixb, mixs, ("mix",), other)
        turn(0)
        for dl, dx in ((0, 0), (0, -1), (0, 1), (0, 2), (1, 0), (1, -1), (1, 1), (1, 2)):
            net.got(whole(dl, dx) if (dl, dx) != (0, 0) else half_of(0, 0, 1), ("ac", dl, dx))
            if (dl, dx) == (0, 2):
                add_row(V)
            elif dl == 1:
                add_chip(dl, dx, V)
        onehot = hits(V).astype(F32)
        for k in range(K):
            eb[0:V, lanes(k)] = jnp.exp(eb[0:V, lanes(k)] - ln_ref[k : k + 1, :]) - onehot
        net.got(sumr, ("sum",))
        factor, mix_grad = shares(sumr[...])
        scaled(factor, 0)
        vocab(0)
        net.got(lgt.at[V : 2 * V], ("lgt",))
        vocab(1)
        chain_round(1)
        net.got(pgs, ("pgs",))
        hidden_part()
        chain_round(2)
        hidden_x()
        chain_round(3)
        hidden_z()
        chain_end()
        hidden_out(mix_grad, mw)
        vocab_out()
        net.got(pgr, ("pgr",))
        pg_ref[...] = pgr[...]
        net.finish()

    before = list(net.bulk)
    pl.when(c == 1)(leader)
    net.bulk = before
    pl.when(c == 0)(helper)


def hand_over(*refs):
    copies = [pltpu.make_async_copy(refs[i], refs[3 + i], refs[6].at[i]) for i in range(3)]
    for copy in copies:
        copy.start()
    for copy in copies:
        copy.wait()


def body(hidden, mix_weight, comp_proj, vocab_weight, log_normalizer, targets, loss_grad):
    hbm, vmem = (pl.BlockSpec(memory_space=m) for m in (pl.ANY, pltpu.VMEM))
    scratch = [
        pltpu.VMEM(shape, dtype)
        for shape, dtype in (
            ((T, D), BF),
            ((D * K, E), BF),
            ((D, E), F32),
            ((D, K * E), BF),
            ((D, 2 * V), BF),
            ((2 * V, D), BF),
            ((K, E), BF),
            ((K, T), F32),
            ((1, T), jnp.int32),
            ((1, T), F32),
            ((8, T), F32),
            ((8, T), F32),
            ((D, K * T), BF),
            ((2 * V, K * T), F32),
            ((2 * V, K * T), BF),
            ((2 * V, K * T), BF),
            ((8, 8, T), F32),
            ((8, T), F32),
            ((8, T), F32),
            ((K, ZL, X, 2 * E, T), BF),
            *[((K, 2 * E, T), BF)] * 5,
            ((K, 3, 2 * E, T), BF),
            ((K, 2, 2 * E, T), BF),
            ((K, 2 * E, ZH * T), BF),
            ((K * E, T), BF),
            ((ZH, T, 512), BF),
            ((512, ZH * T), BF),
            ((K, Y, 64, 2 * E), BF),
            ((K, 3, 64, 2 * E), BF),
            ((K, 3, 64, 2 * E), BF),
            ((K, 4, 64, 2 * E), BF),
            ((2, 64 * K, E), F32),
            ((64 * K, E), BF),
            ((64 * K, E), BF),
            ((8, 2, 128, T), BF),
            ((8, 128, T), BF),
            ((ZL, X, 128, T), BF),
            ((3, ZL, 128, T), BF),
            ((ZL, 128, T), F32),
            ((128, T), BF),
            ((128, T), BF),
            ((2, ZH, Y, 64, V), BF),
            ((2, 2, 2, 4, 2, 64, V), BF),
            ((2, 2, 2, 4, 2, 64, V), BF),
            ((2, ZH, 64, V), BF),
            ((2, ZH, 64, V), BF),
            ((64, V), BF),
            ((64, V), BF),
        )
    ]
    scratch += [pltpu.SemaphoreType.DMA((N_SEND,)), pltpu.SemaphoreType.DMA((N_RECV,)), pltpu.SemaphoreType.DMA((10,))]
    shapes = (
        jax.ShapeDtypeStruct((T, E), BF),
        jax.ShapeDtypeStruct((64 * K, E), BF),
        jax.ShapeDtypeStruct((64, V), BF),
    )
    results = pl.pallas_call(
        kernel,
        out_shape=tuple(pltpu.VMEM(s.shape, s.dtype) for s in shapes),
        in_specs=[hbm] * 7,
        out_specs=(vmem,) * 3,
        scratch_shapes=scratch,
        compiler_params=pltpu.CompilerParams(
            collective_id=0, has_side_effects=True, vmem_limit_bytes=56 * 1024 * 1024
        ),
    )(
        hidden,
        comp_proj.reshape(D * K, E),
        vocab_weight,
        mix_weight,
        log_normalizer,
        targets.reshape(1, T),
        loss_grad.reshape(1, T),
    )
    hidden_grad, proj_grad, vocab_grad = pl.pallas_call(
        hand_over,
        out_shape=shapes,
        in_specs=[vmem] * 3,
        out_specs=(hbm,) * 3,
        scratch_shapes=[pltpu.SemaphoreType.DMA((3,))],
    )(*[pltpu.with_memory_space_constraint(r, pltpu.VMEM) for r in results])
    return hidden_grad, proj_grad.reshape(64, K, E), vocab_grad


def solution(mesh):
    split = Mesh(mesh.devices.reshape(ZH, Y, ZL, X, C), ("zh", "y", "zl", "x", "c"))
    tok, voc = ("zh", "y"), ("zl", "x", "c")
    in_specs = (P(tok, None), P(None, voc), P(None, None, voc), P(None, voc), P(None, tok), P(tok), P(tok))
    out_specs = (P(tok, voc), P(tok, None, voc), P(tok, voc))
    return jax.shard_map(body, mesh=split, in_specs=in_specs, out_specs=out_specs, check_vma=False)
```

```python
import math

import jax
import jax.numpy as jnp
from jax import lax
from jax.experimental import pallas as pl
from jax.experimental.pallas import tpu as pltpu
from jax.sharding import Mesh
from jax.sharding import PartitionSpec as P

MESH = pl.DeviceIdType.MESH
BF, F32 = jnp.bfloat16, jnp.float32
ZH, Y, ZL, X, C = 4, 8, 2, 4, 2
D, K, T, V, E = 2048, 4, 128, 256, 128
SCALE = 2.0**-16
BULK = 2 * 1024 * 1024
N_SEND, N_RECV = 5, 109

NT = (((1,), (1,)), ((), ()))
TN = (((0,), (0,)), ((), ()))


def mm(a, b):
    return jnp.dot(a, b, preferred_element_type=F32)


def mm_nt(a, b):
    return lax.dot_general(a, b, NT, preferred_element_type=F32)


class Net:
    def __init__(self, send_sems, recv_sems, yard):
        self.send_sems, self.recv_sems, self.yard = send_sems, recv_sems, yard
        self.roles, self.bulk = {}, []

    def slot(self, role):
        return self.recv_sems.at[self.roles.setdefault(role, len(self.roles))]

    def copy(self, src, dst, role, device):
        return pltpu.make_async_remote_copy(
            src_ref=src,
            dst_ref=dst,
            send_sem=self.send_sems.at[max(len(self.bulk), 1) - 1],
            recv_sem=self.slot(role),
            device_id=device,
            device_id_type=MESH,
        )

    def send(self, src, dst, role, device):
        size = math.prod(src.shape) * src.dtype.itemsize
        if not self.bulk or self.bulk[-1] + size > BULK:
            self.bulk.append(0)
        self.bulk[-1] += size
        self.copy(src, dst, role, device).start()

    def got(self, dst, role):
        self.copy(dst, dst, role, {"c": 1 - lax.axis_index("c")}).wait_recv()

    def finish(self):
        for i, size in enumerate(self.bulk):
            sent = self.yard.at[pl.ds(0, size // (E * 2))]
            pltpu.make_async_copy(sent, sent, self.send_sems.at[i]).wait()


def kernel(
    hid_hbm, cp_hbm, w_hbm, mw_hbm, ln_hbm, tg_hbm, loss_hbm,
    hg_ref, pg_ref, vg_ref,
    hid, cpraw, stage, cp, w, wt, mw_ref, ln_ref, tg_ref, loss_ref, mixb, mixs, ctx, eb, lgt, lgu, arx, sumb, sumr,
    cgb, zf, sf, r2, sp, zs, rx, ro, pgz, pgs, hx, ht, pp, pc, pn, prx, pst, ppo,
    hpb, hq, hs, hrx, hsum, hz, hzr, vgb, vsb, vrb, vzs, vzr, vgo, vgr,
    send_sems, recv_sems, local_sems,
):
    zh, y = lax.axis_index("zh"), lax.axis_index("y")
    zl, x, c = lax.axis_index("zl"), lax.axis_index("x"), lax.axis_index("c")
    chip = zl * X + x
    voc = chip * 2 + c
    net = Net(send_sems, recv_sems, cpraw)

    def xat(dx):
        return lax.rem(x + dx + X, X)

    def yat(dy):
        return lax.rem(y + dy + Y, Y)

    def zat(dz):
        return lax.rem(zh + dz, ZH)

    def lanes(k, n=1):
        return pl.ds(k * T, n * T)

    right, left = {"x": xat(1)}, {"x": xat(-1)}
    up, down = {"y": yat(1)}, {"y": yat(-1)}
    other, over = {"c": 1 - c}, {"zl": 1 - zl}
    chips = [(dl, dx) for dl in range(2) for dx in range(4)][1:]

    barrier = pltpu.get_barrier_semaphore()
    greeted = [{"zl": (zl + dl) % 2, "x": xat(dx)} for dl, dx in chips] + [other]
    greeted += [{"y": yat(dy), "c": a} for dy in (1, 2, 3, 5, 6, 7) for a in (c, 1 - c)]
    greeted += [{"zh": zat(dz)} for dz in range(1, ZH)]
    greeted += [{"c": 1 - c, **device} for device in (right, left, over)]
    parts = 8
    rows = D * K // parts
    loads = [pltpu.make_async_copy(hid_hbm, hid, local_sems.at[0])]
    for q in range(parts):
        span = pl.ds(q * rows, rows)
        loads.append(pltpu.make_async_copy(cp_hbm.at[span], cpraw.at[span], local_sems.at[1 + q]))
    small = [(mw_hbm, mw_ref), (ln_hbm, ln_ref), (tg_hbm, tg_ref), (loss_hbm, loss_ref)]
    small += [(w_hbm, w.at[:, pl.ds(pl.multiple_of(c * V, V), V)])]
    for i, (src, dst) in enumerate(small):
        loads.append(pltpu.make_async_copy(src, dst, local_sems.at[1 + parts + i]))
    for i in (1, 0, *range(2, len(loads))):
        loads[i].start()
    for device in greeted:
        pl.semaphore_signal(barrier, inc=1, device_id=device, device_id_type=MESH)

    pre = jnp.zeros((T, K * E), F32)
    for q in range(parts):
        loads[1 + q].wait()
        stage[...] = cpraw[pl.ds(q * rows, rows), :].astype(F32)
        span = pl.ds(q * (D // parts), D // parts)
        for k in range(K):
            cp[span, lanes(k)] = stage[pl.ds(k, D // parts, stride=K), :].astype(BF)
        if q == 0:
            loads[0].wait()
        if q % 4 == 3:
            span = pl.ds((q - 3) * (D // parts), D // 2)
            pre = pre + mm(hid[:, span], cp[span, :])
    acts = jnp.tanh(pre)
    for k in range(K):
        ctx[pl.ds(pl.multiple_of(voc * E, E), E), lanes(k)] = acts[:, k * E : (k + 1) * E].T.astype(BF)

    pl.semaphore_wait(barrier, len(greeted))

    def chip_at(dl, dx):
        return (zl + dl) % 2 * X + xat(dx)

    def block(dl, dx, half, k):
        at = chip_at(dl, dx) * 256 + half * E
        return ctx.at[pl.ds(pl.multiple_of(at, E), E), lanes(k)]

    def half_of(dl, dx, half):
        return ctx.at[pl.ds(pl.multiple_of(chip_at(dl, dx) * 256 + half * E, E), E)]

    def whole(dl, dx):
        return ctx.at[pl.ds(pl.multiple_of(chip_at(dl, dx) * 256, 256), 256)]

    def push_own(k, role, device):
        net.send(block(0, 0, c, k), block(0, 0, c, k), role, device)

    def push_both(dl, dx, k, role, device):
        net.send(whole(dl, dx).at[:, lanes(k)], whole(dl, dx).at[:, lanes(k)], role, device)

    def pass_on(dl, dx):
        net.send(whole(dl, dx), whole(dl, dx), ("ac", dl, dx), other)

    def small_loads():
        for i in range(len(small)):
            loads[1 + parts + i].wait()

    def mixing():
        mw = jnp.concatenate([mw_ref[...].astype(F32), jnp.zeros((4, E), F32)], axis=0)
        return mw, mm_nt(mw.astype(BF), hid[:, pl.ds(pl.multiple_of(voc * E, E), E)])

    def turn(start):
        for j in range(16):
            wt[start : start + V, j * 128 : (j + 1) * 128] = w[j * 128 : (j + 1) * 128, start : start + V].T

    def add_chip(dl, dx, n):
        span = pl.ds(pl.multiple_of(chip_at(dl, dx) * 256, 256), 256)
        eb[0:n] += mm(wt[0:n, span], ctx[span, :])

    def add_row(n):
        span = pl.ds(pl.multiple_of(zl * 1024, 1024), 1024)
        eb[0:n] = mm(wt[0:n, span], ctx[span, :])

    def hits(n):
        return (lax.broadcasted_iota(jnp.int32, (n, T), 0) + chip * 512) == tg_ref[...]

    def shares(sums):
        exp_mix = jnp.exp(sums[4:])
        weights = exp_mix / jnp.sum(exp_mix, axis=0, keepdims=True)
        joint = weights * jnp.exp(sums[:4] - ln_ref[...])
        posterior = joint / jnp.sum(joint, axis=0, keepdims=True)
        return loss_ref[...] * posterior, loss_ref[...] * (weights - posterior)

    def both(a, b):
        return (a[...].astype(F32) + b[...].astype(F32)).astype(BF)

    def scaled(factor, start):
        for k in range(K):
            lgt[start : start + V, lanes(k)] = (factor[k : k + 1] * eb[start : start + V, lanes(k)]).astype(BF)

    def vocab(ids):
        for a in range(ZH):
            part = mm_nt(ctx[a * 512 : (a + 1) * 512, :], lgt[ids * V : (ids + 1) * V])
            vgb[ids, a] = part.astype(BF).reshape(Y, 64, V)
        chain_part(ids, 0)

    def chain_send(ids, way, half, dist):
        sign = 1 - 2 * way
        owner = yat(sign * dist)
        src = vgb.at[ids, 2 * half : 2 * half + 2, owner]
        if dist < (4 if half == way else 3):
            got = vrb.at[ids, way, half, dist]
            net.got(got, ("vy", ids, way, half, dist + 1))
            vsb[ids, way, half, dist - 1] = both(src, got)
            src = vsb.at[ids, way, half, dist - 1]
        there = vrb.at[ids, way, half, dist - 1]
        net.send(src, there, ("vy", ids, way, half, dist), up if way == 0 else down)

    def chain_part(ids, n):
        for half in range(2):
            for way in range(2):
                dist = (4 if half == way else 3) - n
                if dist > 0:
                    chain_send(ids, way, half, dist)

    def chain_round(n):
        for ids in range(2):
            chain_part(ids, n)

    def chain_end():
        for ids in range(2):
            for half in range(2):
                span = slice(2 * half, 2 * half + 2)
                total = vgb[ids, span, y].astype(F32)
                for way in range(2):
                    net.got(vrb.at[ids, way, half, 0], ("vy", ids, way, half, 1))
                    total = total + vrb[ids, way, half, 0].astype(F32)
                vzs[ids, span] = total.astype(BF)
            for dz in (2, 1, 3):
                net.send(vzs.at[ids, zat(dz)], vzr.at[ids, dz], ("vz", ids), {"zh": zat(dz)})

    def vocab_out():
        for ids in (1, 0):
            total = vzs[ids, zh].astype(F32)
            net.got(vzr.at[ids, 1:4], ("vz", ids))
            for dz in range(1, ZH):
                total = total + vzr[ids, dz].astype(F32)
            if ids:
                vgo[...] = total.astype(BF)
                net.send(vgo, vgr, ("vgr",), other)
            else:
                vg_ref[...] = total.astype(BF)

    def hidden_part():
        for j in range(4):
            part = mm(cp[j * 512 : (j + 1) * 512, :], pgs[...])
            hpb[2 * j : 2 * j + 2] = part.astype(BF).reshape(2, 2, 128, T)
        net.send(hpb.at[:, 1 - c], hq, ("hq",), other)

    def hidden_x():
        net.got(hq, ("hq",))
        for j in range(8):
            hs[j // X, j % X] = both(hpb.at[j, c], hq.at[j])
        for dx in (1, 3, 2):
            net.send(hs.at[:, xat(dx)], hrx.at[dx - 1], ("hr",), {"x": xat(dx)})

    def hidden_z():
        net.got(hrx, ("hr",))
        hsum[...] = hs[:, x].astype(F32)
        for i in range(3):
            hsum[...] += hrx[i].astype(F32)
        hz[...] = hsum[1 - zl].astype(BF)
        net.send(hz, hzr, ("hz",), over)

    def hidden_out(mix_grad, mw):
        net.got(hzr, ("hz",))
        total = hsum[zl] + hzr[...].astype(F32)
        mix_grad = jnp.concatenate([mix_grad, jnp.zeros((4, T), F32)], axis=0)
        mix_term = lax.dot_general(mix_grad, mw, TN, precision=lax.Precision.HIGHEST, preferred_element_type=F32)
        hg_ref[...] = (total.T + mix_term).astype(BF)

    def proj_out(own):
        for k in range(K):
            net.got(prx.at[k], ("py", k))
            total = own(k).astype(F32)
            for i in range(4):
                total = total + prx[k, i].astype(F32)
            pst[pl.ds(k, 64, stride=K), :] = total
        pg_ref[...] = pst[...].astype(BF)

    def push_first(to_right, to_left, to_over):
        for k, k_right, k_left in zip(range(K), (0, 2, 1, 3), (1, 3, 0, 2)):
            push_own(k_right, ("ag", 0, -1, k_right), to_right)
            push_own(k_left, ("ag", 0, 1, k_left), to_left)
            push_own(k, ("ag", 1, 0, k), to_over)

    def leader():
        push_first(right, left, over)
        net.send(half_of(0, 0, 1), half_of(0, 0, 1), ("ac", 0, 0), other)
        def piece(dx):
            return pl.ds(pl.multiple_of(xat(dx) * 32, 32), 32)

        for dz in (1, 3, 2):
            span = pl.ds(pl.multiple_of(zat(dz) * 512, 512), 512)
            net.send(hid.at[piece(0), span], hx.at[dz, piece(0)], ("hx",), {"zh": zat(dz)})
        hx[0] = hid[:, pl.ds(pl.multiple_of(zh * 512, 512), 512)]
        small_loads()
        mw, mix_part = mixing()
        turn(V)

        def arrived(dl, dx, k):
            net.got(whole(dl, dx).at[:, lanes(k)], ("ag", dl, dx, k))

        for dx, k, device in ((-1, 0, right), (1, 1, left), (-1, 2, right), (1, 3, left)):
            arrived(0, dx, k)
            push_both(0, dx, k, ("ag", 0, 2, k), device)
        for k in range(K):
            arrived(1, 0, k)
            push_both(1, 0, k, ("ag", 1, -1), right)
            push_both(1, 0, k, ("ag", 1, 1), left)
        for dx, k in ((-1, 1), (1, 0), (-1, 3), (1, 2)):
            arrived(0, dx, k)
        for dl, dx in ((0, -1), (0, 1), (1, 0)):
            pass_on(dl, dx)
        net.got(w.at[:, 0:V], ("ws",))
        turn(0)

        for k in range(K):
            arrived(0, 2, k)
            push_both(0, 2, k, ("ag", 1, 2), over)
        pass_on(0, 2)
        net.got(half_of(0, 0, 0), ("own",))
        add_row(512)
        add_chip(1, 0, 512)
        for dx in (-1, 1, 2):
            net.got(whole(1, dx), ("ag", 1, dx))
            pass_on(1, dx)
            add_chip(1, dx, 512)

        hit = hits(512)
        onehot = hit.astype(F32)

        def grads(k):
            return jnp.exp(eb[:, lanes(k)] - ln_ref[k : k + 1, :]) - onehot

        targets = [jnp.sum(jnp.where(hit, eb[:, lanes(k)], 0.0), axis=0, keepdims=True) for k in range(K)]
        net.got(mixs, ("mix",))
        arx[0] = jnp.concatenate([*targets, mix_part[:4] + mixs[0:4]], axis=0)
        for i, (dl, dx) in enumerate(chips):
            net.send(arx.at[0], arx.at[i + 1], ("ar",), {"zl": (zl + dl) % 2, "x": xat(dx)})

        def part_of(row, k):
            part = mm(w[pl.ds(pl.multiple_of(row * 1024, 1024), 1024), :], lgu[:, lanes(k, 2)])
            for j in (k, k + 1):
                cgb[j, row] = part[:, (j - k) * T : (j - k + 1) * T].astype(BF).reshape(X, 2 * E, T)

        for k in (0, 2):
            for j in (k, k + 1):
                lgu[:, lanes(j)] = (grads(j) * SCALE).astype(BF)
            part_of(1 - zl, k)
            for j in (k, k + 1):
                net.send(cgb.at[j, 1 - zl, xat(2)], zf.at[j], ("zf", j), over)
                net.send(cgb.at[j, 1 - zl, xat(1)], ro.at[j, 0], ("ro", j), right)
                net.send(cgb.at[j, 1 - zl, xat(-1)], ro.at[j, 1], ("ro", j), left)
        part_of(zl, 0)
        part_of(zl, 2)
        for k in range(K):
            eb[:, lanes(k)] = grads(k)

        def far(k):
            net.got(zf.at[k], ("zf", k))
            sf[k] = both(cgb.at[k, zl, xat(2)], zf.at[k])
            net.send(sf.at[k], r2.at[k], ("r2", k), left if k % 2 else right)

        def straight(k):
            if k % 2:
                net.send(cgb.at[k, zl, xat(1)], rx.at[k, 0], ("rx", k), right)
            else:
                net.send(cgb.at[k, zl, xat(-1)], rx.at[k, 1], ("rx", k), left)

        def combine(k):
            net.got(r2.at[k], ("r2", k))
            sp[k] = both(cgb.at[k, zl, xat(-1 if k % 2 else 1)], r2.at[k])
            if k % 2:
                net.send(sp.at[k], rx.at[k, 1], ("rx", k), left)
            else:
                net.send(sp.at[k], rx.at[k, 0], ("rx", k), right)

        def cross(k):
            net.got(ro.at[k], ("ro", k))
            zs[k] = (cgb[k, 1 - zl, x].astype(F32) + ro[k, 0].astype(F32) + ro[k, 1].astype(F32)).astype(BF)
            net.send(zs.at[k], rx.at[k, 2], ("rx", k), over)

        far(0)
        far(1)
        straight(0)
        straight(1)
        net.got(arx.at[1:8], ("ar",))
        sums = jnp.sum(arx[...], axis=0)
        sumb[...] = sums
        net.send(sumb, sumr, ("sum",), other)
        factor, mix_grad = shares(sums)
        scaled(factor, V)
        net.send(lgt.at[V : 2 * V], lgt.at[V : 2 * V], ("lgt",), other)
        far(2)
        far(3)
        straight(2)
        straight(3)
        factor = factor * (1.0 / SCALE)
        cross(0)
        cross(1)
        combine(0)
        combine(1)
        cross(2)
        cross(3)
        combine(2)
        combine(3)

        def z_send(k):
            net.send(pgz.at[k, :, lanes(0)], pgz.at[k, :, lanes(1)], ("pz", 1, k), {"zh": zat(1)})
            net.send(pgz.at[k, :, lanes(0)], pgz.at[k, :, lanes(3)], ("pz", 3, k), {"zh": zat(3)})

        def pre_grads(k):
            net.got(rx.at[k], ("rx", k))
            own = whole(0, 0)[:, k * T : (k + 1) * T].astype(F32)
            grad = cgb[k, zl, x].astype(F32) + rx[k, 0].astype(F32) + rx[k, 1].astype(F32) + rx[k, 2].astype(F32)
            grad = (grad * factor[k : k + 1] * (1.0 - own * own)).astype(BF)
            pgz[k, :, 0:T] = grad
            z_send(k)
            net.send(pgz.at[k, 0:E, lanes(0)], pgs.at[k * E : (k + 1) * E], ("pgs",), other)
            pgs[k * E : (k + 1) * E, :] = grad[E:]

        net.got(hx.at[1:4, piece(0)], ("hx",))
        for dx in (1, 3, 2):
            net.send(hx.at[1:4, piece(0)], hx.at[1:4, piece(0)], ("hy", 4 - dx), {"x": xat(dx)})
        pre_grads(0)
        pre_grads(1)
        pre_grads(2)
        pre_grads(3)
        hidden_part()

        def z_forward(k):
            side = 3 if k % 2 else 1
            net.got(pgz.at[k, :, lanes(side)], ("pz", side, k))
            net.send(pgz.at[k, :, lanes(side)], pgz.at[k, :, lanes(2)], ("pz", 2, k), {"zh": zat(side)})

        z_forward(0)
        z_forward(1)
        hidden_x()
        z_forward(2)
        z_forward(3)
        for dx in (1, 3, 2):
            net.got(hx.at[1:4, piece(dx)], ("hy", dx))
        for dz in range(ZH):
            ht[:, lanes(dz)] = hx[dz].T

        def give(src, j, i, dist):
            net.send(src.at[:, 0:E], prx.at[j, i], ("py", j), {"y": yat(dist), **other})
            net.send(src.at[:, E : 2 * E], prx.at[j, i], ("py", j), {"y": yat(dist)})

        def proj(k):
            for j in (k, k + 1):
                net.got(pgz.at[j, :, lanes(1 if j % 2 else 3)], ("pz", 1 if j % 2 else 3, j))
                net.got(pgz.at[j, :, lanes(2)], ("pz", 2, j))
            part = mm_nt(ht[...], pgz[k : k + 2].reshape(4 * E, ZH * T))
            for j in (k, k + 1):
                pp[j] = part[:, (j - k) * 2 * E : (j - k + 1) * 2 * E].astype(BF).reshape(Y, 64, 2 * E)
            for j in (k, k + 1):
                sign, far_way, near_way = (-1, down, up) if j % 2 else (1, up, down)
                net.send(pp.at[j, yat(4 * sign)], pn.at[j, 0], ("pn", j), far_way)
                net.send(pp.at[j, yat(2 * sign)], pn.at[j, 1], ("pn", j), far_way)
                net.send(pp.at[j, yat(-3 * sign)], pn.at[j, 2], ("pn", j), near_way)
                give(pp.at[j, yat(-sign)], j, 3, -sign)
                net.send(pp.at[j, y, :, 0:E], ppo.at[j], ("po",), other)

        def proj_on(j):
            sign = -1 if j % 2 else 1
            net.got(pn.at[j], ("pn", j))
            for i, dist in enumerate((3 * sign, sign, -2 * sign)):
                pc[j, i] = both(pp.at[j, yat(dist)], pn.at[j, i])
                give(pc.at[j, i], j, i, dist)

        proj(0)
        proj(2)
        for k in range(K):
            proj_on(k)
        hidden_z()
        hidden_out(mix_grad, mw)
        net.got(vgr, ("vgr",))
        vg_ref[...] = vgr[...]
        proj_out(lambda k: pp[k, y, :, E : 2 * E])
        net.finish()

    def helper():
        push_first({**right, **other}, {**left, **other}, {**over, **other})
        net.send(half_of(0, 0, 0), half_of(0, 0, 0), ("own",), other)
        small_loads()
        net.send(w.at[:, 0:V], w.at[:, 0:V], ("ws",), other)
        mw, mix_part = mixing()
        mixb[...] = mix_part
        net.send(mixb, mixs, ("mix",), other)
        turn(0)
        for dl, dx in ((0, 0), (0, -1), (0, 1), (0, 2), (1, 0), (1, -1), (1, 1), (1, 2)):
            net.got(whole(dl, dx) if (dl, dx) != (0, 0) else half_of(0, 0, 1), ("ac", dl, dx))
            if (dl, dx) == (0, 2):
                add_row(V)
            elif dl == 1:
                add_chip(dl, dx, V)
        onehot = hits(V).astype(F32)
        for k in range(K):
            eb[0:V, lanes(k)] = jnp.exp(eb[0:V, lanes(k)] - ln_ref[k : k + 1, :]) - onehot
        net.got(sumr, ("sum",))
        factor, mix_grad = shares(sumr[...])
        scaled(factor, 0)
        vocab(0)
        net.got(lgt.at[V : 2 * V], ("lgt",))
        vocab(1)
        chain_round(1)
        net.got(pgs, ("pgs",))
        hidden_part()
        chain_round(2)
        hidden_x()
        chain_round(3)
        hidden_z()
        chain_end()
        hidden_out(mix_grad, mw)
        vocab_out()
        net.got(ppo, ("po",))
        proj_out(lambda k: ppo[k])
        net.finish()

    before = list(net.bulk)
    pl.when(c == 1)(leader)
    net.bulk = before
    pl.when(c == 0)(helper)


def hand_over(*refs):
    copies = [pltpu.make_async_copy(refs[i], refs[3 + i], refs[6].at[i]) for i in range(3)]
    for copy in copies:
        copy.start()
    for copy in copies:
        copy.wait()


def body(hidden, mix_weight, comp_proj, vocab_weight, log_normalizer, targets, loss_grad):
    hbm, vmem = (pl.BlockSpec(memory_space=m) for m in (pl.ANY, pltpu.VMEM))
    scratch = [
        pltpu.VMEM(shape, dtype)
        for shape, dtype in (
            ((T, D), BF),
            ((D * K, E), BF),
            ((D // 2, E), F32),
            ((D, K * E), BF),
            ((D, 2 * V), BF),
            ((2 * V, D), BF),
            ((K, E), BF),
            ((K, T), F32),
            ((1, T), jnp.int32),
            ((1, T), F32),
            ((8, T), F32),
            ((8, T), F32),
            ((D, K * T), BF),
            ((2 * V, K * T), F32),
            ((2 * V, K * T), BF),
            ((2 * V, K * T), BF),
            ((8, 8, T), F32),
            ((8, T), F32),
            ((8, T), F32),
            ((K, ZL, X, 2 * E, T), BF),
            *[((K, 2 * E, T), BF)] * 5,
            ((K, 3, 2 * E, T), BF),
            ((K, 2, 2 * E, T), BF),
            ((K, 2 * E, ZH * T), BF),
            ((K * E, T), BF),
            ((ZH, T, 512), BF),
            ((512, ZH * T), BF),
            ((K, Y, 64, 2 * E), BF),
            ((K, 3, 64, 2 * E), BF),
            ((K, 3, 64, 2 * E), BF),
            ((K, 4, 64, E), BF),
            ((64 * K, E), F32),
            ((K, 64, E), BF),
            ((8, 2, 128, T), BF),
            ((8, 128, T), BF),
            ((ZL, X, 128, T), BF),
            ((3, ZL, 128, T), BF),
            ((ZL, 128, T), F32),
            ((128, T), BF),
            ((128, T), BF),
            ((2, ZH, Y, 64, V), BF),
            ((2, 2, 2, 4, 2, 64, V), BF),
            ((2, 2, 2, 4, 2, 64, V), BF),
            ((2, ZH, 64, V), BF),
            ((2, ZH, 64, V), BF),
            ((64, V), BF),
            ((64, V), BF),
        )
    ]
    scratch += [pltpu.SemaphoreType.DMA((N_SEND,)), pltpu.SemaphoreType.DMA((N_RECV,)), pltpu.SemaphoreType.DMA((14,))]
    shapes = (
        jax.ShapeDtypeStruct((T, E), BF),
        jax.ShapeDtypeStruct((64 * K, E), BF),
        jax.ShapeDtypeStruct((64, V), BF),
    )
    results = pl.pallas_call(
        kernel,
        out_shape=tuple(pltpu.VMEM(s.shape, s.dtype) for s in shapes),
        in_specs=[hbm] * 7,
        out_specs=(vmem,) * 3,
        scratch_shapes=scratch,
        compiler_params=pltpu.CompilerParams(
            collective_id=0, has_side_effects=True, vmem_limit_bytes=56 * 1024 * 1024
        ),
    )(
        hidden,
        comp_proj.reshape(D * K, E),
        vocab_weight,
        mix_weight,
        log_normalizer,
        targets.reshape(1, T),
        loss_grad.reshape(1, T),
    )
    hidden_grad, proj_grad, vocab_grad = pl.pallas_call(
        hand_over,
        out_shape=shapes,
        in_specs=[vmem] * 3,
        out_specs=(hbm,) * 3,
        scratch_shapes=[pltpu.SemaphoreType.DMA((3,))],
    )(*[pltpu.with_memory_space_constraint(r, pltpu.VMEM) for r in results])
    return hidden_grad, proj_grad.reshape(64, K, E), vocab_grad


def solution(mesh):
    split = Mesh(mesh.devices.reshape(ZH, Y, ZL, X, C), ("zh", "y", "zl", "x", "c"))
    tok, voc = ("zh", "y"), ("zl", "x", "c")
    in_specs = (P(tok, None), P(None, voc), P(None, None, voc), P(None, voc), P(None, tok), P(tok), P(tok))
    out_specs = (P(tok, voc), P(tok, None, voc), P(tok, voc))
    return jax.shard_map(body, mesh=split, in_specs=in_specs, out_specs=out_specs, check_vma=False)
```

```python
import math

import jax
import jax.numpy as jnp
from jax import lax
from jax.experimental import pallas as pl
from jax.experimental.pallas import tpu as pltpu
from jax.sharding import Mesh
from jax.sharding import PartitionSpec as P

MESH = pl.DeviceIdType.MESH
BF, F32 = jnp.bfloat16, jnp.float32
ZH, Y, ZL, X, C = 4, 8, 2, 4, 2
D, K, T, V, E = 2048, 4, 128, 256, 128
SCALE = 2.0**-16
BULK = 2 * 1024 * 1024
N_SEND, N_RECV = 5, 109

NT = (((1,), (1,)), ((), ()))
TN = (((0,), (0,)), ((), ()))


def mm(a, b):
    return jnp.dot(a, b, preferred_element_type=F32)


def mm_nt(a, b):
    return lax.dot_general(a, b, NT, preferred_element_type=F32)


class Net:
    def __init__(self, send_sems, recv_sems, yard):
        self.send_sems, self.recv_sems, self.yard = send_sems, recv_sems, yard
        self.roles, self.bulk = {}, []

    def slot(self, role):
        return self.recv_sems.at[self.roles.setdefault(role, len(self.roles))]

    def copy(self, src, dst, role, device):
        return pltpu.make_async_remote_copy(
            src_ref=src,
            dst_ref=dst,
            send_sem=self.send_sems.at[max(len(self.bulk), 1) - 1],
            recv_sem=self.slot(role),
            device_id=device,
            device_id_type=MESH,
        )

    def send(self, src, dst, role, device):
        size = math.prod(src.shape) * src.dtype.itemsize
        if not self.bulk or self.bulk[-1] + size > BULK:
            self.bulk.append(0)
        self.bulk[-1] += size
        self.copy(src, dst, role, device).start()

    def got(self, dst, role):
        self.copy(dst, dst, role, {"c": 1 - lax.axis_index("c")}).wait_recv()

    def finish(self):
        for i, size in enumerate(self.bulk):
            sent = self.yard.at[pl.ds(0, size // (E * 2))]
            pltpu.make_async_copy(sent, sent, self.send_sems.at[i]).wait()


def kernel(
    hid_hbm, cp_hbm, w_hbm, mw_hbm, ln_hbm, tg_hbm, loss_hbm,
    hg_ref, pg_ref, vg_ref,
    hid, cpraw, stage, cp, w, wt, mw_ref, ln_ref, tg_ref, loss_ref, mixb, mixs, ctx, eb, lgt, lgu, arx, sumb, sumr,
    cgb, zf, sf, r2, sp, zs, rx, ro, pgz, pgs, hx, ht, pp, pc, pn, prx, pst, ppo,
    hpb, hq, hs, hrx, hsum, hz, hzr, vgb, vsb, vrb, vzs, vzr, vgo, vgr,
    send_sems, recv_sems, local_sems,
):
    zh, y = lax.axis_index("zh"), lax.axis_index("y")
    zl, x, c = lax.axis_index("zl"), lax.axis_index("x"), lax.axis_index("c")
    chip = zl * X + x
    voc = chip * 2 + c
    net = Net(send_sems, recv_sems, cpraw)

    def xat(dx):
        return lax.rem(x + dx + X, X)

    def yat(dy):
        return lax.rem(y + dy + Y, Y)

    def zat(dz):
        return lax.rem(zh + dz, ZH)

    def lanes(k, n=1):
        return pl.ds(k * T, n * T)

    right, left = {"x": xat(1)}, {"x": xat(-1)}
    up, down = {"y": yat(1)}, {"y": yat(-1)}
    other, over = {"c": 1 - c}, {"zl": 1 - zl}
    chips = [(dl, dx) for dl in range(2) for dx in range(4)][1:]

    barrier = pltpu.get_barrier_semaphore()
    greeted = [{"zl": (zl + dl) % 2, "x": xat(dx)} for dl, dx in chips] + [other]
    greeted += [{"y": yat(dy), "c": a} for dy in (1, 2, 3, 5, 6, 7) for a in (c, 1 - c)]
    greeted += [{"zh": zat(dz)} for dz in range(1, ZH)]
    greeted += [{"c": 1 - c, **device} for device in (right, left, over)]
    parts = 8
    rows = D * K // parts
    loads = [pltpu.make_async_copy(hid_hbm, hid, local_sems.at[0])]
    for q in range(parts):
        span = pl.ds(q * rows, rows)
        loads.append(pltpu.make_async_copy(cp_hbm.at[span], cpraw.at[span], local_sems.at[1 + q]))
    small = [(mw_hbm, mw_ref), (ln_hbm, ln_ref), (tg_hbm, tg_ref), (loss_hbm, loss_ref)]
    small += [(w_hbm, w.at[:, pl.ds(pl.multiple_of(c * V, V), V)])]
    for i, (src, dst) in enumerate(small):
        loads.append(pltpu.make_async_copy(src, dst, local_sems.at[1 + parts + i]))
    for i in (1, 0, *range(2, len(loads))):
        loads[i].start()
    for device in greeted:
        pl.semaphore_signal(barrier, inc=1, device_id=device, device_id_type=MESH)

    pre = jnp.zeros((T, K * E), F32)
    for q in range(parts):
        loads[1 + q].wait()
        stage[...] = cpraw[pl.ds(q * rows, rows), :].astype(F32)
        span = pl.ds(q * (D // parts), D // parts)
        for k in range(K):
            cp[span, lanes(k)] = stage[pl.ds(k, D // parts, stride=K), :].astype(BF)
        if q == 0:
            loads[0].wait()
        if q % 4 == 3:
            span = pl.ds((q - 3) * (D // parts), D // 2)
            pre = pre + mm(hid[:, span], cp[span, :])
    acts = jnp.tanh(pre)
    for k in range(K):
        ctx[pl.ds(pl.multiple_of(voc * E, E), E), lanes(k)] = acts[:, k * E : (k + 1) * E].T.astype(BF)

    pl.semaphore_wait(barrier, len(greeted))

    def chip_at(dl, dx):
        return (zl + dl) % 2 * X + xat(dx)

    def block(dl, dx, half, k):
        at = chip_at(dl, dx) * 256 + half * E
        return ctx.at[pl.ds(pl.multiple_of(at, E), E), lanes(k)]

    def half_of(dl, dx, half):
        return ctx.at[pl.ds(pl.multiple_of(chip_at(dl, dx) * 256 + half * E, E), E)]

    def whole(dl, dx):
        return ctx.at[pl.ds(pl.multiple_of(chip_at(dl, dx) * 256, 256), 256)]

    def push_own(k, role, device):
        net.send(block(0, 0, c, k), block(0, 0, c, k), role, device)

    def push_both(dl, dx, k, role, device):
        net.send(whole(dl, dx).at[:, lanes(k)], whole(dl, dx).at[:, lanes(k)], role, device)

    def pass_on(dl, dx):
        net.send(whole(dl, dx), whole(dl, dx), ("ac", dl, dx), other)

    def small_loads():
        for i in range(len(small)):
            loads[1 + parts + i].wait()

    def mixing():
        mw = jnp.concatenate([mw_ref[...].astype(F32), jnp.zeros((4, E), F32)], axis=0)
        return mw, mm_nt(mw.astype(BF), hid[:, pl.ds(pl.multiple_of(voc * E, E), E)])

    def turn(start):
        for j in range(16):
            wt[start : start + V, j * 128 : (j + 1) * 128] = w[j * 128 : (j + 1) * 128, start : start + V].T

    def add_chip(dl, dx, n):
        span = pl.ds(pl.multiple_of(chip_at(dl, dx) * 256, 256), 256)
        eb[0:n] += mm(wt[0:n, span], ctx[span, :])

    def add_row(n):
        span = pl.ds(pl.multiple_of(zl * 1024, 1024), 1024)
        eb[0:n] = mm(wt[0:n, span], ctx[span, :])

    def hits(n):
        return (lax.broadcasted_iota(jnp.int32, (n, T), 0) + chip * 512) == tg_ref[...]

    def shares(sums):
        exp_mix = jnp.exp(sums[4:])
        weights = exp_mix / jnp.sum(exp_mix, axis=0, keepdims=True)
        joint = weights * jnp.exp(sums[:4] - ln_ref[...])
        posterior = joint / jnp.sum(joint, axis=0, keepdims=True)
        return loss_ref[...] * posterior, loss_ref[...] * (weights - posterior)

    def both(a, b):
        return (a[...].astype(F32) + b[...].astype(F32)).astype(BF)

    def scaled(factor, start):
        for k in range(K):
            lgt[start : start + V, lanes(k)] = (factor[k : k + 1] * eb[start : start + V, lanes(k)]).astype(BF)

    def vocab(ids):
        for a in range(ZH):
            part = mm_nt(ctx[a * 512 : (a + 1) * 512, :], lgt[ids * V : (ids + 1) * V])
            vgb[ids, a] = part.astype(BF).reshape(Y, 64, V)
        chain_part(ids, 0)

    def chain_send(ids, way, half, dist):
        sign = 1 - 2 * way
        owner = yat(sign * dist)
        src = vgb.at[ids, 2 * half : 2 * half + 2, owner]
        if dist < (4 if half == way else 3):
            got = vrb.at[ids, way, half, dist]
            net.got(got, ("vy", ids, way, half, dist + 1))
            vsb[ids, way, half, dist - 1] = both(src, got)
            src = vsb.at[ids, way, half, dist - 1]
        there = vrb.at[ids, way, half, dist - 1]
        net.send(src, there, ("vy", ids, way, half, dist), up if way == 0 else down)

    def chain_part(ids, n):
        for half in range(2):
            for way in range(2):
                dist = (4 if half == way else 3) - n
                if dist > 0:
                    chain_send(ids, way, half, dist)

    def chain_round(n):
        for ids in range(2):
            chain_part(ids, n)

    def chain_end():
        for ids in range(2):
            for half in range(2):
                span = slice(2 * half, 2 * half + 2)
                total = vgb[ids, span, y].astype(F32)
                for way in range(2):
                    net.got(vrb.at[ids, way, half, 0], ("vy", ids, way, half, 1))
                    total = total + vrb[ids, way, half, 0].astype(F32)
                vzs[ids, span] = total.astype(BF)
            for dz in (2, 1, 3):
                net.send(vzs.at[ids, zat(dz)], vzr.at[ids, dz], ("vz", ids), {"zh": zat(dz)})

    def vocab_out():
        for ids in (1, 0):
            total = vzs[ids, zh].astype(F32)
            net.got(vzr.at[ids, 1:4], ("vz", ids))
            for dz in range(1, ZH):
                total = total + vzr[ids, dz].astype(F32)
            if ids:
                vgo[...] = total.astype(BF)
                net.send(vgo, vgr, ("vgr",), other)
            else:
                vg_ref[...] = total.astype(BF)

    def hidden_part():
        for j in range(4):
            part = mm(cp[j * 512 : (j + 1) * 512, :], pgs[...])
            hpb[2 * j : 2 * j + 2] = part.astype(BF).reshape(2, 2, 128, T)
        net.send(hpb.at[:, 1 - c], hq, ("hq",), other)

    def hidden_x():
        net.got(hq, ("hq",))
        for j in range(8):
            hs[j // X, j % X] = both(hpb.at[j, c], hq.at[j])
        for dx in (1, 3, 2):
            net.send(hs.at[:, xat(dx)], hrx.at[dx - 1], ("hr",), {"x": xat(dx)})

    def hidden_z():
        net.got(hrx, ("hr",))
        hsum[...] = hs[:, x].astype(F32)
        for i in range(3):
            hsum[...] += hrx[i].astype(F32)
        hz[...] = hsum[1 - zl].astype(BF)
        net.send(hz, hzr, ("hz",), over)

    def hidden_out(mix_grad, mw):
        net.got(hzr, ("hz",))
        total = hsum[zl] + hzr[...].astype(F32)
        mix_grad = jnp.concatenate([mix_grad, jnp.zeros((4, T), F32)], axis=0)
        mix_term = lax.dot_general(mix_grad, mw, TN, precision=lax.Precision.HIGHEST, preferred_element_type=F32)
        hg_ref[...] = (total.T + mix_term).astype(BF)

    def proj_out(own):
        for k in range(K):
            net.got(prx.at[k], ("py", k))
            total = own(k).astype(F32)
            for i in range(4):
                total = total + prx[k, i].astype(F32)
            pst[pl.ds(k, 64, stride=K), :] = total
        pg_ref[...] = pst[...].astype(BF)

    def push_first(to_right, to_left, to_over):
        for k, k_right, k_left in zip(range(K), (0, 2, 1, 3), (1, 3, 0, 2)):
            push_own(k_right, ("ag", 0, -1, k_right), to_right)
            push_own(k_left, ("ag", 0, 1, k_left), to_left)
            push_own(k, ("ag", 1, 0, k), to_over)

    def leader():
        push_first(right, left, over)
        net.send(half_of(0, 0, 1), half_of(0, 0, 1), ("ac", 0, 0), other)
        def piece(dx):
            return pl.ds(pl.multiple_of(xat(dx) * 32, 32), 32)

        for dz in (1, 3, 2):
            span = pl.ds(pl.multiple_of(zat(dz) * 512, 512), 512)
            net.send(hid.at[piece(0), span], hx.at[dz, piece(0)], ("hx",), {"zh": zat(dz)})
        hx[0] = hid[:, pl.ds(pl.multiple_of(zh * 512, 512), 512)]
        small_loads()
        mw, mix_part = mixing()
        turn(V)

        def arrived(dl, dx, k):
            net.got(whole(dl, dx).at[:, lanes(k)], ("ag", dl, dx, k))

        for dx, k, device in ((-1, 0, right), (1, 1, left), (-1, 2, right), (1, 3, left)):
            arrived(0, dx, k)
            push_both(0, dx, k, ("ag", 0, 2, k), device)
        for k in range(K):
            arrived(1, 0, k)
            push_both(1, 0, k, ("ag", 1, -1), right)
            push_both(1, 0, k, ("ag", 1, 1), left)
        for dx, k in ((-1, 1), (1, 0), (-1, 3), (1, 2)):
            arrived(0, dx, k)
        for dl, dx in ((0, -1), (0, 1), (1, 0)):
            pass_on(dl, dx)
        net.got(w.at[:, 0:V], ("ws",))
        turn(0)

        for k in range(K):
            arrived(0, 2, k)
            push_both(0, 2, k, ("ag", 1, 2), over)
        pass_on(0, 2)
        net.got(half_of(0, 0, 0), ("own",))
        add_row(512)
        add_chip(1, 0, 512)
        for dx in (-1, 1, 2):
            net.got(whole(1, dx), ("ag", 1, dx))
            pass_on(1, dx)
            add_chip(1, dx, 512)

        hit = hits(512)
        onehot = hit.astype(F32)

        def grads(k):
            return jnp.exp(eb[:, lanes(k)] - ln_ref[k : k + 1, :]) - onehot

        targets = [jnp.sum(jnp.where(hit, eb[:, lanes(k)], 0.0), axis=0, keepdims=True) for k in range(K)]
        net.got(mixs, ("mix",))
        arx[0] = jnp.concatenate([*targets, mix_part[:4] + mixs[0:4]], axis=0)
        for i, (dl, dx) in enumerate(chips):
            net.send(arx.at[0], arx.at[i + 1], ("ar",), {"zl": (zl + dl) % 2, "x": xat(dx)})

        def part_of(row, k):
            part = mm(w[pl.ds(pl.multiple_of(row * 1024, 1024), 1024), :], lgu[:, lanes(k, 2)])
            for j in (k, k + 1):
                cgb[j, row] = part[:, (j - k) * T : (j - k + 1) * T].astype(BF).reshape(X, 2 * E, T)

        for k in (0, 2):
            for j in (k, k + 1):
                lgu[:, lanes(j)] = (grads(j) * SCALE).astype(BF)
            part_of(1 - zl, k)
            for j in (k, k + 1):
                net.send(cgb.at[j, 1 - zl, xat(2)], zf.at[j], ("zf", j), over)
                net.send(cgb.at[j, 1 - zl, xat(1)], ro.at[j, 0], ("ro", j), right)
                net.send(cgb.at[j, 1 - zl, xat(-1)], ro.at[j, 1], ("ro", j), left)
        part_of(zl, 0)
        part_of(zl, 2)
        for k in range(K):
            eb[:, lanes(k)] = grads(k)

        def far(k):
            net.got(zf.at[k], ("zf", k))
            sf[k] = both(cgb.at[k, zl, xat(2)], zf.at[k])
            net.send(sf.at[k], r2.at[k], ("r2", k), left if k % 2 else right)

        def straight(k):
            if k % 2:
                net.send(cgb.at[k, zl, xat(1)], rx.at[k, 0], ("rx", k), right)
            else:
                net.send(cgb.at[k, zl, xat(-1)], rx.at[k, 1], ("rx", k), left)

        def combine(k):
            net.got(r2.at[k], ("r2", k))
            sp[k] = both(cgb.at[k, zl, xat(-1 if k % 2 else 1)], r2.at[k])
            if k % 2:
                net.send(sp.at[k], rx.at[k, 1], ("rx", k), left)
            else:
                net.send(sp.at[k], rx.at[k, 0], ("rx", k), right)

        def cross(k):
            net.got(ro.at[k], ("ro", k))
            zs[k] = (cgb[k, 1 - zl, x].astype(F32) + ro[k, 0].astype(F32) + ro[k, 1].astype(F32)).astype(BF)
            net.send(zs.at[k], rx.at[k, 2], ("rx", k), over)

        far(0)
        far(1)
        straight(0)
        straight(1)
        net.got(arx.at[1:8], ("ar",))
        sums = jnp.sum(arx[...], axis=0)
        sumb[...] = sums
        net.send(sumb, sumr, ("sum",), other)
        factor, mix_grad = shares(sums)
        scaled(factor, V)
        net.send(lgt.at[V : 2 * V], lgt.at[V : 2 * V], ("lgt",), other)
        far(2)
        far(3)
        straight(2)
        straight(3)
        factor = factor * (1.0 / SCALE)
        cross(0)
        cross(1)
        combine(0)
        combine(1)
        cross(2)
        cross(3)
        combine(2)
        combine(3)

        def z_send(k):
            net.send(pgz.at[k, :, lanes(0)], pgz.at[k, :, lanes(1)], ("pz", 1, k), {"zh": zat(1)})
            net.send(pgz.at[k, :, lanes(0)], pgz.at[k, :, lanes(3)], ("pz", 3, k), {"zh": zat(3)})

        def pre_grads(k):
            net.got(rx.at[k], ("rx", k))
            own = whole(0, 0)[:, k * T : (k + 1) * T].astype(F32)
            grad = cgb[k, zl, x].astype(F32) + rx[k, 0].astype(F32) + rx[k, 1].astype(F32) + rx[k, 2].astype(F32)
            grad = (grad * factor[k : k + 1] * (1.0 - own * own)).astype(BF)
            pgz[k, :, 0:T] = grad
            z_send(k)
            net.send(pgz.at[k, 0:E, lanes(0)], pgs.at[k * E : (k + 1) * E], ("pgs",), other)
            pgs[k * E : (k + 1) * E, :] = grad[E:]

        net.got(hx.at[1:4, piece(0)], ("hx",))
        for dx in (1, 3, 2):
            net.send(hx.at[1:4, piece(0)], hx.at[1:4, piece(0)], ("hy", 4 - dx), {"x": xat(dx)})
        pre_grads(0)
        pre_grads(1)
        pre_grads(2)
        pre_grads(3)
        hidden_part()

        def z_forward(k):
            side = 3 if k % 2 else 1
            net.got(pgz.at[k, :, lanes(side)], ("pz", side, k))
            net.send(pgz.at[k, :, lanes(side)], pgz.at[k, :, lanes(2)], ("pz", 2, k), {"zh": zat(side)})

        z_forward(0)
        z_forward(1)
        hidden_x()
        z_forward(2)
        z_forward(3)
        for dx in (1, 3, 2):
            net.got(hx.at[1:4, piece(dx)], ("hy", dx))
        for dz in range(ZH):
            ht[:, lanes(dz)] = hx[dz].T

        def give(src, j, i, dist):
            net.send(src.at[:, 0:E], prx.at[j, i], ("py", j), {"y": yat(dist), **other})
            net.send(src.at[:, E : 2 * E], prx.at[j, i], ("py", j), {"y": yat(dist)})

        def proj(j):
            net.got(pgz.at[j, :, lanes(1 if j % 2 else 3)], ("pz", 1 if j % 2 else 3, j))
            net.got(pgz.at[j, :, lanes(2)], ("pz", 2, j))
            pp[j] = mm_nt(ht[...], pgz[j]).astype(BF).reshape(Y, 64, 2 * E)
            sign, far_way, near_way = (-1, down, up) if j % 2 else (1, up, down)
            net.send(pp.at[j, yat(4 * sign)], pn.at[j, 0], ("pn", j), far_way)
            net.send(pp.at[j, yat(2 * sign)], pn.at[j, 1], ("pn", j), far_way)
            net.send(pp.at[j, yat(-3 * sign)], pn.at[j, 2], ("pn", j), near_way)
            give(pp.at[j, yat(-sign)], j, 3, -sign)
            net.send(pp.at[j, y, :, 0:E], ppo.at[j], ("po",), other)

        def proj_on(j):
            sign = -1 if j % 2 else 1
            net.got(pn.at[j], ("pn", j))
            for i, dist in enumerate((3 * sign, sign, -2 * sign)):
                pc[j, i] = both(pp.at[j, yat(dist)], pn.at[j, i])
                give(pc.at[j, i], j, i, dist)

        proj(0)
        proj(1)
        proj(2)
        proj(3)
        for k in range(K):
            proj_on(k)
        hidden_z()
        hidden_out(mix_grad, mw)
        net.got(vgr, ("vgr",))
        vg_ref[...] = vgr[...]
        proj_out(lambda k: pp[k, y, :, E : 2 * E])
        net.finish()

    def helper():
        push_first({**right, **other}, {**left, **other}, {**over, **other})
        net.send(half_of(0, 0, 0), half_of(0, 0, 0), ("own",), other)
        small_loads()
        net.send(w.at[:, 0:V], w.at[:, 0:V], ("ws",), other)
        mw, mix_part = mixing()
        mixb[...] = mix_part
        net.send(mixb, mixs, ("mix",), other)
        turn(0)
        for dl, dx in ((0, 0), (0, -1), (0, 1), (0, 2), (1, 0), (1, -1), (1, 1), (1, 2)):
            net.got(whole(dl, dx) if (dl, dx) != (0, 0) else half_of(0, 0, 1), ("ac", dl, dx))
            if (dl, dx) == (0, 2):
                add_row(V)
            elif dl == 1:
                add_chip(dl, dx, V)
        onehot = hits(V).astype(F32)
        for k in range(K):
            eb[0:V, lanes(k)] = jnp.exp(eb[0:V, lanes(k)] - ln_ref[k : k + 1, :]) - onehot
        net.got(sumr, ("sum",))
        factor, mix_grad = shares(sumr[...])
        scaled(factor, 0)
        vocab(0)
        net.got(lgt.at[V : 2 * V], ("lgt",))
        vocab(1)
        chain_round(1)
        net.got(pgs, ("pgs",))
        hidden_part()
        chain_round(2)
        hidden_x()
        chain_round(3)
        hidden_z()
        chain_end()
        hidden_out(mix_grad, mw)
        vocab_out()
        net.got(ppo, ("po",))
        proj_out(lambda k: ppo[k])
        net.finish()

    before = list(net.bulk)
    pl.when(c == 1)(leader)
    net.bulk = before
    pl.when(c == 0)(helper)


def hand_over(*refs):
    copies = [pltpu.make_async_copy(refs[i], refs[3 + i], refs[6].at[i]) for i in range(3)]
    for copy in copies:
        copy.start()
    for copy in copies:
        copy.wait()


def body(hidden, mix_weight, comp_proj, vocab_weight, log_normalizer, targets, loss_grad):
    hbm, vmem = (pl.BlockSpec(memory_space=m) for m in (pl.ANY, pltpu.VMEM))
    scratch = [
        pltpu.VMEM(shape, dtype)
        for shape, dtype in (
            ((T, D), BF),
            ((D * K, E), BF),
            ((D // 2, E), F32),
            ((D, K * E), BF),
            ((D, 2 * V), BF),
            ((2 * V, D), BF),
            ((K, E), BF),
            ((K, T), F32),
            ((1, T), jnp.int32),
            ((1, T), F32),
            ((8, T), F32),
            ((8, T), F32),
            ((D, K * T), BF),
            ((2 * V, K * T), F32),
            ((2 * V, K * T), BF),
            ((2 * V, K * T), BF),
            ((8, 8, T), F32),
            ((8, T), F32),
            ((8, T), F32),
            ((K, ZL, X, 2 * E, T), BF),
            *[((K, 2 * E, T), BF)] * 5,
            ((K, 3, 2 * E, T), BF),
            ((K, 2, 2 * E, T), BF),
            ((K, 2 * E, ZH * T), BF),
            ((K * E, T), BF),
            ((ZH, T, 512), BF),
            ((512, ZH * T), BF),
            ((K, Y, 64, 2 * E), BF),
            ((K, 3, 64, 2 * E), BF),
            ((K, 3, 64, 2 * E), BF),
            ((K, 4, 64, E), BF),
            ((64 * K, E), F32),
            ((K, 64, E), BF),
            ((8, 2, 128, T), BF),
            ((8, 128, T), BF),
            ((ZL, X, 128, T), BF),
            ((3, ZL, 128, T), BF),
            ((ZL, 128, T), F32),
            ((128, T), BF),
            ((128, T), BF),
            ((2, ZH, Y, 64, V), BF),
            ((2, 2, 2, 4, 2, 64, V), BF),
            ((2, 2, 2, 4, 2, 64, V), BF),
            ((2, ZH, 64, V), BF),
            ((2, ZH, 64, V), BF),
            ((64, V), BF),
            ((64, V), BF),
        )
    ]
    scratch += [pltpu.SemaphoreType.DMA((N_SEND,)), pltpu.SemaphoreType.DMA((N_RECV,)), pltpu.SemaphoreType.DMA((14,))]
    shapes = (
        jax.ShapeDtypeStruct((T, E), BF),
        jax.ShapeDtypeStruct((64 * K, E), BF),
        jax.ShapeDtypeStruct((64, V), BF),
    )
    results = pl.pallas_call(
        kernel,
        out_shape=tuple(pltpu.VMEM(s.shape, s.dtype) for s in shapes),
        in_specs=[hbm] * 7,
        out_specs=(vmem,) * 3,
        scratch_shapes=scratch,
        compiler_params=pltpu.CompilerParams(
            collective_id=0, has_side_effects=True, vmem_limit_bytes=56 * 1024 * 1024
        ),
    )(
        hidden,
        comp_proj.reshape(D * K, E),
        vocab_weight,
        mix_weight,
        log_normalizer,
        targets.reshape(1, T),
        loss_grad.reshape(1, T),
    )
    hidden_grad, proj_grad, vocab_grad = pl.pallas_call(
        hand_over,
        out_shape=shapes,
        in_specs=[vmem] * 3,
        out_specs=(hbm,) * 3,
        scratch_shapes=[pltpu.SemaphoreType.DMA((3,))],
    )(*[pltpu.with_memory_space_constraint(r, pltpu.VMEM) for r in results])
    return hidden_grad, proj_grad.reshape(64, K, E), vocab_grad


def solution(mesh):
    split = Mesh(mesh.devices.reshape(ZH, Y, ZL, X, C), ("zh", "y", "zl", "x", "c"))
    tok, voc = ("zh", "y"), ("zl", "x", "c")
    in_specs = (P(tok, None), P(None, voc), P(None, None, voc), P(None, voc), P(None, tok), P(tok), P(tok))
    out_specs = (P(tok, voc), P(tok, None, voc), P(tok, voc))
    return jax.shard_map(body, mesh=split, in_specs=in_specs, out_specs=out_specs, check_vma=False)
```

```python
import math

import jax
import jax.numpy as jnp
from jax import lax
from jax.experimental import pallas as pl
from jax.experimental.pallas import tpu as pltpu
from jax.sharding import Mesh
from jax.sharding import PartitionSpec as P

MESH = pl.DeviceIdType.MESH
BF, F32 = jnp.bfloat16, jnp.float32
ZH, Y, ZL, X, C = 4, 8, 2, 4, 2
D, K, T, V, E = 2048, 4, 128, 256, 128
SCALE = 2.0**-16
BULK = 2 * 1024 * 1024
N_SEND, N_RECV = 5, 109

NT = (((1,), (1,)), ((), ()))
TN = (((0,), (0,)), ((), ()))


def mm(a, b):
    return jnp.dot(a, b, preferred_element_type=F32)


def mm_nt(a, b):
    return lax.dot_general(a, b, NT, preferred_element_type=F32)


class Net:
    def __init__(self, send_sems, recv_sems, yard):
        self.send_sems, self.recv_sems, self.yard = send_sems, recv_sems, yard
        self.roles, self.bulk = {}, []

    def slot(self, role):
        return self.recv_sems.at[self.roles.setdefault(role, len(self.roles))]

    def copy(self, src, dst, role, device):
        return pltpu.make_async_remote_copy(
            src_ref=src,
            dst_ref=dst,
            send_sem=self.send_sems.at[max(len(self.bulk), 1) - 1],
            recv_sem=self.slot(role),
            device_id=device,
            device_id_type=MESH,
        )

    def send(self, src, dst, role, device):
        size = math.prod(src.shape) * src.dtype.itemsize
        if not self.bulk or self.bulk[-1] + size > BULK:
            self.bulk.append(0)
        self.bulk[-1] += size
        self.copy(src, dst, role, device).start()

    def got(self, dst, role):
        self.copy(dst, dst, role, {"c": 1 - lax.axis_index("c")}).wait_recv()

    def finish(self):
        for i, size in enumerate(self.bulk):
            sent = self.yard.at[pl.ds(0, size // (E * 2))]
            pltpu.make_async_copy(sent, sent, self.send_sems.at[i]).wait()


def kernel(
    hid_hbm, cp_hbm, w_hbm, mw_hbm, ln_hbm, tg_hbm, loss_hbm,
    hg_ref, pg_ref, vg_ref,
    hid, cpraw, stage, cp, w, wt, mw_ref, ln_ref, tg_ref, loss_ref, mixb, mixs, ctx, eb, lgt, lgu, arx, sumb, sumr,
    cgb, zf, sf, r2, sp, zs, rx, ro, pgz, pgs, hx, ht, pp, pc, pn, prx, pst, ppo,
    hpb, hq, hs, hrx, hsum, hz, hzr, vgb, vsb, vrb, vzs, vzr, vgo, vgr,
    send_sems, recv_sems, local_sems,
):
    zh, y = lax.axis_index("zh"), lax.axis_index("y")
    zl, x, c = lax.axis_index("zl"), lax.axis_index("x"), lax.axis_index("c")
    chip = zl * X + x
    voc = chip * 2 + c
    net = Net(send_sems, recv_sems, cpraw)

    def xat(dx):
        return lax.rem(x + dx + X, X)

    def yat(dy):
        return lax.rem(y + dy + Y, Y)

    def zat(dz):
        return lax.rem(zh + dz, ZH)

    def lanes(k, n=1):
        return pl.ds(k * T, n * T)

    right, left = {"x": xat(1)}, {"x": xat(-1)}
    up, down = {"y": yat(1)}, {"y": yat(-1)}
    other, over = {"c": 1 - c}, {"zl": 1 - zl}
    chips = [(dl, dx) for dl in range(2) for dx in range(4)][1:]

    barrier = pltpu.get_barrier_semaphore()
    greeted = [{"zl": (zl + dl) % 2, "x": xat(dx)} for dl, dx in chips] + [other]
    greeted += [{"y": yat(dy), "c": a} for dy in (1, 2, 3, 5, 6, 7) for a in (c, 1 - c)]
    greeted += [{"zh": zat(dz)} for dz in range(1, ZH)]
    greeted += [{"c": 1 - c, **device} for device in (right, left, over)]
    parts = 8
    rows = D * K // parts
    loads = [pltpu.make_async_copy(hid_hbm, hid, local_sems.at[0])]
    for q in range(parts):
        span = pl.ds(q * rows, rows)
        loads.append(pltpu.make_async_copy(cp_hbm.at[span], cpraw.at[span], local_sems.at[1 + q]))
    small = [(mw_hbm, mw_ref), (ln_hbm, ln_ref), (tg_hbm, tg_ref), (loss_hbm, loss_ref)]
    small += [(w_hbm, w.at[:, pl.ds(pl.multiple_of(c * V, V), V)])]
    for i, (src, dst) in enumerate(small):
        loads.append(pltpu.make_async_copy(src, dst, local_sems.at[1 + parts + i]))
    for i in (1, 0, *range(2, len(loads))):
        loads[i].start()
    for device in greeted:
        pl.semaphore_signal(barrier, inc=1, device_id=device, device_id_type=MESH)

    pre = jnp.zeros((T, K * E), F32)
    for q in range(parts):
        loads[1 + q].wait()
        stage[...] = cpraw[pl.ds(q * rows, rows), :].astype(F32)
        span = pl.ds(q * (D // parts), D // parts)
        for k in range(K):
            cp[span, lanes(k)] = stage[pl.ds(k, D // parts, stride=K), :].astype(BF)
        if q == 0:
            loads[0].wait()
        if q % 4 == 3:
            span = pl.ds((q - 3) * (D // parts), D // 2)
            pre = pre + mm(hid[:, span], cp[span, :])
    acts = jnp.tanh(pre)
    for k in range(K):
        ctx[pl.ds(pl.multiple_of(voc * E, E), E), lanes(k)] = acts[:, k * E : (k + 1) * E].T.astype(BF)

    pl.semaphore_wait(barrier, len(greeted))

    def chip_at(dl, dx):
        return (zl + dl) % 2 * X + xat(dx)

    def block(dl, dx, half, k):
        at = chip_at(dl, dx) * 256 + half * E
        return ctx.at[pl.ds(pl.multiple_of(at, E), E), lanes(k)]

    def half_of(dl, dx, half):
        return ctx.at[pl.ds(pl.multiple_of(chip_at(dl, dx) * 256 + half * E, E), E)]

    def whole(dl, dx):
        return ctx.at[pl.ds(pl.multiple_of(chip_at(dl, dx) * 256, 256), 256)]

    def push_own(k, role, device):
        net.send(block(0, 0, c, k), block(0, 0, c, k), role, device)

    def push_both(dl, dx, k, role, device):
        net.send(whole(dl, dx).at[:, lanes(k)], whole(dl, dx).at[:, lanes(k)], role, device)

    def pass_on(dl, dx):
        net.send(whole(dl, dx), whole(dl, dx), ("ac", dl, dx), other)

    def small_loads():
        for i in range(len(small)):
            loads[1 + parts + i].wait()

    def mixing():
        mw = jnp.concatenate([mw_ref[...].astype(F32), jnp.zeros((4, E), F32)], axis=0)
        return mw, mm_nt(mw.astype(BF), hid[:, pl.ds(pl.multiple_of(voc * E, E), E)])

    def turn(start):
        for j in range(16):
            wt[start : start + V, j * 128 : (j + 1) * 128] = w[j * 128 : (j + 1) * 128, start : start + V].T

    def add_chip(dl, dx, n):
        span = pl.ds(pl.multiple_of(chip_at(dl, dx) * 256, 256), 256)
        eb[0:n] += mm(wt[0:n, span], ctx[span, :])

    def add_row(n):
        span = pl.ds(pl.multiple_of(zl * 1024, 1024), 1024)
        eb[0:n] = mm(wt[0:n, span], ctx[span, :])

    def hits(n):
        return (lax.broadcasted_iota(jnp.int32, (n, T), 0) + chip * 512) == tg_ref[...]

    def shares(sums):
        exp_mix = jnp.exp(sums[4:])
        weights = exp_mix / jnp.sum(exp_mix, axis=0, keepdims=True)
        joint = weights * jnp.exp(sums[:4] - ln_ref[...])
        posterior = joint / jnp.sum(joint, axis=0, keepdims=True)
        return loss_ref[...] * posterior, loss_ref[...] * (weights - posterior)

    def both(a, b):
        return (a[...].astype(F32) + b[...].astype(F32)).astype(BF)

    def scaled(factor, start):
        for k in range(K):
            lgt[start : start + V, lanes(k)] = (factor[k : k + 1] * eb[start : start + V, lanes(k)]).astype(BF)

    def vocab(ids):
        for a in range(ZH):
            part = mm_nt(ctx[a * 512 : (a + 1) * 512, :], lgt[ids * V : (ids + 1) * V])
            vgb[ids, a] = part.astype(BF).reshape(Y, 64, V)
        chain_part(ids, 0)

    def chain_send(ids, way, half, dist):
        sign = 1 - 2 * way
        owner = yat(sign * dist)
        src = vgb.at[ids, 2 * half : 2 * half + 2, owner]
        if dist < (4 if half == way else 3):
            got = vrb.at[ids, way, half, dist]
            net.got(got, ("vy", ids, way, half, dist + 1))
            vsb[ids, way, half, dist - 1] = both(src, got)
            src = vsb.at[ids, way, half, dist - 1]
        there = vrb.at[ids, way, half, dist - 1]
        net.send(src, there, ("vy", ids, way, half, dist), up if way == 0 else down)

    def chain_part(ids, n):
        for half in range(2):
            for way in range(2):
                dist = (4 if half == way else 3) - n
                if dist > 0:
                    chain_send(ids, way, half, dist)

    def chain_round(n):
        for ids in range(2):
            chain_part(ids, n)

    def chain_end():
        for ids in range(2):
            for half in range(2):
                span = slice(2 * half, 2 * half + 2)
                total = vgb[ids, span, y].astype(F32)
                for way in range(2):
                    net.got(vrb.at[ids, way, half, 0], ("vy", ids, way, half, 1))
                    total = total + vrb[ids, way, half, 0].astype(F32)
                vzs[ids, span] = total.astype(BF)
            for dz in (2, 1, 3):
                net.send(vzs.at[ids, zat(dz)], vzr.at[ids, dz], ("vz", ids), {"zh": zat(dz)})

    def vocab_out():
        for ids in (1, 0):
            total = vzs[ids, zh].astype(F32)
            net.got(vzr.at[ids, 1:4], ("vz", ids))
            for dz in range(1, ZH):
                total = total + vzr[ids, dz].astype(F32)
            if ids:
                vgo[...] = total.astype(BF)
                net.send(vgo, vgr, ("vgr",), other)
            else:
                vg_ref[...] = total.astype(BF)

    def hidden_part():
        for j in range(4):
            part = mm(cp[j * 512 : (j + 1) * 512, :], pgs[...])
            hpb[2 * j : 2 * j + 2] = part.astype(BF).reshape(2, 2, 128, T)
        net.send(hpb.at[:, 1 - c], hq, ("hq",), other)

    def hidden_x():
        net.got(hq, ("hq",))
        for j in range(8):
            hs[j // X, j % X] = both(hpb.at[j, c], hq.at[j])
        for dx in (1, 3, 2):
            net.send(hs.at[:, xat(dx)], hrx.at[dx - 1], ("hr",), {"x": xat(dx)})

    def hidden_z():
        net.got(hrx, ("hr",))
        hsum[...] = hs[:, x].astype(F32)
        for i in range(3):
            hsum[...] += hrx[i].astype(F32)
        hz[...] = hsum[1 - zl].astype(BF)
        net.send(hz, hzr, ("hz",), over)

    def hidden_out(mix_grad, mw):
        net.got(hzr, ("hz",))
        total = hsum[zl] + hzr[...].astype(F32)
        mix_grad = jnp.concatenate([mix_grad, jnp.zeros((4, T), F32)], axis=0)
        mix_term = lax.dot_general(mix_grad, mw, TN, precision=lax.Precision.HIGHEST, preferred_element_type=F32)
        hg_ref[...] = (total.T + mix_term).astype(BF)

    def proj_out(own):
        for k in range(K):
            net.got(prx.at[k], ("py", k))
            total = own(k).astype(F32)
            for i in range(4):
                total = total + prx[k, i].astype(F32)
            pst[pl.ds(k, 64, stride=K), :] = total
        pg_ref[...] = pst[...].astype(BF)

    def push_first(to_right, to_left, to_over):
        for k, k_right, k_left in zip(range(K), (0, 2, 1, 3), (1, 3, 0, 2)):
            push_own(k_right, ("ag", 0, -1, k_right), to_right)
            push_own(k_left, ("ag", 0, 1, k_left), to_left)
            push_own(k, ("ag", 1, 0, k), to_over)

    def leader():
        push_first(right, left, over)
        net.send(half_of(0, 0, 1), half_of(0, 0, 1), ("ac", 0, 0), other)
        def piece(dx):
            return pl.ds(pl.multiple_of(xat(dx) * 32, 32), 32)

        for dz in (1, 3, 2):
            span = pl.ds(pl.multiple_of(zat(dz) * 512, 512), 512)
            net.send(hid.at[piece(0), span], hx.at[dz, piece(0)], ("hx",), {"zh": zat(dz)})
        hx[0] = hid[:, pl.ds(pl.multiple_of(zh * 512, 512), 512)]
        small_loads()
        mw, mix_part = mixing()
        turn(V)

        def arrived(dl, dx, k):
            net.got(whole(dl, dx).at[:, lanes(k)], ("ag", dl, dx, k))

        for dx, k, device in ((-1, 0, right), (1, 1, left), (-1, 2, right), (1, 3, left)):
            arrived(0, dx, k)
            push_both(0, dx, k, ("ag", 0, 2, k), device)
        for k in range(K):
            arrived(1, 0, k)
            push_both(1, 0, k, ("ag", 1, -1), right)
            push_both(1, 0, k, ("ag", 1, 1), left)
        for dx, k in ((-1, 1), (1, 0), (-1, 3), (1, 2)):
            arrived(0, dx, k)
        for dl, dx in ((0, -1), (0, 1), (1, 0)):
            pass_on(dl, dx)
        net.got(w.at[:, 0:V], ("ws",))
        turn(0)

        for k in range(K):
            arrived(0, 2, k)
            push_both(0, 2, k, ("ag", 1, 2), over)
        pass_on(0, 2)
        net.got(half_of(0, 0, 0), ("own",))
        add_row(512)
        add_chip(1, 0, 512)
        for dx in (-1, 1, 2):
            net.got(whole(1, dx), ("ag", 1, dx))
            pass_on(1, dx)
            add_chip(1, dx, 512)

        hit = hits(512)
        onehot = hit.astype(F32)

        def grads(k):
            return jnp.exp(eb[:, lanes(k)] - ln_ref[k : k + 1, :]) - onehot

        targets = [jnp.sum(jnp.where(hit, eb[:, lanes(k)], 0.0), axis=0, keepdims=True) for k in range(K)]
        net.got(mixs, ("mix",))
        arx[0] = jnp.concatenate([*targets, mix_part[:4] + mixs[0:4]], axis=0)
        for i, (dl, dx) in enumerate(chips):
            net.send(arx.at[0], arx.at[i + 1], ("ar",), {"zl": (zl + dl) % 2, "x": xat(dx)})

        def part_of(row, k):
            part = mm(w[pl.ds(pl.multiple_of(row * 1024, 1024), 1024), :], lgu[:, lanes(k, 2)])
            for j in (k, k + 1):
                cgb[j, row] = part[:, (j - k) * T : (j - k + 1) * T].astype(BF).reshape(X, 2 * E, T)

        for k in (0, 2):
            for j in (k, k + 1):
                lgu[:, lanes(j)] = (grads(j) * SCALE).astype(BF)
            part_of(1 - zl, k)
            for j in (k, k + 1):
                net.send(cgb.at[j, 1 - zl, xat(2)], zf.at[j], ("zf", j), over)
                net.send(cgb.at[j, 1 - zl, xat(1)], ro.at[j, 0], ("ro", j), right)
                net.send(cgb.at[j, 1 - zl, xat(-1)], ro.at[j, 1], ("ro", j), left)
        part_of(zl, 0)
        part_of(zl, 2)
        for k in range(K):
            eb[:, lanes(k)] = grads(k)

        def far(k):
            net.got(zf.at[k], ("zf", k))
            sf[k] = both(cgb.at[k, zl, xat(2)], zf.at[k])
            net.send(sf.at[k], r2.at[k], ("r2", k), left if k % 2 else right)

        def straight(k):
            if k % 2:
                net.send(cgb.at[k, zl, xat(1)], rx.at[k, 0], ("rx", k), right)
            else:
                net.send(cgb.at[k, zl, xat(-1)], rx.at[k, 1], ("rx", k), left)

        def combine(k):
            net.got(r2.at[k], ("r2", k))
            sp[k] = both(cgb.at[k, zl, xat(-1 if k % 2 else 1)], r2.at[k])
            if k % 2:
                net.send(sp.at[k], rx.at[k, 1], ("rx", k), left)
            else:
                net.send(sp.at[k], rx.at[k, 0], ("rx", k), right)

        def cross(k):
            net.got(ro.at[k], ("ro", k))
            zs[k] = (cgb[k, 1 - zl, x].astype(F32) + ro[k, 0].astype(F32) + ro[k, 1].astype(F32)).astype(BF)
            net.send(zs.at[k], rx.at[k, 2], ("rx", k), over)

        far(0)
        far(1)
        straight(0)
        straight(1)
        net.got(arx.at[1:8], ("ar",))
        sums = jnp.sum(arx[...], axis=0)
        sumb[...] = sums
        net.send(sumb, sumr, ("sum",), other)
        factor, mix_grad = shares(sums)
        scaled(factor, V)
        net.send(lgt.at[V : 2 * V], lgt.at[V : 2 * V], ("lgt",), other)
        far(2)
        far(3)
        straight(2)
        straight(3)
        factor = factor * (1.0 / SCALE)
        cross(0)
        cross(1)
        combine(0)
        combine(1)
        cross(2)
        cross(3)
        combine(2)
        combine(3)

        def z_send(k):
            net.send(pgz.at[k, :, lanes(0)], pgz.at[k, :, lanes(1)], ("pz", 1, k), {"zh": zat(1)})
            net.send(pgz.at[k, :, lanes(0)], pgz.at[k, :, lanes(3)], ("pz", 3, k), {"zh": zat(3)})

        def pre_grads(k):
            net.got(rx.at[k], ("rx", k))
            own = whole(0, 0)[:, k * T : (k + 1) * T].astype(F32)
            grad = cgb[k, zl, x].astype(F32) + rx[k, 0].astype(F32) + rx[k, 1].astype(F32) + rx[k, 2].astype(F32)
            grad = (grad * factor[k : k + 1] * (1.0 - own * own)).astype(BF)
            pgz[k, :, 0:T] = grad
            z_send(k)
            net.send(pgz.at[k, 0:E, lanes(0)], pgs.at[k * E : (k + 1) * E], ("pgs",), other)
            pgs[k * E : (k + 1) * E, :] = grad[E:]

        net.got(hx.at[1:4, piece(0)], ("hx",))
        for dx in (1, 3, 2):
            net.send(hx.at[1:4, piece(0)], hx.at[1:4, piece(0)], ("hy", 4 - dx), {"x": xat(dx)})
        pre_grads(0)
        pre_grads(1)
        pre_grads(2)
        pre_grads(3)
        hidden_part()

        def z_forward(k):
            side = 3 if k % 2 else 1
            net.got(pgz.at[k, :, lanes(side)], ("pz", side, k))
            net.send(pgz.at[k, :, lanes(side)], pgz.at[k, :, lanes(2)], ("pz", 2, k), {"zh": zat(side)})

        z_forward(0)
        z_forward(1)
        z_forward(2)
        z_forward(3)
        hidden_x()
        for dx in (1, 3, 2):
            net.got(hx.at[1:4, piece(dx)], ("hy", dx))
        for dz in range(ZH):
            ht[:, lanes(dz)] = hx[dz].T

        def give(src, j, i, dist):
            net.send(src.at[:, 0:E], prx.at[j, i], ("py", j), {"y": yat(dist), **other})
            net.send(src.at[:, E : 2 * E], prx.at[j, i], ("py", j), {"y": yat(dist)})

        def proj(j):
            net.got(pgz.at[j, :, lanes(1 if j % 2 else 3)], ("pz", 1 if j % 2 else 3, j))
            net.got(pgz.at[j, :, lanes(2)], ("pz", 2, j))
            pp[j] = mm_nt(ht[...], pgz[j]).astype(BF).reshape(Y, 64, 2 * E)
            sign, far_way, near_way = (-1, down, up) if j % 2 else (1, up, down)
            net.send(pp.at[j, yat(4 * sign)], pn.at[j, 0], ("pn", j), far_way)
            net.send(pp.at[j, yat(2 * sign)], pn.at[j, 1], ("pn", j), far_way)
            net.send(pp.at[j, yat(-3 * sign)], pn.at[j, 2], ("pn", j), near_way)
            give(pp.at[j, yat(-sign)], j, 3, -sign)
            net.send(pp.at[j, y, :, 0:E], ppo.at[j], ("po",), other)

        def proj_on(j):
            sign = -1 if j % 2 else 1
            net.got(pn.at[j], ("pn", j))
            for i, dist in enumerate((3 * sign, sign, -2 * sign)):
                pc[j, i] = both(pp.at[j, yat(dist)], pn.at[j, i])
                give(pc.at[j, i], j, i, dist)

        proj(0)
        proj(1)
        proj(2)
        proj(3)
        for k in range(K):
            proj_on(k)
        hidden_z()
        hidden_out(mix_grad, mw)
        net.got(vgr, ("vgr",))
        vg_ref[...] = vgr[...]
        proj_out(lambda k: pp[k, y, :, E : 2 * E])
        net.finish()

    def helper():
        push_first({**right, **other}, {**left, **other}, {**over, **other})
        net.send(half_of(0, 0, 0), half_of(0, 0, 0), ("own",), other)
        small_loads()
        net.send(w.at[:, 0:V], w.at[:, 0:V], ("ws",), other)
        mw, mix_part = mixing()
        mixb[...] = mix_part
        net.send(mixb, mixs, ("mix",), other)
        turn(0)
        for dl, dx in ((0, 0), (0, -1), (0, 1), (0, 2), (1, 0), (1, -1), (1, 1), (1, 2)):
            net.got(whole(dl, dx) if (dl, dx) != (0, 0) else half_of(0, 0, 1), ("ac", dl, dx))
            if (dl, dx) == (0, 2):
                add_row(V)
            elif dl == 1:
                add_chip(dl, dx, V)
        onehot = hits(V).astype(F32)
        for k in range(K):
            eb[0:V, lanes(k)] = jnp.exp(eb[0:V, lanes(k)] - ln_ref[k : k + 1, :]) - onehot
        net.got(sumr, ("sum",))
        factor, mix_grad = shares(sumr[...])
        scaled(factor, 0)
        vocab(0)
        net.got(lgt.at[V : 2 * V], ("lgt",))
        vocab(1)
        chain_round(1)
        net.got(pgs, ("pgs",))
        hidden_part()
        chain_round(2)
        hidden_x()
        chain_round(3)
        hidden_z()
        chain_end()
        hidden_out(mix_grad, mw)
        vocab_out()
        net.got(ppo, ("po",))
        proj_out(lambda k: ppo[k])
        net.finish()

    before = list(net.bulk)
    pl.when(c == 1)(leader)
    net.bulk = before
    pl.when(c == 0)(helper)


def hand_over(*refs):
    copies = [pltpu.make_async_copy(refs[i], refs[3 + i], refs[6].at[i]) for i in range(3)]
    for copy in copies:
        copy.start()
    for copy in copies:
        copy.wait()


def body(hidden, mix_weight, comp_proj, vocab_weight, log_normalizer, targets, loss_grad):
    hbm, vmem = (pl.BlockSpec(memory_space=m) for m in (pl.ANY, pltpu.VMEM))
    scratch = [
        pltpu.VMEM(shape, dtype)
        for shape, dtype in (
            ((T, D), BF),
            ((D * K, E), BF),
            ((D // 2, E), F32),
            ((D, K * E), BF),
            ((D, 2 * V), BF),
            ((2 * V, D), BF),
            ((K, E), BF),
            ((K, T), F32),
            ((1, T), jnp.int32),
            ((1, T), F32),
            ((8, T), F32),
            ((8, T), F32),
            ((D, K * T), BF),
            ((2 * V, K * T), F32),
            ((2 * V, K * T), BF),
            ((2 * V, K * T), BF),
            ((8, 8, T), F32),
            ((8, T), F32),
            ((8, T), F32),
            ((K, ZL, X, 2 * E, T), BF),
            *[((K, 2 * E, T), BF)] * 5,
            ((K, 3, 2 * E, T), BF),
            ((K, 2, 2 * E, T), BF),
            ((K, 2 * E, ZH * T), BF),
            ((K * E, T), BF),
            ((ZH, T, 512), BF),
            ((512, ZH * T), BF),
            ((K, Y, 64, 2 * E), BF),
            ((K, 3, 64, 2 * E), BF),
            ((K, 3, 64, 2 * E), BF),
            ((K, 4, 64, E), BF),
            ((64 * K, E), F32),
            ((K, 64, E), BF),
            ((8, 2, 128, T), BF),
            ((8, 128, T), BF),
            ((ZL, X, 128, T), BF),
            ((3, ZL, 128, T), BF),
            ((ZL, 128, T), F32),
            ((128, T), BF),
            ((128, T), BF),
            ((2, ZH, Y, 64, V), BF),
            ((2, 2, 2, 4, 2, 64, V), BF),
            ((2, 2, 2, 4, 2, 64, V), BF),
            ((2, ZH, 64, V), BF),
            ((2, ZH, 64, V), BF),
            ((64, V), BF),
            ((64, V), BF),
        )
    ]
    scratch += [pltpu.SemaphoreType.DMA((N_SEND,)), pltpu.SemaphoreType.DMA((N_RECV,)), pltpu.SemaphoreType.DMA((14,))]
    shapes = (
        jax.ShapeDtypeStruct((T, E), BF),
        jax.ShapeDtypeStruct((64 * K, E), BF),
        jax.ShapeDtypeStruct((64, V), BF),
    )
    results = pl.pallas_call(
        kernel,
        out_shape=tuple(pltpu.VMEM(s.shape, s.dtype) for s in shapes),
        in_specs=[hbm] * 7,
        out_specs=(vmem,) * 3,
        scratch_shapes=scratch,
        compiler_params=pltpu.CompilerParams(
            collective_id=0, has_side_effects=True, vmem_limit_bytes=56 * 1024 * 1024
        ),
    )(
        hidden,
        comp_proj.reshape(D * K, E),
        vocab_weight,
        mix_weight,
        log_normalizer,
        targets.reshape(1, T),
        loss_grad.reshape(1, T),
    )
    hidden_grad, proj_grad, vocab_grad = pl.pallas_call(
        hand_over,
        out_shape=shapes,
        in_specs=[vmem] * 3,
        out_specs=(hbm,) * 3,
        scratch_shapes=[pltpu.SemaphoreType.DMA((3,))],
    )(*[pltpu.with_memory_space_constraint(r, pltpu.VMEM) for r in results])
    return hidden_grad, proj_grad.reshape(64, K, E), vocab_grad


def solution(mesh):
    split = Mesh(mesh.devices.reshape(ZH, Y, ZL, X, C), ("zh", "y", "zl", "x", "c"))
    tok, voc = ("zh", "y"), ("zl", "x", "c")
    in_specs = (P(tok, None), P(None, voc), P(None, None, voc), P(None, voc), P(None, tok), P(tok), P(tok))
    out_specs = (P(tok, voc), P(tok, None, voc), P(tok, voc))
    return jax.shard_map(body, mesh=split, in_specs=in_specs, out_specs=out_specs, check_vma=False)
```
